32 devices in a mesh: row: 8 (over z, core), col: 2 (over x), gz: 2 (over y).
Axes of the slice: x: 2, y: 2, z: 4, core: 2. Of those that a mesh axis runs over, the one named last changes fastest.
Arguments:
- initial_field: float32 [8, 32, 32, 256], P(None, 'row', 'col', 'gz'), may hold values from -6 to 6
- source_term: float32 [8, 32, 32, 256], P(None, 'row', 'col', 'gz'), may hold values from -6 to 6
- cell_class: int32 [32, 32, 256], P('row', 'col', 'gz'), may hold values from 0 to 15
- class_shift: float32 [16], replicated, may hold values from 0.05 to 4
- surface_cell: int32 [4096], P(('row', 'col', 'gz')), may hold values from 0 to 8191
- live_count: int32 [32], P(('row', 'col', 'gz')), may hold values from 1 to 128, 2560 in all
- panel_geometry: float32 [4, 4096], P(None, ('row', 'col', 'gz')), may hold values from 0.5 to 2
Outputs:
- final_field: float32 [8, 32, 32, 256], P(None, 'row', 'col', 'gz')
- boundary_potential: float32 [8, 4096], P(None, ('row', 'col', 'gz'))
The draws below stay inside these ranges and needn't reach their ends.
Inputs may be any that keep to these rules, and one draw needn't show every extreme that they name: Slots 0 to live_count[b] - 1 of brick b are in use; the counts sum to 2560. `surface_cell`: A cell index inside the panel's own brick, x * 16 * 128 + y * 128 + z.
All inputs are finite; a program needn't handle non-finite values. No bound on the sum of `live_count` on one device may be relied on, other than what follows from the above.
Results may differ from the reference program's by a relative error of at most 0.004.
Values may be sent and summed in bfloat16 or wider, within the bound.
A program may use at most 128 MiB of HBM per device.

```python
import math
import jax
import jax.numpy as jnp
import numpy as np
from jax import lax

EXC = 8
CLASSES = 16
CX = 4
CY = 16
CZ = 128
SLOTS = 128
SWEEPS = 3
ROUNDS = 2
NX = 32
NY = 32
NZ = 256
PANELS = 4096
N_COL = 2
N_GZ = 2
DEVICES = 32


def plant(result, stream_key, smallest, largest):
    index_at = [jax.random.randint(jax.random.fold_in(stream_key, axis), (), 0, length) for axis, length in enumerate(result.shape)]
    widest = result.shape.index(max(result.shape))
    beside = index_at[:widest] + [(index_at[widest] + 1) % result.shape[widest]] + index_at[widest + 1:]
    return result.at[tuple(index_at)].set(smallest).at[tuple(beside)].set(largest)


def shard_levels(key, extent, pieces, smallest, high):
    loudness = 1.0
    for position, blocks in pieces:
        heights = jax.random.uniform(jax.random.fold_in(jax.random.fold_in(key, 6), position), (blocks,), jnp.float32, smallest / len(pieces), high / len(pieces))
        loudness = loudness * jnp.repeat(jnp.exp(heights), extent[position] // blocks).reshape((-1,) + (1,) * (len(extent) - 1 - position))
    return loudness


def split_up(count, total, most, lean):
    weights = [(1 << 20) // math.isqrt(grade ** lean) + 1 for grade in range(2, count + 1)]
    spare, holding = total - most - (count - 1), [1] * (count - 1)
    while spare > 0:
        candidates = [i for i in range(count - 1) if holding[i] < most]
        mass, budget = sum([weights[i] for i in candidates]), spare
        for i in candidates:
            extra = min(most - holding[i], max(1, budget * weights[i] // mass), spare)
            holding[i] = holding[i] + extra
            spare = spare - extra
    return np.array([most] + holding)


def uneven_parts(own_key, number_of, total, limit, slope):
    if number_of == 2:
        one = jax.random.randint(own_key, (), max(1, total - limit), min(limit, total - 1) + 1)
        return jnp.stack([one, total - one])
    tallies = jnp.asarray(split_up(number_of, total, limit, slope), jnp.int32)
    couples = (number_of - 1) // 2
    donor, receiver = tallies[1:1 + 2 * couples:2], tallies[2:2 + 2 * couples:2]
    room = jnp.minimum(donor - 1, limit - receiver)
    shifted = jax.random.randint(jax.random.fold_in(own_key, 1), (couples,), 0, 1 << 20) % (room + 1)
    tallies = tallies.at[1:1 + 2 * couples:2].set(donor - shifted).at[2:2 + 2 * couples:2].set(receiver + shifted)
    return tallies[jax.random.permutation(jax.random.fold_in(own_key, 2), number_of)]


def bell_draw(stream_key, extent, scale, most, cuts=(), held_as=jnp.bfloat16):
    values = jax.random.normal(stream_key, extent, jnp.float32) * scale
    if len(cuts) > 0:
        values = shard_levels(stream_key, extent, cuts, -0.22, 0.18) * values
    return jnp.clip(values, min=-most, max=most).astype(held_as)


def setup_inputs(seed: int = 0) -> dict:
    seeds = jax.random.split(jax.random.key(seed), 8)
    return {
        "initial_field": bell_draw(seeds[0], (EXC, NX, NY, NZ), 1.0, 6.0, ((1, 8), (2, 2), (3, 2)), jnp.float32),
        "source_term": bell_draw(seeds[1], (EXC, NX, NY, NZ), 1.0, 6.0, ((1, 8), (2, 2), (3, 2)), jnp.float32),
        "cell_class": plant(jax.random.randint(seeds[2], (NX, NY, NZ), 0, CLASSES), jax.random.fold_in(seeds[2], 1), 0, CLASSES - 1).astype(jnp.int32),
        "class_shift": jnp.clip(jnp.exp(jax.random.uniform(seeds[3], (CLASSES,), jnp.float32, math.log(0.05), math.log(4.0))), 0.05, 4.0),
        "surface_cell": plant(jax.random.randint(seeds[4], (PANELS,), 0, CX * CY * CZ), jax.random.fold_in(seeds[4], 1), 0, (CX * CY * CZ) - 1).astype(jnp.int32),
        "live_count": uneven_parts(seeds[5], DEVICES, PANELS * 5 // 8, SLOTS, 2).astype(jnp.int32),
        "panel_geometry": jnp.clip(0.5 + 1.5 * jax.random.uniform(seeds[6], (4, PANELS), jnp.float32) ** shard_levels(seeds[6], (4, PANELS), ((1, 32),), -0.2, 0.2), 0.5, 2.0),
    }


relax_weight = 0.8
wave_number = 25.0
soften = 0.05
coupling = 0.5

def neighbours(padded):
    total = padded[:, 2:, 1:-1, 1:-1] + padded[:, :-2, 1:-1, 1:-1]
    total = total + padded[:, 1:-1, 2:, 1:-1] + padded[:, 1:-1, :-2, 1:-1]
    total = total + padded[:, 1:-1, 1:-1, 2:] + padded[:, 1:-1, 1:-1, :-2]
    return total

def relax(state, padded, forcing, shift_field):
    diagonal = 6.0 + shift_field
    residual = forcing - (diagonal * state - neighbours(padded))
    return state + relax_weight * residual / diagonal

def kernel_tile(sources, targets, factor):
    delta_x = targets[0][None, :] - sources[0][:, None]
    delta_y = targets[1][None, :] - sources[1][:, None]
    delta_z = targets[2][None, :] - sources[2][:, None]
    distance = jnp.sqrt(delta_x * delta_x + delta_y * delta_y + delta_z * delta_z)
    values = sources[3][:, None] * jnp.cos(wave_number * distance) / (distance + soften)
    return (values * factor).astype(jnp.bfloat16)

def reference(initial_field, source_term, cell_class, class_shift, surface_cell, live_count, panel_geometry):
    shift_field = class_shift[cell_class]
    factor = 1.0 / math.sqrt(PANELS)
    slot_index = jnp.arange(PANELS, dtype=jnp.int32)
    owner = (slot_index // SLOTS).astype(jnp.int32)
    live = (slot_index % SLOTS < live_count[owner]).astype(jnp.float32)
    brick_row = owner // (N_COL * N_GZ)
    brick_col = owner // N_GZ % N_COL
    brick_depth = owner % N_GZ
    global_x = brick_row * CX + surface_cell // (CY * CZ)
    global_y = brick_col * CY + surface_cell // CZ % CY
    global_z = brick_depth * CZ + surface_cell % CZ
    cell_of = ((global_x * NY + global_y) * NZ + global_z).astype(jnp.int32)
    width = math.gcd(PANELS, 512)
    blocks = panel_geometry.reshape(4, PANELS // width, width).transpose(1, 0, 2)
    state = initial_field
    load = jnp.zeros_like(source_term)
    potential = jnp.zeros((EXC, PANELS), jnp.float32)
    for round_index in range(ROUNDS):
        forcing = source_term + load
        for sweep_index in range(SWEEPS):
            padded = jnp.pad(state, ((0, 0), (1, 1), (1, 1), (1, 1)))
            state = relax(state, padded, forcing, shift_field)
        density = (state.reshape(EXC, -1)[:, cell_of] * live).astype(jnp.bfloat16)
        density = lax.optimization_barrier(density).astype(jnp.float32)

        def target_block(targets):
            tile = lax.optimization_barrier(kernel_tile(panel_geometry, targets, factor)).astype(jnp.float32)
            return jnp.dot(density, tile, precision=lax.Precision.HIGHEST)
        potential = lax.map(target_block, blocks)
        potential = potential.transpose(1, 0, 2).reshape(EXC, PANELS) * live
        if round_index + 1 < ROUNDS:
            spread = jnp.zeros((EXC, NX * NY * NZ), jnp.float32).at[:, cell_of].add(coupling * potential)
            load = spread.reshape(source_term.shape)
    return (state, potential)
```

```python
import functools
import math

import jax
import jax.numpy as jnp
import numpy as np
from jax import lax
from jax.experimental import pallas as pl
from jax.experimental.pallas import tpu as pltpu
from jax.sharding import PartitionSpec as P

SWEEPS = 3
ROUNDS = 2
STEPS = SWEEPS * ROUNDS

relax_weight = 0.8
wave_number = 25.0
soften = 0.05
coupling = 0.5

MESH = pl.DeviceIdType.MESH
AXES = ("row", "col", "gz")


def cosine_terms(degree=6):
    nodes = 0.125 * (1.0 + np.cos(np.pi * (np.arange(64) + 0.5) / 64))
    fitted = np.polynomial.Polynomial.fit(
        nodes, np.cos(2 * np.pi * np.sqrt(nodes)), degree, domain=[0.0, 0.25]
    )
    return [float(c) for c in fitted.convert().coef]


COSINE = cosine_terms()


def cosine_of_turns(turns):
    fraction = turns - jnp.floor(turns + 0.5)
    square = fraction * fraction
    value = jnp.full_like(square, COSINE[-1])
    for term in reversed(COSINE[:-1]):
        value = value * square + term
    return value


def kernel(
    sizes,
    init_hbm, source_hbm, class_hbm, shift_hbm, cell_hbm, live_hbm, geo_hbm,
    field_ref, potential_ref,
    init_v, source_v, forcing_v, class_v, weight_v, state_v,
    x_out, x_in, y_out, y_in, z_out, z_in,
    geo_all, column_v, tile_v, density_out, density_all, at_cell,
    shift_ref, live_ref, cell_ref, geo_ref,
    local_sem, face_send, face_recv, gather_send, geo_recv, density_recv,
):
    rows, cols, depths = sizes
    devices = rows * cols * depths
    group = cols * depths
    channels, size_x, size_y, size_z = init_hbm.shape
    slots = cell_hbm.shape[1]
    classes = shift_ref.shape[0]
    factor = 1.0 / math.sqrt(slots * devices)
    here = tuple(lax.axis_index(axis) for axis in AXES)
    me = (here[0] * cols + here[1]) * depths + here[2]

    def brick_copies(hbm, vmem, sem):
        return [
            pltpu.make_async_copy(hbm.at[e], vmem.at[:, :, e, :], sem) for e in range(channels)
        ]

    def brick_wait(vmem, sem):
        pltpu.make_async_copy(vmem, vmem, sem).wait()

    copies = [
        pltpu.make_async_copy(class_hbm, class_v, local_sem.at[1]),
        pltpu.make_async_copy(geo_hbm, geo_ref, local_sem.at[3]),
        pltpu.make_async_copy(shift_hbm, shift_ref, local_sem.at[4]),
        pltpu.make_async_copy(cell_hbm, cell_ref, local_sem.at[5]),
        pltpu.make_async_copy(live_hbm, live_ref, local_sem.at[6]),
    ]
    for copy in brick_copies(init_hbm, init_v, local_sem.at[0]):
        copy.start()
    for copy in copies:
        copy.start()

    def nth(k):
        below, above = here[0], rows - 1 - here[0]
        near = here[0] + jnp.where(lax.rem(k, 2) == 1, (k + 1) // 2, -(k // 2))
        far = jnp.where(below < above, k, rows - 1 - k)
        return jnp.where((k <= 2 * below) & (k <= 2 * above), near, far)

    def each_other(action):
        def at(row, first):
            for b in reversed(range(cols)):
                for c in reversed(range(depths)):
                    if first and b == 0 and c == 0:
                        continue
                    action((row, lax.rem(here[1] + b, cols), lax.rem(here[2] + c, depths)))

        def others(i, carry):
            at(nth(rows - 1 - i), False)
            return carry

        lax.fori_loop(0, rows - 1, others, 0)
        at(here[0], True)

    barrier = pltpu.get_barrier_semaphore()
    each_other(
        lambda device: pl.semaphore_signal(barrier, inc=1, device_id=device, device_id_type=MESH)
    )
    for copy in brick_copies(source_hbm, source_v, local_sem.at[2]):
        copy.start()

    cell_shape = (channels, size_z)
    lane = lax.broadcasted_iota(jnp.int32, cell_shape, 1)
    pair = lane >> 1
    edge = (lane == 0) | (lane == size_z - 1)
    slab = (size_y * channels, size_z)
    slab_lane = lax.broadcasted_iota(jnp.int32, slab, 1)

    def pack(k, x, values, packed):
        if x == 0 or x == size_x - 1:
            for y in range(0, size_y, 2):
                both = jnp.concatenate([values[y], values[y + 1]], axis=0).astype(x_out.dtype)
                if x == 0:
                    x_out[k, 0, y // 2] = both
                if x == size_x - 1:
                    x_out[k, 1, y // 2] = both
        half = pl.ds(channels * (x % 2), channels)
        y_out[k, 0, x // 2, half, :] = values[0].astype(y_out.dtype)
        y_out[k, 1, x // 2, half, :] = values[size_y - 1].astype(y_out.dtype)
        for y in range(size_y):
            at = x * size_y + y
            turned = pltpu.roll(values[y], (2 * at + 1) % size_z, 1)
            packed = jnp.where(pair == at, turned, packed)
        return packed

    def face_copies(k):
        made = []
        for axis, (send, receive) in enumerate(((x_out, x_in), (y_out, y_in), (z_out, z_in))):
            count = sizes[axis]
            if count == 1:
                continue
            for up in (0, 1):
                target = {AXES[axis]: here[axis] + (1 if up else -1)}
                source = send.at[k] if axis == 2 else send.at[k, up]
                side = 0 if count == 2 else 1 - up
                copy = functools.partial(
                    pltpu.make_async_remote_copy,
                    src_ref=source,
                    dst_ref=receive.at[k, 1 - up],
                    send_sem=face_send.at[0],
                    recv_sem=face_recv.at[k % 2, 2 * axis + side],
                    device_id=target,
                    device_id_type=MESH,
                )
                landed = receive.at[k, up]
                got = functools.partial(
                    pltpu.make_async_copy,
                    landed,
                    landed,
                    face_recv.at[k % 2, 2 * axis + (0 if count == 2 else up)],
                )
                exists = here[axis] < count - 1 if up else here[axis] > 0
                made.append((copy, got, exists))
        return made

    def start_faces(k):
        for copy, _, exists in face_copies(k):
            pl.when(exists)(lambda copy=copy: copy().start())

    def await_faces(k):
        for _, got, exists in face_copies(k):
            pl.when(exists)(lambda got=got: got().wait())

    def finish_faces(k):
        for copy, _, exists in face_copies(k):
            pl.when(exists)(lambda copy=copy: copy().wait_send())

    x_in[STEPS] = jnp.zeros(x_in.shape[1:], x_in.dtype)
    y_in[STEPS] = jnp.zeros(y_in.shape[1:], y_in.dtype)
    z_in[STEPS] = jnp.zeros(z_in.shape[1:], z_in.dtype)

    with jax.named_scope("w_init"):
        brick_wait(init_v, local_sem.at[0])

    packed = jnp.zeros(cell_shape, jnp.float32)
    for x in range(size_x):
        packed = pack(0, x, [init_v[x, y] for y in range(size_y)], packed)
    z_out[0] = packed

    copies[1].wait()
    eye = lax.broadcasted_iota(jnp.int32, (slots, slots), 0) == lax.broadcasted_iota(
        jnp.int32, (slots, slots), 1
    )
    for i in range(3):
        column = jnp.sum(jnp.where(eye, geo_ref[i : i + 1, :], 0.0), axis=1, keepdims=True)
        column_v[i] = jnp.broadcast_to(column, (slots, slots))
    geo_all[me] = geo_ref[...]

    with jax.named_scope("w_barrier"):
        pl.semaphore_wait(barrier, devices - 1)
    start_faces(0)

    def start_gather(source, gathered, sem):
        def send(device):
            pltpu.make_async_remote_copy(
                src_ref=source,
                dst_ref=gathered.at[me],
                send_sem=gather_send.at[0],
                recv_sem=sem,
                device_id=device,
                device_id_type=MESH,
            ).start()

        each_other(send)

    def await_gather(gathered, count, sem):
        whole = gathered.at[pl.ds(0, count)]
        pltpu.make_async_copy(whole, whole, sem).wait()

    with jax.named_scope("st_geo"):
        start_gather(geo_ref, geo_all, geo_recv.at[0])

    copies[0].wait()
    copies[2].wait()
    for x in range(size_x):
        kind = class_v[x]
        shift = jnp.zeros(kind.shape, jnp.float32)
        for level in range(classes):
            shift = jnp.where(kind == level, shift_ref[level], shift)
        weight = relax_weight / (6.0 + shift)
        weight_v[x] = jnp.broadcast_to(weight[:, None, :], (size_y, channels, size_z))

    copies[3].wait()
    copies[4].wait()
    cell = cell_ref[...]
    bits = size_z.bit_length() - 1
    cell_z = cell & (size_z - 1)
    cell_xy = cell >> bits
    pick_z = lax.broadcasted_iota(jnp.int32, (size_z, slots), 0) == cell_z
    pick_z = jnp.where(pick_z, 1.0, 0.0).astype(jnp.bfloat16)
    for at in range(size_x * size_y):
        at_cell[at] = jnp.broadcast_to(
            jnp.where(cell_xy == at, 1.0, 0.0), (channels, slots)
        )
    live = lax.broadcasted_iota(jnp.int32, (channels, slots), 1) < live_ref[...]
    brick_wait(source_v, local_sem.at[2])

    def now(k, x):
        return init_v[x] if k == 0 else state_v[k - 1, x]

    def inner(k):
        force = source_v if k <= SWEEPS else forcing_v
        blank = jnp.zeros((1,) + cell_shape, jnp.float32)
        for x in range(size_x):
            value = now(k, x)
            around = force[x]
            if x + 1 < size_x:
                around = around + now(k, x + 1)
            if x > 0:
                around = around + now(k, x - 1)
            around = around + jnp.concatenate([value[1:], blank], axis=0)
            around = around + jnp.concatenate([blank, value[:-1]], axis=0)
            flat = value.reshape(slab)
            beside = jnp.where(slab_lane == size_z - 1, 0.0, pltpu.roll(flat, size_z - 1, 1))
            beside = beside + jnp.where(slab_lane == 0, 0.0, pltpu.roll(flat, 1, 1))
            around = around + beside.reshape(value.shape)
            state_v[k, x] = (1.0 - relax_weight) * value + weight_v[x] * around

    def outer(k):
        last = k == STEPS - 1
        slot = []
        for axis in range(3):
            below = jnp.where(here[axis] > 0, k, STEPS)
            above = jnp.where(here[axis] < sizes[axis] - 1, k, STEPS)
            slot.append((below, above))
        beyond = jnp.where(
            (lane & 1) == 0, z_in[slot[2][0], 0], pltpu.roll(z_in[slot[2][1], 1], size_z - 2, 1)
        )
        packed = jnp.zeros(cell_shape, jnp.float32)
        for x in range(size_x):
            results = []
            for y in range(size_y):
                at = x * size_y + y
                around = jnp.where(
                    edge, pltpu.roll(beyond, (2 * size_z - 2 * at) % size_z, 1), 0.0
                )
                half = slice(channels * (y % 2), channels * (y % 2 + 1))
                if x == 0:
                    around = around + x_in[slot[0][0], 0, y // 2].astype(jnp.float32)[half]
                if x == size_x - 1:
                    around = around + x_in[slot[0][1], 1, y // 2].astype(jnp.float32)[half]
                half = slice(channels * (x % 2), channels * (x % 2 + 1))
                if y == 0:
                    around = around + y_in[slot[1][0], 0, x // 2].astype(jnp.float32)[half]
                if y == size_y - 1:
                    around = around + y_in[slot[1][1], 1, x // 2].astype(jnp.float32)[half]
                result = state_v[k, x, y] + weight_v[x, y] * around
                if last:
                    field_ref[x, y] = result
                else:
                    state_v[k, x, y] = result
                results.append(result)
            if not last:
                packed = pack(k + 1, x, results, packed)
        if not last:
            z_out[k + 1] = packed

    pieces = 4
    chunk = slots // pieces

    def make_tiles(first, stop):
        def body(q, carry):
            for j in range(group):
                source = geo_all[q * group + j]
                for piece in range(pieces):
                    span = slice(piece * chunk, (piece + 1) * chunk)
                    delta_x = column_v[0, span, :] - source[0:1, :]
                    delta_y = column_v[1, span, :] - source[1:2, :]
                    delta_z = column_v[2, span, :] - source[2:3, :]
                    square = delta_x * delta_x + delta_y * delta_y + delta_z * delta_z + 1e-30
                    distance = square * lax.rsqrt(square)
                    wave = cosine_of_turns(distance * (wave_number / (2.0 * math.pi)))
                    value = (source[3:4, :] * factor) * wave / (distance + soften)
                    tile_v[q, span, j * slots : (j + 1) * slots] = value.astype(tile_v.dtype)
            return carry

        lax.fori_loop(first, stop, body, 0)

    def apply_tiles(r):
        total = jnp.zeros((channels, slots), jnp.float32)
        for k in range(rows):
            q = nth(k)
            with jax.named_scope(f"w_dens{r}_{k}"):
                await_gather(density_all.at[r], group - (k == 0), density_recv.at[r, q])
            values = jnp.concatenate(
                [density_all[r, q * group + j] for j in range(group)], axis=1
            )
            total = total + lax.dot_general(
                values, tile_v[q], (((1,), (1,)), ((), ())), preferred_element_type=jnp.float32
            )
        return total

    for k in range(STEPS):
        if k != SWEEPS:
            with jax.named_scope(f"inner{k}"):
                inner(k)
        if k == 2:
            with jax.named_scope("w_geogather"):
                await_gather(geo_all, devices - 1, geo_recv.at[0])
            with jax.named_scope("tilesA"):
                make_tiles(0, rows // 4)
        with jax.named_scope(f"w_faces{k}"):
            await_faces(k)
        with jax.named_scope(f"outer{k}"):
            outer(k)
        end = k % SWEEPS == SWEEPS - 1
        if k + 1 < STEPS:
            start_faces(k + 1)
        if not end:
            continue
        r = k // SWEEPS
        with jax.named_scope(f"density{r}"):
            ending = field_ref if k == STEPS - 1 else state_v.at[k]
            flat = ending[...].reshape(size_x * size_y * channels, size_z).astype(jnp.bfloat16)
            picked = jnp.dot(flat, pick_z, preferred_element_type=jnp.float32)
            picked = picked.reshape(size_x * size_y, channels, slots)
            density = jnp.sum(picked * at_cell[...], axis=0)
            density = jnp.where(live, density, 0.0).astype(jnp.bfloat16)
            density_out[r] = density
            density_all[r, me] = density
        with jax.named_scope(f"st_dens{r}"):
            start_gather(density_out.at[r], density_all.at[r], density_recv.at[r, here[0]])
        if r < ROUNDS - 1:
            with jax.named_scope(f"inner{k+1}"):
                inner(k + 1)
        if r == 0:
            with jax.named_scope("tilesB"):
                make_tiles(rows // 4, rows)
        with jax.named_scope(f"apply{r}"):
            potential = jnp.where(live, apply_tiles(r), 0.0)
        if r == ROUNDS - 1:
            potential_ref[...] = potential
        else:
            with jax.named_scope(f"load{r}"):
                half_of = coupling * potential
                big = half_of.astype(jnp.bfloat16).astype(jnp.float32)
                small = half_of - big
                load = jnp.zeros((size_x * size_y * channels, size_z), jnp.float32)
                for part in (big, small):
                    placed = (at_cell[...] * part[None]).astype(jnp.bfloat16)
                    load = load + lax.dot_general(
                        placed.reshape(size_x * size_y * channels, slots), pick_z,
                        (((1,), (1,)), ((), ())), preferred_element_type=jnp.float32,
                    )
                load = load.reshape(size_x, size_y, channels, size_z)
                forcing_v[...] = source_v[...] + load
                state_v[k + 1] = state_v[k + 1] + weight_v[...] * load

    with jax.named_scope("finish"):
        for k in range(STEPS):
            finish_faces(k)
        await_gather(geo_all, devices - 1, gather_send.at[0])
        for r in range(ROUNDS):
            await_gather(density_all.at[r], devices - 1, gather_send.at[0])


def place(field_v, potential_v, field_hbm, potential_hbm, sem):
    channels = field_hbm.shape[0]
    copies = [
        pltpu.make_async_copy(field_v.at[:, :, e, :], field_hbm.at[e], sem.at[0])
        for e in range(channels)
    ]
    copies.append(pltpu.make_async_copy(potential_v, potential_hbm, sem.at[1]))
    for copy in copies:
        copy.start()
    pltpu.make_async_copy(field_v, field_v, sem.at[0]).wait()
    copies[-1].wait()


def local(sizes, initial_field, source_term, cell_class, class_shift, surface_cell, live_count,
          panel_geometry):
    channels, size_x, size_y, size_z = initial_field.shape
    slots = surface_cell.shape[0]
    rows, cols, depths = sizes
    devices, group = rows * cols * depths, cols * depths
    brick = (size_x, size_y, channels, size_z)
    vmem = pl.BlockSpec(memory_space=pltpu.VMEM)
    hbm = pl.BlockSpec(memory_space=pltpu.HBM)
    per_device = slots * (2 * slots + 4 * 8 + ROUNDS * 2 * 2 * channels)
    grant = devices * per_device + 24 * 4 * math.prod(brick)
    operands = [
        pltpu.with_memory_space_constraint(array, pltpu.HBM)
        for array in (
            initial_field, source_term, cell_class, class_shift,
            surface_cell.reshape(1, slots), panel_geometry,
        )
    ]
    operands.insert(5, live_count.reshape(1, 1))
    two = 2 * channels
    field, potential = pl.pallas_call(
        functools.partial(kernel, sizes),
        out_shape=(
            jax.ShapeDtypeStruct(brick, jnp.float32),
            jax.ShapeDtypeStruct((channels, slots), jnp.float32),
        ),
        in_specs=[hbm] * 5 + [pl.BlockSpec(memory_space=pl.ANY), hbm],
        out_specs=(vmem, vmem),
        scratch_shapes=[
            pltpu.VMEM(brick, jnp.float32),
            pltpu.VMEM(brick, jnp.float32),
            pltpu.VMEM(brick, jnp.float32),
            pltpu.VMEM((size_x, size_y, size_z), jnp.int32),
            pltpu.VMEM(brick, jnp.float32),
            pltpu.VMEM((STEPS,) + brick, jnp.float32),
            pltpu.VMEM((STEPS, 2, size_y // 2, two, size_z), jnp.bfloat16),
            pltpu.VMEM((STEPS + 1, 2, size_y // 2, two, size_z), jnp.bfloat16),
            pltpu.VMEM((STEPS, 2, size_x // 2, two, size_z), jnp.bfloat16),
            pltpu.VMEM((STEPS + 1, 2, size_x // 2, two, size_z), jnp.bfloat16),
            pltpu.VMEM((STEPS, channels, size_z), jnp.float32),
            pltpu.VMEM((STEPS + 1, 2, channels, size_z), jnp.float32),
            pltpu.VMEM((devices, 4, slots), jnp.float32),
            pltpu.VMEM((3, slots, slots), jnp.float32),
            pltpu.VMEM((rows, slots, group * slots), jnp.bfloat16),
            pltpu.VMEM((ROUNDS, channels, slots), jnp.bfloat16),
            pltpu.VMEM((ROUNDS, devices, channels, slots), jnp.bfloat16),
            pltpu.VMEM((size_x * size_y, channels, slots), jnp.float32),
            pltpu.SMEM(class_shift.shape, jnp.float32),
            pltpu.VMEM((1, 1), jnp.int32),
            pltpu.VMEM((1, slots), jnp.int32),
            pltpu.VMEM(panel_geometry.shape, jnp.float32),
            pltpu.SemaphoreType.DMA((7,)),
            pltpu.SemaphoreType.DMA((1,)),
            pltpu.SemaphoreType.DMA((2, 6)),
            pltpu.SemaphoreType.DMA((1,)),
            pltpu.SemaphoreType.DMA((1,)),
            pltpu.SemaphoreType.DMA((ROUNDS, rows)),
        ],
        compiler_params=pltpu.CompilerParams(
            collective_id=0, has_side_effects=True, vmem_limit_bytes=grant
        ),
    )(*operands)
    return pl.pallas_call(
        place,
        out_shape=(
            jax.ShapeDtypeStruct(initial_field.shape, jnp.float32),
            jax.ShapeDtypeStruct((channels, slots), jnp.float32),
        ),
        in_specs=[vmem] * 2,
        out_specs=(hbm, hbm),
        scratch_shapes=[pltpu.SemaphoreType.DMA((2,))],
        compiler_params=pltpu.CompilerParams(vmem_limit_bytes=8 * math.prod(brick)),
    )(field, potential)


def solution(mesh):
    placed = (
        P(None, "row", "col", "gz"),
        P(None, "row", "col", "gz"),
        P("row", "col", "gz"),
        P(),
        P(("row", "col", "gz")),
        P(("row", "col", "gz")),
        P(None, ("row", "col", "gz")),
    )
    return jax.shard_map(
        functools.partial(local, tuple(mesh.shape[axis] for axis in AXES)),
        mesh=mesh,
        in_specs=placed,
        out_specs=(P(None, "row", "col", "gz"), P(None, ("row", "col", "gz"))),
        check_vma=False,
    )
```

```python
import functools
import math

import jax
import jax.numpy as jnp
import numpy as np
from jax import lax
from jax.experimental import pallas as pl
from jax.experimental.pallas import tpu as pltpu
from jax.sharding import PartitionSpec as P

ROUNDS = 2

relax_weight = 0.8
wave_number = 25.0
soften = 0.05
coupling = 0.5

MESH = pl.DeviceIdType.MESH
AXES = ("row", "col", "gz")


def cosine_terms(degree=6):
    nodes = 0.125 * (1.0 + np.cos(np.pi * (np.arange(64) + 0.5) / 64))
    fitted = np.polynomial.Polynomial.fit(
        nodes, np.cos(2 * np.pi * np.sqrt(nodes)), degree, domain=[0.0, 0.25]
    )
    return [float(c) for c in fitted.convert().coef]


COSINE = cosine_terms()


def cosine_of_turns(turns):
    fraction = turns - jnp.floor(turns + 0.5)
    square = fraction * fraction
    value = jnp.full_like(square, COSINE[-1])
    for term in reversed(COSINE[:-1]):
        value = value * square + term
    return value


def kernel(
    sizes,
    init_hbm, source_hbm, class_hbm, shift_hbm, cell_hbm, live_hbm, geo_hbm,
    field_ref, potential_ref,
    init_v, source_v, forcing_v, class_v, weight_v, state_v,
    x_out, x_in, y_out, y_in, z_out, z_in, xy_in, xz_in, yz_in,
    wx_out, wx_in, wy_out, wy_in, wz_out, wz_in, rim_x, rim_y, rim_z,
    geo_all, column_v, tile_v, density_out, density_all, at_cell,
    shift_ref, live_ref, cell_ref, geo_ref,
    local_sem, face_send, face_recv, gather_send, geo_recv, density_recv,
):
    rows, cols, depths = sizes
    devices = rows * cols * depths
    group = cols * depths
    channels, size_x, size_y, size_z = init_hbm.shape
    slots = cell_hbm.shape[1]
    classes = shift_ref.shape[0]
    factor = 1.0 / math.sqrt(slots * devices)
    here = tuple(lax.axis_index(axis) for axis in AXES)
    me = (here[0] * cols + here[1]) * depths + here[2]

    def brick_copies(hbm, vmem, sem):
        return [
            pltpu.make_async_copy(hbm.at[e], vmem.at[:, :, e, :], sem) for e in range(channels)
        ]

    def brick_wait(vmem, sem):
        pltpu.make_async_copy(vmem, vmem, sem).wait()

    copies = [
        pltpu.make_async_copy(class_hbm, class_v, local_sem.at[1]),
        pltpu.make_async_copy(geo_hbm, geo_ref, local_sem.at[3]),
        pltpu.make_async_copy(shift_hbm, shift_ref, local_sem.at[4]),
        pltpu.make_async_copy(cell_hbm, cell_ref, local_sem.at[5]),
        pltpu.make_async_copy(live_hbm, live_ref, local_sem.at[6]),
    ]
    for copy in brick_copies(init_hbm, init_v, local_sem.at[0]):
        copy.start()
    for copy in copies:
        copy.start()

    def nth(k):
        below, above = here[0], rows - 1 - here[0]
        near = here[0] + jnp.where(lax.rem(k, 2) == 1, (k + 1) // 2, -(k // 2))
        far = jnp.where(below < above, k, rows - 1 - k)
        return jnp.where((k <= 2 * below) & (k <= 2 * above), near, far)

    def each_other(action):
        def at(row, first):
            for b in reversed(range(cols)):
                for c in reversed(range(depths)):
                    if first and b == 0 and c == 0:
                        continue
                    action((row, lax.rem(here[1] + b, cols), lax.rem(here[2] + c, depths)))

        def others(i, carry):
            at(nth(rows - 1 - i), False)
            return carry

        lax.fori_loop(0, rows - 1, others, 0)
        at(here[0], True)

    barrier = pltpu.get_barrier_semaphore()
    each_other(
        lambda device: pl.semaphore_signal(barrier, inc=1, device_id=device, device_id_type=MESH)
    )
    for copy in brick_copies(source_hbm, source_v, local_sem.at[2]):
        copy.start()

    cell_shape = (channels, size_z)
    lane = lax.broadcasted_iota(jnp.int32, cell_shape, 1)
    pair = lane >> 1
    even = (lane & 1) == 0
    edge = (lane == 0) | (lane == size_z - 1)
    slab = (size_y * channels, size_z)
    slab_lane = lax.broadcasted_iota(jnp.int32, slab, 1)
    first_line = lax.rem(pair, size_y) == 0
    last_line = lax.rem(pair, size_y) == size_y - 1
    low_plane, high_plane = pair < size_y, pair >= (size_x - 1) * size_y

    def turn(value, shift):
        return pltpu.roll(value, shift % size_z, 1)

    def half_of_pair(i):
        return slice(channels * (i % 2), channels * (i % 2) + channels)

    def pack_flat(q, level, values, depth=1):
        for step in range(depth):
            for side, x in ((0, step), (1, size_x - 1 - step)):
                for y in range(0, size_y, 2):
                    both = jnp.concatenate([values[x][y], values[x][y + 1]], axis=0)
                    x_out[q, side, level + step, y // 2] = both.astype(x_out.dtype)
            for side, y in ((0, step), (1, size_y - 1 - step)):
                for x in range(0, size_x, 2):
                    both = jnp.concatenate([values[x][y], values[x + 1][y]], axis=0)
                    y_out[q, side, level + step, x // 2] = both.astype(y_out.dtype)

    def pack_deep(values, depth=1):
        packed = [jnp.zeros(cell_shape, jnp.float32)] * depth
        for x in range(size_x):
            for y in range(size_y):
                at, value = x * size_y + y, values[x][y]
                here_now = pair == at
                packed[0] = jnp.where(here_now, turn(value, 2 * at + 1), packed[0])
                if depth == 2:
                    both = jnp.where(even, turn(value, 2 * at + 2), turn(value, 2 * at))
                    packed[1] = jnp.where(here_now, both, packed[1])
        return packed

    def planes(ref):
        return [[ref[x, y] for y in range(size_y)] for x in range(size_x)]

    def pack(q, values, depth=1):
        pack_flat(q, 0, values, depth)
        for step, packed in enumerate(pack_deep(values, depth)):
            z_out[q, step] = packed

    def pack_force(q, values):
        pack_flat(q, 2, values)
        z_out[q, 2] = pack_deep(values)[0]

    numbers = {}

    def number(*key):
        return numbers.setdefault(key, len(numbers))

    def sided(axis, side):
        return 0 if sizes[axis] == 2 else side

    def there(axis, up):
        return here[axis] + (1 if up else -1)

    def exists(axis, up):
        return here[axis] < sizes[axis] - 1 if up else here[axis] > 0

    faces = [(axis, up) for axis in range(3) if sizes[axis] > 1 for up in (0, 1)]
    corners = [
        (a, ua, b, ub)
        for a, b in ((0, 1), (0, 2), (1, 2))
        if sizes[a] > 1 and sizes[b] > 1
        for ua in (0, 1)
        for ub in (0, 1)
    ]
    outs, ins = (x_out, y_out, z_out), (x_in, y_in, z_in)
    edge_ins = {(0, 1): xy_in, (0, 2): xz_in, (1, 2): yz_in}

    def exchange(q):
        double = q % 2
        span = pl.ds(0, 3 if double else 1)
        made = []

        def add(source, landing, key_out, key_in, target, present):
            send = functools.partial(
                pltpu.make_async_remote_copy,
                src_ref=source,
                dst_ref=landing[0],
                send_sem=face_send.at[0],
                recv_sem=face_recv.at[number(double, *key_out)],
                device_id=target,
                device_id_type=MESH,
            )
            wait = functools.partial(
                pltpu.make_async_copy, landing[1], landing[1], face_recv.at[number(double, *key_in)]
            )
            made.append((send, wait, present))

        for axis, up in faces:
            source = outs[axis].at[q, span] if axis == 2 else outs[axis].at[q, up, span]
            landing = [ins[axis].at[q, side, span] for side in (1 - up, up)]
            add(
                source, landing, (axis, sided(axis, 1 - up)), (axis, sided(axis, up)),
                {AXES[axis]: there(axis, up)}, exists(axis, up),
            )
        for a, ua, b, ub in corners if double else ():
            if (a, b) == (0, 1):
                source = y_out.at[q, ub, 0, (size_x - 1) // 2 if ua else 0]
            else:
                source = z_out.at[q, 0]
            into = edge_ins[a, b]
            landing = [into.at[q // 2, 1 - ua, 1 - ub], into.at[q // 2, ua, ub]]
            add(
                source, landing,
                (a, b, sided(a, 1 - ua), sided(b, 1 - ub)), (a, b, sided(a, ua), sided(b, ub)),
                {AXES[a]: there(a, ua), AXES[b]: there(b, ub)}, exists(a, ua) & exists(b, ub),
            )
        return made

    def weight_messages():
        made = []
        for axis, up in faces:
            send_ref, receive = ((wx_out, wx_in), (wy_out, wy_in), (wz_out, wz_in))[axis]
            source = send_ref if axis == 2 else send_ref.at[up]
            send = functools.partial(
                pltpu.make_async_remote_copy,
                src_ref=source,
                dst_ref=receive.at[1 - up],
                send_sem=face_send.at[0],
                recv_sem=face_recv.at[number("weight", axis, sided(axis, 1 - up))],
                device_id={AXES[axis]: there(axis, up)},
                device_id_type=MESH,
            )
            landed = receive.at[up]
            wait = functools.partial(
                pltpu.make_async_copy, landed, landed,
                face_recv.at[number("weight", axis, sided(axis, up))],
            )
            made.append((send, wait, exists(axis, up)))
        return made

    def start(made):
        for send, _, present in made:
            pl.when(present)(lambda send=send: send().start())

    def land(made):
        for _, wait, present in made:
            pl.when(present)(lambda wait=wait: wait().wait())

    def drain(made):
        for send, _, present in made:
            pl.when(present)(lambda send=send: send().wait_send())

    none = 2 * ROUNDS
    x_in[none] = jnp.zeros(x_in.shape[1:], x_in.dtype)
    y_in[none] = jnp.zeros(y_in.shape[1:], y_in.dtype)
    z_in[none] = jnp.zeros(z_in.shape[1:], z_in.dtype)
    for into in edge_ins.values():
        into[ROUNDS] = jnp.zeros(into.shape[1:], into.dtype)
    wx_in[2] = jnp.zeros(wx_in.shape[1:], wx_in.dtype)
    wy_in[2] = jnp.zeros(wy_in.shape[1:], wy_in.dtype)
    wz_in[2] = jnp.zeros(wz_in.shape[1:], wz_in.dtype)

    with jax.named_scope("w_init"):
        brick_wait(init_v, local_sem.at[0])

    pack(0, planes(init_v))

    copies[1].wait()
    eye = lax.broadcasted_iota(jnp.int32, (slots, slots), 0) == lax.broadcasted_iota(
        jnp.int32, (slots, slots), 1
    )
    for i in range(3):
        column = jnp.sum(jnp.where(eye, geo_ref[i : i + 1, :], 0.0), axis=1, keepdims=True)
        column_v[i] = jnp.broadcast_to(column, (slots, slots))
    geo_all[me] = geo_ref[...]

    with jax.named_scope("w_barrier"):
        pl.semaphore_wait(barrier, devices - 1)
    start(exchange(0))

    def start_gather(source, gathered, sem):
        def send(device):
            pltpu.make_async_remote_copy(
                src_ref=source,
                dst_ref=gathered.at[me],
                send_sem=gather_send.at[0],
                recv_sem=sem,
                device_id=device,
                device_id_type=MESH,
            ).start()

        each_other(send)

    def await_gather(gathered, count, sem):
        whole = gathered.at[pl.ds(0, count)]
        pltpu.make_async_copy(whole, whole, sem).wait()

    with jax.named_scope("st_geo"):
        start_gather(geo_ref, geo_all, geo_recv.at[0])

    copies[0].wait()
    copies[2].wait()
    for x in range(size_x):
        kind = class_v[x]
        shift = jnp.zeros(kind.shape, jnp.float32)
        for level in range(classes):
            shift = jnp.where(kind == level, shift_ref[level], shift)
        weight = relax_weight / (6.0 + shift)
        weight_v[x] = jnp.broadcast_to(weight[:, None, :], (size_y, channels, size_z))
        if x == 0:
            wx_out[0] = weight
        if x == size_x - 1:
            wx_out[1] = weight
        wy_out[0, x : x + 1, :] = weight[0:1]
        wy_out[1, x : x + 1, :] = weight[size_y - 1 : size_y]
    wz_out[...] = pack_deep(planes(weight_v))[0]
    start(weight_messages())

    copies[3].wait()
    copies[4].wait()
    cell = cell_ref[...]
    bits = size_z.bit_length() - 1
    cell_z = cell & (size_z - 1)
    cell_xy = cell >> bits
    pick_z = lax.broadcasted_iota(jnp.int32, (size_z, slots), 0) == cell_z
    pick_z = jnp.where(pick_z, 1.0, 0.0).astype(jnp.bfloat16)
    for at in range(size_x * size_y):
        at_cell[at] = jnp.broadcast_to(
            jnp.where(cell_xy == at, 1.0, 0.0), (channels, slots)
        )
    live = lax.broadcasted_iota(jnp.int32, (channels, slots), 1) < live_ref[...]
    brick_wait(source_v, local_sem.at[2])
    for x in range(size_x):
        forcing_v[0, x] = weight_v[x] * source_v[x]
    pack_force(1, planes(forcing_v.at[0]))

    def inside(value, above, below, first=None, final=None):
        blank = jnp.zeros((1,) + cell_shape, jnp.float32)
        first = blank if first is None else first[None]
        final = blank if final is None else final[None]
        around = jnp.concatenate([value[1:], final], axis=0)
        around = around + jnp.concatenate([first, value[:-1]], axis=0)
        for other in (above, below):
            if other is not None:
                around = around + other
        flat = value.reshape(slab)
        beside = jnp.where(slab_lane == size_z - 1, 0.0, turn(flat, size_z - 1))
        beside = beside + jnp.where(slab_lane == 0, 0.0, turn(flat, 1))
        return around + beside.reshape(value.shape)

    def ends(beyond, at):
        return jnp.where(edge, turn(beyond, -2 * at), 0.0)

    def inner(source, target, force):
        for x in range(size_x):
            value = source[x]
            around = inside(
                value,
                source[x + 1] if x + 1 < size_x else None,
                source[x - 1] if x > 0 else None,
            )
            target[x] = (1.0 - relax_weight) * value + force[x] + weight_v[x] * around

    def pick(axis, q):
        return (
            jnp.where(here[axis] > 0, q, none),
            jnp.where(here[axis] < sizes[axis] - 1, q, none),
        )

    def from_x(q, side, level, y):
        both = x_in[pick(0, q)[side], side, level, y // 2].astype(jnp.float32)
        return both[half_of_pair(y)]

    def from_y(q, side, level, x):
        both = y_in[pick(1, q)[side], side, level, x // 2].astype(jnp.float32)
        return both[half_of_pair(x)]

    def from_z(q, level):
        below, above = pick(2, q)
        return jnp.where(even, z_in[below, 0, level], z_in[above, 1, level])

    def beside_ends(natural):
        return jnp.where(even, natural, turn(natural, -2))

    def corner(a, b, q, side_a, side_b):
        there_a = here[a] > 0 if side_a == 0 else here[a] < sizes[a] - 1
        there_b = here[b] > 0 if side_b == 0 else here[b] < sizes[b] - 1
        return edge_ins[a, b][jnp.where(there_a & there_b, q // 2, ROUNDS), side_a, side_b]

    def corner_xy(q, side_x, side_y):
        both = corner(0, 1, q, side_x, side_y).astype(jnp.float32)
        return both[half_of_pair(size_x - 1 if side_x == 0 else 0)]

    def corner_z(axis, q, side):
        return jnp.where(even, corner(axis, 2, q, side, 0), corner(axis, 2, q, side, 1))

    def outer(target, q):
        beyond = beside_ends(from_z(q, 0))
        for x in range(size_x):
            for y in range(size_y):
                around = ends(beyond, x * size_y + y)
                if x == 0:
                    around = around + from_x(q, 0, 0, y)
                if x == size_x - 1:
                    around = around + from_x(q, 1, 0, y)
                if y == 0:
                    around = around + from_y(q, 0, 0, x)
                if y == size_y - 1:
                    around = around + from_y(q, 1, 0, x)
                target[x, y] = target[x, y] + weight_v[x, y] * around

    def rim(source, q):
        for side in (0, 1):
            x = (size_x - 1) * side
            value = jnp.stack([from_x(q, side, 0, y) for y in range(size_y)])
            far = jnp.stack([from_x(q, side, 1, y) for y in range(size_y)])
            force = jnp.stack([from_x(q, side, 2, y) for y in range(size_y)])
            across = beside_ends(corner_z(0, q, side))
            theirs = size_x - 1 - x
            beyond = jnp.stack([ends(across, theirs * size_y + y) for y in range(size_y)])
            around = beyond + inside(
                value, source[x], far, corner_xy(q, side, 0), corner_xy(q, side, 1)
            )
            weight = wx_in[jnp.where(exists(0, side), side, 2)]
            weight = jnp.broadcast_to(weight[:, None, :], value.shape)
            rim_x[side] = (1.0 - relax_weight) * value + force + weight * around
        for side in (0, 1):
            y = (size_y - 1) * side
            theirs = size_y - 1 - y
            across = beside_ends(corner_z(1, q, side))
            values = [from_y(q, side, 0, x) for x in range(size_x)]
            values = [corner_xy(q, 0, side)] + values + [corner_xy(q, 1, side)]
            weight = wy_in[jnp.where(exists(1, side), side, 2)]
            for x in range(size_x):
                value = values[x + 1]
                around = values[x] + values[x + 2] + source[x, y] + from_y(q, side, 1, x)
                around = around + ends(across, x * size_y + theirs)
                around = around + jnp.where(lane == size_z - 1, 0.0, turn(value, size_z - 1))
                around = around + jnp.where(lane == 0, 0.0, turn(value, 1))
                rim_y[side, x] = (
                    (1.0 - relax_weight) * value
                    + from_y(q, side, 2, x)
                    + weight[x : x + 1, :] * around
                )
        value = from_z(q, 0)
        own = z_out[q, 0]
        around = from_z(q, 1) + jnp.where(even, turn(own, -1), turn(own, 1))
        step = 2 * size_y
        around = around + turn(jnp.where(high_plane, corner_z(0, q, 0), value), step)
        around = around + turn(jnp.where(low_plane, corner_z(0, q, 1), value), -step)
        wrap = 2 * (size_y - 1)
        around = around + jnp.where(first_line, turn(corner_z(1, q, 0), -wrap), turn(value, 2))
        around = around + jnp.where(last_line, turn(corner_z(1, q, 1), wrap), turn(value, -2))
        weight = jnp.where(
            even, wz_in[jnp.where(exists(2, 0), 0, 2)], wz_in[jnp.where(exists(2, 1), 1, 2)]
        )
        rim_z[...] = (1.0 - relax_weight) * value + from_z(q, 2) + weight * around

    def whole(source, target, force):
        beyond = beside_ends(rim_z[...])
        for x in range(size_x):
            value = source[x]
            around = inside(
                value,
                source[x + 1] if x + 1 < size_x else rim_x[1],
                source[x - 1] if x > 0 else rim_x[0],
                rim_y[0, x],
                rim_y[1, x],
            )
            around = around + jnp.stack([ends(beyond, x * size_y + y) for y in range(size_y)])
            target[x] = (1.0 - relax_weight) * value + force[x] + weight_v[x] * around

    pieces = 4
    chunk = slots // pieces

    def make_tiles(first, stop):
        def body(q, carry):
            for j in range(group):
                source = geo_all[q * group + j]
                for piece in range(pieces):
                    span = slice(piece * chunk, (piece + 1) * chunk)
                    delta_x = column_v[0, span, :] - source[0:1, :]
                    delta_y = column_v[1, span, :] - source[1:2, :]
                    delta_z = column_v[2, span, :] - source[2:3, :]
                    square = delta_x * delta_x + delta_y * delta_y + delta_z * delta_z + 1e-30
                    distance = square * lax.rsqrt(square)
                    wave = cosine_of_turns(distance * (wave_number / (2.0 * math.pi)))
                    value = (source[3:4, :] * factor) * wave / (distance + soften)
                    tile_v[q, span, j * slots : (j + 1) * slots] = value.astype(tile_v.dtype)
            return carry

        lax.fori_loop(first, stop, body, 0)

    def apply_tiles(r):
        total = jnp.zeros((channels, slots), jnp.float32)
        for k in range(rows):
            q = nth(k)
            with jax.named_scope(f"w_dens{r}_{k}"):
                await_gather(density_all.at[r], group - (k == 0), density_recv.at[r, q])
            values = jnp.concatenate(
                [density_all[r, q * group + j] for j in range(group)], axis=1
            )
            total = total + lax.dot_general(
                values, tile_v[q], (((1,), (1,)), ((), ())), preferred_element_type=jnp.float32
            )
        return total

    for r in range(ROUNDS):
        single, double = 2 * r, 2 * r + 1
        before = init_v if r == 0 else state_v.at[2]
        once, mid, after = state_v.at[0], state_v.at[1], state_v.at[2]
        if r == ROUNDS - 1:
            after = field_ref
        force = forcing_v.at[r]
        with jax.named_scope(f"inner{r}"):
            inner(before, once, forcing_v.at[0])
        if r > 0:
            with jax.named_scope("tilesB"):
                make_tiles(rows // 4, rows)
        with jax.named_scope(f"w_single{r}"):
            land(exchange(single))
        with jax.named_scope(f"outer{r}"):
            outer(once, single)
        if r > 0:
            with jax.named_scope(f"apply{r-1}"):
                potential = jnp.where(live, apply_tiles(r - 1), 0.0)
            with jax.named_scope(f"load{r}"):
                half_of = coupling * potential
                big = half_of.astype(jnp.bfloat16).astype(jnp.float32)
                small = half_of - big
                load = jnp.zeros((size_x * size_y * channels, size_z), jnp.float32)
                for part in (big, small):
                    placed = (at_cell[...] * part[None]).astype(jnp.bfloat16)
                    load = load + lax.dot_general(
                        placed.reshape(size_x * size_y * channels, slots), pick_z,
                        (((1,), (1,)), ((), ())), preferred_element_type=jnp.float32,
                    )
                load = load.reshape(size_x, size_y, channels, size_z)
                for x in range(size_x):
                    change = weight_v[x] * load[x]
                    force[x] = forcing_v[0, x] + change
                    once[x] = once[x] + change
                pack_force(double, planes(force))
        with jax.named_scope(f"pack{r}"):
            pack(double, planes(once), 2)
        start(exchange(double))
        with jax.named_scope(f"innerd{r}"):
            inner(once, mid, force)
        if r == 0:
            with jax.named_scope("w_weights"):
                land(weight_messages())
            with jax.named_scope("w_geogather"):
                await_gather(geo_all, devices - 1, geo_recv.at[0])
            with jax.named_scope("tilesA"):
                make_tiles(0, rows // 4)
        with jax.named_scope(f"w_double{r}"):
            land(exchange(double))
        with jax.named_scope(f"outerd{r}"):
            outer(mid, double)
        with jax.named_scope(f"rim{r}"):
            rim(once, double)
        with jax.named_scope(f"whole{r}"):
            whole(mid, after, force)
        if r < ROUNDS - 1:
            with jax.named_scope(f"pack_s{r}"):
                pack(2 * r + 2, planes(after))
            start(exchange(2 * r + 2))
        with jax.named_scope(f"density{r}"):
            flat = after[...].reshape(size_x * size_y * channels, size_z).astype(jnp.bfloat16)
            picked = jnp.dot(flat, pick_z, preferred_element_type=jnp.float32)
            picked = picked.reshape(size_x * size_y, channels, slots)
            density = jnp.sum(picked * at_cell[...], axis=0)
            density = jnp.where(live, density, 0.0).astype(jnp.bfloat16)
            density_out[r] = density
            density_all[r, me] = density
        with jax.named_scope(f"st_dens{r}"):
            start_gather(density_out.at[r], density_all.at[r], density_recv.at[r, here[0]])
    with jax.named_scope(f"apply{ROUNDS-1}"):
        potential_ref[...] = jnp.where(live, apply_tiles(ROUNDS - 1), 0.0)

    with jax.named_scope("finish"):
        for q in range(2 * ROUNDS):
            drain(exchange(q))
        drain(weight_messages())
        await_gather(geo_all, devices - 1, gather_send.at[0])
        for r in range(ROUNDS):
            await_gather(density_all.at[r], devices - 1, gather_send.at[0])


def place(field_v, potential_v, field_hbm, potential_hbm, sem):
    channels = field_hbm.shape[0]
    copies = [
        pltpu.make_async_copy(field_v.at[:, :, e, :], field_hbm.at[e], sem.at[0])
        for e in range(channels)
    ]
    copies.append(pltpu.make_async_copy(potential_v, potential_hbm, sem.at[1]))
    for copy in copies:
        copy.start()
    pltpu.make_async_copy(field_v, field_v, sem.at[0]).wait()
    copies[-1].wait()


def local(sizes, initial_field, source_term, cell_class, class_shift, surface_cell, live_count,
          panel_geometry):
    channels, size_x, size_y, size_z = initial_field.shape
    slots = surface_cell.shape[0]
    rows, cols, depths = sizes
    devices, group = rows * cols * depths, cols * depths
    brick = (size_x, size_y, channels, size_z)
    vmem = pl.BlockSpec(memory_space=pltpu.VMEM)
    hbm = pl.BlockSpec(memory_space=pltpu.HBM)
    per_device = slots * (2 * slots + 4 * 8 + ROUNDS * 2 * 2 * channels)
    grant = devices * per_device + 36 * 4 * math.prod(brick)
    operands = [
        pltpu.with_memory_space_constraint(array, pltpu.HBM)
        for array in (
            initial_field, source_term, cell_class, class_shift,
            surface_cell.reshape(1, slots), panel_geometry,
        )
    ]
    operands.insert(5, live_count.reshape(1, 1))
    two, turns = 2 * channels, 2 * ROUNDS
    sides = [min(count, 3) - 1 for count in sizes]
    crossed = sides[0] * sides[1] + sides[0] * sides[2] + sides[1] * sides[2]
    field, potential = pl.pallas_call(
        functools.partial(kernel, sizes),
        out_shape=(
            jax.ShapeDtypeStruct(brick, jnp.float32),
            jax.ShapeDtypeStruct((channels, slots), jnp.float32),
        ),
        in_specs=[hbm] * 5 + [pl.BlockSpec(memory_space=pl.ANY), hbm],
        out_specs=(vmem, vmem),
        scratch_shapes=[
            pltpu.VMEM(brick, jnp.float32),
            pltpu.VMEM(brick, jnp.float32),
            pltpu.VMEM((ROUNDS,) + brick, jnp.float32),
            pltpu.VMEM((size_x, size_y, size_z), jnp.int32),
            pltpu.VMEM(brick, jnp.float32),
            pltpu.VMEM((3,) + brick, jnp.float32),
            pltpu.VMEM((turns, 2, 3, size_y // 2, two, size_z), jnp.bfloat16),
            pltpu.VMEM((turns + 1, 2, 3, size_y // 2, two, size_z), jnp.bfloat16),
            pltpu.VMEM((turns, 2, 3, size_x // 2, two, size_z), jnp.bfloat16),
            pltpu.VMEM((turns + 1, 2, 3, size_x // 2, two, size_z), jnp.bfloat16),
            pltpu.VMEM((turns, 3, channels, size_z), jnp.float32),
            pltpu.VMEM((turns + 1, 2, 3, channels, size_z), jnp.float32),
            pltpu.VMEM((ROUNDS + 1, 2, 2, two, size_z), jnp.bfloat16),
            pltpu.VMEM((ROUNDS + 1, 2, 2, channels, size_z), jnp.float32),
            pltpu.VMEM((ROUNDS + 1, 2, 2, channels, size_z), jnp.float32),
            pltpu.VMEM((2, size_y, size_z), jnp.float32),
            pltpu.VMEM((3, size_y, size_z), jnp.float32),
            pltpu.VMEM((2, size_x, size_z), jnp.float32),
            pltpu.VMEM((3, size_x, size_z), jnp.float32),
            pltpu.VMEM((channels, size_z), jnp.float32),
            pltpu.VMEM((3, channels, size_z), jnp.float32),
            pltpu.VMEM((2, size_y, channels, size_z), jnp.float32),
            pltpu.VMEM((2, size_x, channels, size_z), jnp.float32),
            pltpu.VMEM((channels, size_z), jnp.float32),
            pltpu.VMEM((devices, 4, slots), jnp.float32),
            pltpu.VMEM((3, slots, slots), jnp.float32),
            pltpu.VMEM((rows, slots, group * slots), jnp.bfloat16),
            pltpu.VMEM((ROUNDS, channels, slots), jnp.bfloat16),
            pltpu.VMEM((ROUNDS, devices, channels, slots), jnp.bfloat16),
            pltpu.VMEM((size_x * size_y, channels, slots), jnp.float32),
            pltpu.SMEM(class_shift.shape, jnp.float32),
            pltpu.VMEM((1, 1), jnp.int32),
            pltpu.VMEM((1, slots), jnp.int32),
            pltpu.VMEM(panel_geometry.shape, jnp.float32),
            pltpu.SemaphoreType.DMA((7,)),
            pltpu.SemaphoreType.DMA((1,)),
            pltpu.SemaphoreType.DMA((3 * sum(sides) + crossed,)),
            pltpu.SemaphoreType.DMA((1,)),
            pltpu.SemaphoreType.DMA((1,)),
            pltpu.SemaphoreType.DMA((ROUNDS, rows)),
        ],
        compiler_params=pltpu.CompilerParams(
            collective_id=0, has_side_effects=True, vmem_limit_bytes=grant
        ),
    )(*operands)
    return pl.pallas_call(
        place,
        out_shape=(
            jax.ShapeDtypeStruct(initial_field.shape, jnp.float32),
            jax.ShapeDtypeStruct((channels, slots), jnp.float32),
        ),
        in_specs=[vmem] * 2,
        out_specs=(hbm, hbm),
        scratch_shapes=[pltpu.SemaphoreType.DMA((2,))],
        compiler_params=pltpu.CompilerParams(vmem_limit_bytes=8 * math.prod(brick)),
    )(field, potential)


def solution(mesh):
    placed = (
        P(None, "row", "col", "gz"),
        P(None, "row", "col", "gz"),
        P("row", "col", "gz"),
        P(),
        P(("row", "col", "gz")),
        P(("row", "col", "gz")),
        P(None, ("row", "col", "gz")),
    )
    return jax.shard_map(
        functools.partial(local, tuple(mesh.shape[axis] for axis in AXES)),
        mesh=mesh,
        in_specs=placed,
        out_specs=(P(None, "row", "col", "gz"), P(None, ("row", "col", "gz"))),
        check_vma=False,
    )
```

```python
import functools
import math

import jax
import jax.numpy as jnp
import numpy as np
from jax import lax
from jax.experimental import pallas as pl
from jax.experimental.pallas import tpu as pltpu
from jax.sharding import PartitionSpec as P

ROUNDS = 2

relax_weight = 0.8
wave_number = 25.0
soften = 0.05
coupling = 0.5

MESH = pl.DeviceIdType.MESH
AXES = ("row", "col", "gz")


def cosine_terms(degree=6):
    nodes = 0.125 * (1.0 + np.cos(np.pi * (np.arange(64) + 0.5) / 64))
    fitted = np.polynomial.Polynomial.fit(
        nodes, np.cos(2 * np.pi * np.sqrt(nodes)), degree, domain=[0.0, 0.25]
    )
    return [float(c) for c in fitted.convert().coef]


COSINE = cosine_terms()


def cosine_of_turns(turns):
    fraction = turns - jnp.floor(turns + 0.5)
    square = fraction * fraction
    value = jnp.full_like(square, COSINE[-1])
    for term in reversed(COSINE[:-1]):
        value = value * square + term
    return value


def known_stages(rows):
    stages, reach = [], max(1, rows // 4)
    while reach < rows - 1:
        stages.append(reach)
        reach *= 2
    return stages


def kernel(
    sizes,
    init_hbm, source_hbm, class_hbm, shift_hbm, cell_hbm, live_hbm, geo_hbm,
    field_ref, potential_ref,
    init_v, source_v, forcing_v, class_v, weight_v, state_v,
    x_out, x_in, y_out, y_in, z_out, z_in, xy_in, xz_in, yz_in,
    wx_out, wx_in, wy_out, wy_in, wz_out, wz_in, rim_x, rim_y, rim_z,
    rim_wx, rim_wy, rim_wz,
    geo_all, column_v, tile_v, density_out, density_all, at_cell,
    shift_ref, live_ref, cell_ref, geo_ref,
    known, local_sem, face_send, face_recv, gather_send, geo_recv, density_recv,
):
    rows, cols, depths = sizes
    devices = rows * cols * depths
    group = cols * depths
    channels, size_x, size_y, size_z = init_hbm.shape
    slots = cell_hbm.shape[1]
    classes = shift_ref.shape[0]
    factor = 1.0 / math.sqrt(slots * devices)
    here = tuple(lax.axis_index(axis) for axis in AXES)
    me = (here[0] * cols + here[1]) * depths + here[2]

    reach = max(1, rows // 4)
    barrier = pltpu.get_barrier_semaphore()

    def greet(row, first):
        for b in range(cols):
            for c in range(depths):
                if first and b == 0 and c == 0:
                    continue
                pl.semaphore_signal(
                    barrier, inc=1, device_id_type=MESH,
                    device_id=(row, lax.rem(here[1] + b, cols), lax.rem(here[2] + c, depths)),
                )

    greet(here[0], True)
    for away in range(1, reach + 1):
        pl.when(here[0] >= away)(lambda: greet(here[0] - away, False))
        pl.when(here[0] + away < rows)(lambda: greet(here[0] + away, False))
    near_low = jnp.where(here[0] > reach, here[0] - reach, 0)
    near_high = jnp.where(here[0] + reach < rows, here[0] + reach, rows - 1)
    near = (near_high - near_low + 1) * group - 1

    stages = known_stages(rows)

    def pass_on(stage):
        d = stages[stage]

        def tell(row):
            pl.semaphore_signal(
                known.at[stage], inc=1, device_id={"row": row}, device_id_type=MESH
            )

        pl.when((here[0] >= d) & (here[0] < rows - 1))(lambda: tell(here[0] - d))
        pl.when((here[0] + d < rows) & (here[0] > 0))(lambda: tell(here[0] + d))

    def hear(stage):
        d = stages[stage]
        told = jnp.where(here[0] + d < rows - 1, 1, 0) + jnp.where(here[0] > d, 1, 0)
        pl.when(told > 0)(lambda: pl.semaphore_wait(known.at[stage], told))

    def brick_copies(hbm, vmem, sem):
        return [
            pltpu.make_async_copy(hbm.at[e], vmem.at[:, :, e, :], sem) for e in range(channels)
        ]

    def brick_wait(vmem, sem):
        pltpu.make_async_copy(vmem, vmem, sem).wait()

    copies = [
        pltpu.make_async_copy(class_hbm, class_v, local_sem.at[1]),
        pltpu.make_async_copy(geo_hbm, geo_ref, local_sem.at[3]),
        pltpu.make_async_copy(shift_hbm, shift_ref, local_sem.at[4]),
        pltpu.make_async_copy(cell_hbm, cell_ref, local_sem.at[5]),
        pltpu.make_async_copy(live_hbm, live_ref, local_sem.at[6]),
    ]
    for copy in brick_copies(init_hbm, init_v, local_sem.at[0]):
        copy.start()
    for copy in copies:
        copy.start()

    def nth(k):
        below, above = here[0], rows - 1 - here[0]
        near = here[0] + jnp.where(lax.rem(k, 2) == 1, (k + 1) // 2, -(k // 2))
        far = jnp.where(below < above, k, rows - 1 - k)
        return jnp.where((k <= 2 * below) & (k <= 2 * above), near, far)

    def each_other(action):
        def at(row, first):
            for b in reversed(range(cols)):
                for c in reversed(range(depths)):
                    if first and b == 0 and c == 0:
                        continue
                    action((row, lax.rem(here[1] + b, cols), lax.rem(here[2] + c, depths)))

        def others(i, carry):
            at(nth(rows - 1 - i), False)
            return carry

        lax.fori_loop(0, rows - 1, others, 0)
        at(here[0], True)

    for copy in brick_copies(source_hbm, source_v, local_sem.at[2]):
        copy.start()

    cell_shape = (channels, size_z)
    lane = lax.broadcasted_iota(jnp.int32, cell_shape, 1)
    pair = lane >> 1
    even = (lane & 1) == 0
    edge = (lane == 0) | (lane == size_z - 1)
    slab = (size_y * channels, size_z)
    slab_lane = lax.broadcasted_iota(jnp.int32, slab, 1)
    first_line = lax.rem(pair, size_y) == 0
    last_line = lax.rem(pair, size_y) == size_y - 1
    low_plane, high_plane = pair < size_y, pair >= (size_x - 1) * size_y

    def turn(value, shift):
        return pltpu.roll(value, shift % size_z, 1)

    def half_of_pair(i):
        return slice(channels * (i % 2), channels * (i % 2) + channels)

    def pack_deep(values):
        packed = jnp.zeros(cell_shape, jnp.float32)
        for x in range(size_x):
            for y in range(size_y):
                at = x * size_y + y
                packed = jnp.where(pair == at, turn(values[x][y], 2 * at + 1), packed)
        return packed

    def planes(ref):
        return [[ref[x, y] for y in range(size_y)] for x in range(size_x)]

    def pack(q, values):
        for side, x in ((0, 0), (1, size_x - 1)):
            for y in range(0, size_y, 2):
                both = jnp.concatenate([values[x][y], values[x][y + 1]], axis=0)
                x_out[q, side, y // 2] = both.astype(x_out.dtype)
        for side, y in ((0, 0), (1, size_y - 1)):
            for x in range(0, size_x, 2):
                both = jnp.concatenate([values[x][y], values[x + 1][y]], axis=0)
                y_out[q, side, x // 2] = both.astype(y_out.dtype)
        z_out[q] = pack_deep(values)

    numbers = {}

    def number(*key):
        return numbers.setdefault(key, len(numbers))

    def sided(axis, side):
        return 0 if sizes[axis] == 2 else side

    def there(axis, up):
        return here[axis] + (1 if up else -1)

    def exists(axis, up):
        return here[axis] < sizes[axis] - 1 if up else here[axis] > 0

    faces = [(axis, up) for axis in range(3) if sizes[axis] > 1 for up in (0, 1)]
    corners = [
        (a, ua, b, ub)
        for a, b in ((0, 1), (0, 2), (1, 2))
        if sizes[a] > 1 and sizes[b] > 1
        for ua in (0, 1)
        for ub in (0, 1)
    ]
    outs, ins = (x_out, y_out, z_out), (x_in, y_in, z_in)
    edge_ins = {(0, 1): xy_in, (0, 2): xz_in, (1, 2): yz_in}

    def exchange(q, edges=False):
        kind = q % 3
        made = []

        def add(source, landing, key_out, key_in, target, present):
            send = functools.partial(
                pltpu.make_async_remote_copy,
                src_ref=source,
                dst_ref=landing[0],
                send_sem=face_send.at[0],
                recv_sem=face_recv.at[number(kind, *key_out)],
                device_id=target,
                device_id_type=MESH,
            )
            wait = functools.partial(
                pltpu.make_async_copy, landing[1], landing[1], face_recv.at[number(kind, *key_in)]
            )
            made.append((send, wait, present))

        for axis, up in () if edges else faces:
            source = outs[axis].at[q] if axis == 2 else outs[axis].at[q, up]
            landing = [ins[axis].at[q, side] for side in (1 - up, up)]
            add(
                source, landing, (axis, sided(axis, 1 - up)), (axis, sided(axis, up)),
                {AXES[axis]: there(axis, up)}, exists(axis, up),
            )
        for a, ua, b, ub in corners if edges else ():
            if (a, b) == (0, 1):
                source = y_out.at[q, ub, (size_x - 1) // 2 if ua else 0]
            else:
                source = z_out.at[q]
            into = edge_ins[a, b]
            landing = [into.at[q // 3, 1 - ua, 1 - ub], into.at[q // 3, ua, ub]]
            add(
                source, landing,
                (a, b, sided(a, 1 - ua), sided(b, 1 - ub)), (a, b, sided(a, ua), sided(b, ub)),
                {AXES[a]: there(a, ua), AXES[b]: there(b, ub)}, exists(a, ua) & exists(b, ub),
            )
        return made

    def weight_messages():
        made = []
        for axis, up in faces:
            send_ref, receive = ((wx_out, wx_in), (wy_out, wy_in), (wz_out, wz_in))[axis]
            source = send_ref if axis == 2 else send_ref.at[up]
            send = functools.partial(
                pltpu.make_async_remote_copy,
                src_ref=source,
                dst_ref=receive.at[1 - up],
                send_sem=face_send.at[0],
                recv_sem=face_recv.at[number("weight", axis, sided(axis, 1 - up))],
                device_id={AXES[axis]: there(axis, up)},
                device_id_type=MESH,
            )
            landed = receive.at[up]
            wait = functools.partial(
                pltpu.make_async_copy, landed, landed,
                face_recv.at[number("weight", axis, sided(axis, up))],
            )
            made.append((send, wait, exists(axis, up)))
        return made

    def start(made):
        for send, _, present in made:
            pl.when(present)(lambda send=send: send().start())

    def land(made):
        for _, wait, present in made:
            pl.when(present)(lambda wait=wait: wait().wait())

    def drain(made):
        for send, _, present in made:
            pl.when(present)(lambda send=send: send().wait_send())

    none = 3 * ROUNDS
    x_in[none] = jnp.zeros(x_in.shape[1:], x_in.dtype)
    y_in[none] = jnp.zeros(y_in.shape[1:], y_in.dtype)
    z_in[none] = jnp.zeros(z_in.shape[1:], z_in.dtype)
    for into in edge_ins.values():
        into[ROUNDS] = jnp.zeros(into.shape[1:], into.dtype)
    wx_in[2] = jnp.zeros(wx_in.shape[1:], wx_in.dtype)
    wy_in[2] = jnp.zeros(wy_in.shape[1:], wy_in.dtype)
    wz_in[2] = jnp.zeros(wz_in.shape[1:], wz_in.dtype)

    with jax.named_scope("w_init"):
        brick_wait(init_v, local_sem.at[0])

    pack(0, planes(init_v))

    copies[1].wait()
    eye = lax.broadcasted_iota(jnp.int32, (slots, slots), 0) == lax.broadcasted_iota(
        jnp.int32, (slots, slots), 1
    )
    for i in range(3):
        column = jnp.sum(jnp.where(eye, geo_ref[i : i + 1, :], 0.0), axis=1, keepdims=True)
        column_v[i] = jnp.broadcast_to(column, (slots, slots))
    geo_all[me] = geo_ref[...]

    with jax.named_scope("w_barrier"):
        pl.semaphore_wait(barrier, near)
    if stages:
        pass_on(0)
    start(exchange(0))

    def start_gather(source, gathered, sem):
        def send(device):
            pltpu.make_async_remote_copy(
                src_ref=source,
                dst_ref=gathered.at[me],
                send_sem=gather_send.at[0],
                recv_sem=sem,
                device_id=device,
                device_id_type=MESH,
            ).start()

        each_other(send)

    def await_gather(gathered, count, sem):
        whole = gathered.at[pl.ds(0, count)]
        pltpu.make_async_copy(whole, whole, sem).wait()

    copies[0].wait()
    copies[2].wait()
    for x in range(size_x):
        kind = class_v[x]
        shift = jnp.zeros(kind.shape, jnp.float32)
        for level in range(classes):
            shift = jnp.where(kind == level, shift_ref[level], shift)
        weight = relax_weight / (6.0 + shift)
        weight_v[x] = jnp.broadcast_to(weight[:, None, :], (size_y, channels, size_z))
        if x == 0:
            wx_out[0] = weight
        if x == size_x - 1:
            wx_out[1] = weight
        wy_out[0, x : x + 1, :] = weight[0:1]
        wy_out[1, x : x + 1, :] = weight[size_y - 1 : size_y]
    wz_out[...] = pack_deep(planes(weight_v))
    start(weight_messages())

    copies[3].wait()
    copies[4].wait()
    cell = cell_ref[...]
    bits = size_z.bit_length() - 1
    cell_z = cell & (size_z - 1)
    cell_xy = cell >> bits
    pick_z = lax.broadcasted_iota(jnp.int32, (size_z, slots), 0) == cell_z
    pick_z = jnp.where(pick_z, 1.0, 0.0).astype(jnp.bfloat16)
    for at in range(size_x * size_y):
        at_cell[at] = jnp.broadcast_to(
            jnp.where(cell_xy == at, 1.0, 0.0), (channels, slots)
        )
    live = lax.broadcasted_iota(jnp.int32, (channels, slots), 1) < live_ref[...]
    brick_wait(source_v, local_sem.at[2])
    for x in range(size_x):
        forcing_v[0, x] = weight_v[x] * source_v[x]

    def inside(value, above, below):
        blank = jnp.zeros((1,) + cell_shape, jnp.float32)
        around = jnp.concatenate([value[1:], blank], axis=0)
        around = around + jnp.concatenate([blank, value[:-1]], axis=0)
        for other in (above, below):
            if other is not None:
                around = around + other
        flat = value.reshape(slab)
        beside = jnp.where(slab_lane == size_z - 1, 0.0, turn(flat, size_z - 1))
        beside = beside + jnp.where(slab_lane == 0, 0.0, turn(flat, 1))
        return around + beside.reshape(value.shape)

    def ends(beyond, at):
        return jnp.where(edge, turn(beyond, -2 * at), 0.0)

    def inner(source, target, force):
        for x in range(size_x):
            value = source[x]
            around = inside(
                value,
                source[x + 1] if x + 1 < size_x else None,
                source[x - 1] if x > 0 else None,
            )
            target[x] = (1.0 - relax_weight) * value + force[x] + weight_v[x] * around

    def pick(axis, q):
        return (
            jnp.where(here[axis] > 0, q, none),
            jnp.where(here[axis] < sizes[axis] - 1, q, none),
        )

    def from_x(q, side, y):
        both = x_in[pick(0, q)[side], side, y // 2].astype(jnp.float32)
        return both[half_of_pair(y)]

    def from_y(q, side, x):
        both = y_in[pick(1, q)[side], side, x // 2].astype(jnp.float32)
        return both[half_of_pair(x)]

    def from_z(q):
        below, above = pick(2, q)
        return jnp.where(even, z_in[below, 0], z_in[above, 1])

    def beside_ends(natural):
        return jnp.where(even, natural, turn(natural, -2))

    def corner(a, b, q, side_a, side_b):
        there_a = here[a] > 0 if side_a == 0 else here[a] < sizes[a] - 1
        there_b = here[b] > 0 if side_b == 0 else here[b] < sizes[b] - 1
        return edge_ins[a, b][jnp.where(there_a & there_b, q // 3, ROUNDS), side_a, side_b]

    def corner_xy(q, side_x, side_y):
        both = corner(0, 1, q, side_x, side_y).astype(jnp.float32)
        return both[half_of_pair(size_x - 1 if side_x == 0 else 0)]

    def corner_z(axis, q, side):
        return jnp.where(even, corner(axis, 2, q, side, 0), corner(axis, 2, q, side, 1))

    def outer(target, q):
        beyond = beside_ends(from_z(q))
        for x in range(size_x):
            for y in range(size_y):
                around = ends(beyond, x * size_y + y)
                if x == 0:
                    around = around + from_x(q, 0, y)
                if x == size_x - 1:
                    around = around + from_x(q, 1, y)
                if y == 0:
                    around = around + from_y(q, 0, x)
                if y == size_y - 1:
                    around = around + from_y(q, 1, x)
                target[x, y] = target[x, y] + weight_v[x, y] * around

    def spread_weights():
        for side in (0, 1):
            weight = wx_in[jnp.where(exists(0, side), side, 2)]
            rim_wx[side] = jnp.broadcast_to(weight[:, None, :], (size_y,) + cell_shape)
            weight = wy_in[jnp.where(exists(1, side), side, 2)]
            rim_wy[side] = jnp.broadcast_to(weight[:, None, :], (size_x,) + cell_shape)
        rim_wz[...] = jnp.where(
            even, wz_in[jnp.where(exists(2, 0), 0, 2)], wz_in[jnp.where(exists(2, 1), 1, 2)]
        )

    def own_rim(source, q):
        for side in (0, 1):
            rim_x[side] = rim_wx[side] * source[(size_x - 1) * side]
            for x in range(size_x):
                rim_y[side, x] = rim_wy[side, x] * source[x, (size_y - 1) * side]
        own = z_out[q]
        rim_z[...] = rim_wz[...] * jnp.where(even, turn(own, -1), turn(own, 1))

    def edge_rim(q):
        for side in (0, 1):
            across = beside_ends(corner_z(0, q, side))
            theirs = (size_x - 1) * (1 - side)
            for y in range(size_y):
                around = ends(across, theirs * size_y + y)
                if y == 0:
                    around = around + corner_xy(q, side, 0)
                if y == size_y - 1:
                    around = around + corner_xy(q, side, 1)
                rim_x[side, y] = rim_x[side, y] + rim_wx[side, y] * around
        for side in (0, 1):
            across = beside_ends(corner_z(1, q, side))
            theirs = (size_y - 1) * (1 - side)
            for x in range(size_x):
                around = ends(across, x * size_y + theirs)
                if x == 0:
                    around = around + corner_xy(q, 0, side)
                if x == size_x - 1:
                    around = around + corner_xy(q, 1, side)
                rim_y[side, x] = rim_y[side, x] + rim_wy[side, x] * around
        step, wrap = 2 * size_y, 2 * (size_y - 1)
        around = turn(jnp.where(high_plane, corner_z(0, q, 0), 0.0), step)
        around = around + turn(jnp.where(low_plane, corner_z(0, q, 1), 0.0), -step)
        around = around + jnp.where(first_line, turn(corner_z(1, q, 0), -wrap), 0.0)
        around = around + jnp.where(last_line, turn(corner_z(1, q, 1), wrap), 0.0)
        rim_z[...] = rim_z[...] + rim_wz[...] * around

    def add_rim(target, q):
        beyond = beside_ends(rim_z[...] + from_z(q))
        for x in range(size_x):
            for y in range(size_y):
                around = ends(beyond, x * size_y + y)
                if x == 0:
                    around = around + (rim_x[0, y] + from_x(q, 0, y))
                if x == size_x - 1:
                    around = around + (rim_x[1, y] + from_x(q, 1, y))
                if y == 0:
                    around = around + (rim_y[0, x] + from_y(q, 0, x))
                if y == size_y - 1:
                    around = around + (rim_y[1, x] + from_y(q, 1, x))
                target[x, y] = target[x, y] + weight_v[x, y] * around

    pieces = 4
    chunk = slots // pieces

    def make_tiles(first, stop):
        def body(q, carry):
            for j in range(group):
                source = geo_all[q * group + j]
                for piece in range(pieces):
                    span = slice(piece * chunk, (piece + 1) * chunk)
                    delta_x = column_v[0, span, :] - source[0:1, :]
                    delta_y = column_v[1, span, :] - source[1:2, :]
                    delta_z = column_v[2, span, :] - source[2:3, :]
                    square = delta_x * delta_x + delta_y * delta_y + delta_z * delta_z + 1e-30
                    distance = square * lax.rsqrt(square)
                    wave = cosine_of_turns(distance * (wave_number / (2.0 * math.pi)))
                    value = (source[3:4, :] * factor) * wave / (distance + soften)
                    tile_v[q, span, j * slots : (j + 1) * slots] = value.astype(tile_v.dtype)
            return carry

        lax.fori_loop(first, stop, body, 0)

    def apply_tiles(r):
        total = jnp.zeros((channels, slots), jnp.float32)
        for k in range(rows):
            q = nth(k)
            with jax.named_scope(f"w_dens{r}_{k}"):
                await_gather(density_all.at[r], group - (k == 0), density_recv.at[r, q])
            values = jnp.concatenate(
                [density_all[r, q * group + j] for j in range(group)], axis=1
            )
            total = total + lax.dot_general(
                values, tile_v[q], (((1,), (1,)), ((), ())), preferred_element_type=jnp.float32
            )
        return total

    def drain_now():
        for q in range(3 * ROUNDS - 2):
            drain(exchange(q))
            if q % 3 == 1:
                drain(exchange(q, edges=True))
        drain(weight_messages())
        await_gather(geo_all, devices - 1, gather_send.at[0])
        for r in range(ROUNDS - 1):
            await_gather(density_all.at[r], devices - 1, gather_send.at[0])

    for r in range(ROUNDS):
        single, double = 3 * r, 3 * r + 1
        before = init_v if r == 0 else state_v.at[2]
        once, mid, after = state_v.at[0], state_v.at[1], state_v.at[2]
        if r == ROUNDS - 1:
            after = field_ref
        force = forcing_v.at[r]
        with jax.named_scope(f"inner{r}"):
            inner(before, once, forcing_v.at[0])
        if r > 0:
            with jax.named_scope("tilesB"):
                await_gather(geo_all, devices - 1, geo_recv.at[0])
                make_tiles(0, rows)
        if r == 0:
            with jax.named_scope("w_known0"):
                for stage in range(len(stages) - 1):
                    hear(stage)
                    pass_on(stage + 1)
        with jax.named_scope(f"w_single{r}"):
            land(exchange(single))
        with jax.named_scope(f"outer{r}"):
            outer(once, single)
        if r > 0:
            with jax.named_scope(f"apply{r-1}"):
                potential = jnp.where(live, apply_tiles(r - 1), 0.0)
            with jax.named_scope(f"load{r}"):
                half_of = coupling * potential
                big = half_of.astype(jnp.bfloat16).astype(jnp.float32)
                small = half_of - big
                load = jnp.zeros((size_x * size_y * channels, size_z), jnp.float32)
                for part in (big, small):
                    placed = (at_cell[...] * part[None]).astype(jnp.bfloat16)
                    load = load + lax.dot_general(
                        placed.reshape(size_x * size_y * channels, slots), pick_z,
                        (((1,), (1,)), ((), ())), preferred_element_type=jnp.float32,
                    )
                load = load.reshape(size_x, size_y, channels, size_z)
                for x in range(size_x):
                    change = weight_v[x] * load[x]
                    force[x] = forcing_v[0, x] + change
                    once[x] = once[x] + change
        with jax.named_scope(f"pack{r}"):
            pack(double, planes(once))
        start(exchange(double, edges=True))
        start(exchange(double))
        with jax.named_scope(f"innerd{r}"):
            inner(once, mid, force)
        with jax.named_scope(f"packd{r}"):
            pack(double + 1, planes(mid))
        start(exchange(double + 1))
        if r == 0:
            with jax.named_scope("w_weights"):
                land(weight_messages())
                spread_weights()
            with jax.named_scope("w_known"):
                if stages:
                    hear(len(stages) - 1)
            with jax.named_scope("st_geo"):
                start_gather(geo_ref, geo_all, geo_recv.at[0])
        else:
            drain_now()
        own_rim(once, double)
        with jax.named_scope(f"w_double{r}"):
            land(exchange(double))
        with jax.named_scope(f"outerd{r}"):
            outer(mid, double)
            inner(mid, after, force)
        with jax.named_scope(f"w_edges{r}"):
            land(exchange(double, edges=True))
        with jax.named_scope(f"before_rim{r}"):
            edge_rim(double)
        with jax.named_scope(f"w_rim{r}"):
            land(exchange(double + 1))
        with jax.named_scope(f"rim{r}"):
            add_rim(after, double + 1)
        with jax.named_scope(f"density{r}"):
            flat = after[...].reshape(size_x * size_y * channels, size_z).astype(jnp.bfloat16)
            picked = jnp.dot(flat, pick_z, preferred_element_type=jnp.float32)
            picked = picked.reshape(size_x * size_y, channels, slots)
            density = jnp.sum(picked * at_cell[...], axis=0)
            density = jnp.where(live, density, 0.0).astype(jnp.bfloat16)
            density_out[r] = density
            density_all[r, me] = density
        with jax.named_scope(f"st_dens{r}"):
            start_gather(density_out.at[r], density_all.at[r], density_recv.at[r, here[0]])
        if r < ROUNDS - 1:
            with jax.named_scope(f"pack_s{r}"):
                pack(single + 3, planes(after))
            start(exchange(single + 3))
    drain(exchange(3 * ROUNDS - 2))
    drain(exchange(3 * ROUNDS - 2, edges=True))
    drain(exchange(3 * ROUNDS - 1))
    with jax.named_scope(f"apply{ROUNDS-1}"):
        potential_ref[...] = jnp.where(live, apply_tiles(ROUNDS - 1), 0.0)

    with jax.named_scope("finish"):
        await_gather(density_all.at[ROUNDS - 1], devices - 1, gather_send.at[0])


def place(field_v, potential_v, field_hbm, potential_hbm, sem):
    channels = field_hbm.shape[0]
    copies = [
        pltpu.make_async_copy(field_v.at[:, :, e, :], field_hbm.at[e], sem.at[0])
        for e in range(channels)
    ]
    copies.append(pltpu.make_async_copy(potential_v, potential_hbm, sem.at[1]))
    for copy in copies:
        copy.start()
    pltpu.make_async_copy(field_v, field_v, sem.at[0]).wait()
    copies[-1].wait()


def local(sizes, initial_field, source_term, cell_class, class_shift, surface_cell, live_count,
          panel_geometry):
    channels, size_x, size_y, size_z = initial_field.shape
    slots = surface_cell.shape[0]
    rows, cols, depths = sizes
    devices, group = rows * cols * depths, cols * depths
    brick = (size_x, size_y, channels, size_z)
    vmem = pl.BlockSpec(memory_space=pltpu.VMEM)
    hbm = pl.BlockSpec(memory_space=pltpu.HBM)
    per_device = slots * (2 * slots + 4 * 8 + ROUNDS * 2 * 2 * channels)
    grant = devices * per_device + 36 * 4 * math.prod(brick)
    operands = [
        pltpu.with_memory_space_constraint(array, pltpu.HBM)
        for array in (
            initial_field, source_term, cell_class, class_shift,
            surface_cell.reshape(1, slots), panel_geometry,
        )
    ]
    operands.insert(5, live_count.reshape(1, 1))
    two, turns = 2 * channels, 3 * ROUNDS
    sides = [min(count, 3) - 1 for count in sizes]
    crossed = sides[0] * sides[1] + sides[0] * sides[2] + sides[1] * sides[2]
    field, potential = pl.pallas_call(
        functools.partial(kernel, sizes),
        out_shape=(
            jax.ShapeDtypeStruct(brick, jnp.float32),
            jax.ShapeDtypeStruct((channels, slots), jnp.float32),
        ),
        in_specs=[hbm] * 5 + [pl.BlockSpec(memory_space=pl.ANY), hbm],
        out_specs=(vmem, vmem),
        scratch_shapes=[
            pltpu.VMEM(brick, jnp.float32),
            pltpu.VMEM(brick, jnp.float32),
            pltpu.VMEM((ROUNDS,) + brick, jnp.float32),
            pltpu.VMEM((size_x, size_y, size_z), jnp.int32),
            pltpu.VMEM(brick, jnp.float32),
            pltpu.VMEM((3,) + brick, jnp.float32),
            pltpu.VMEM((turns, 2, size_y // 2, two, size_z), jnp.bfloat16),
            pltpu.VMEM((turns + 1, 2, size_y // 2, two, size_z), jnp.bfloat16),
            pltpu.VMEM((turns, 2, size_x // 2, two, size_z), jnp.bfloat16),
            pltpu.VMEM((turns + 1, 2, size_x // 2, two, size_z), jnp.bfloat16),
            pltpu.VMEM((turns, channels, size_z), jnp.float32),
            pltpu.VMEM((turns + 1, 2, channels, size_z), jnp.float32),
            pltpu.VMEM((ROUNDS + 1, 2, 2, two, size_z), jnp.bfloat16),
            pltpu.VMEM((ROUNDS + 1, 2, 2, channels, size_z), jnp.float32),
            pltpu.VMEM((ROUNDS + 1, 2, 2, channels, size_z), jnp.float32),
            pltpu.VMEM((2, size_y, size_z), jnp.float32),
            pltpu.VMEM((3, size_y, size_z), jnp.float32),
            pltpu.VMEM((2, size_x, size_z), jnp.float32),
            pltpu.VMEM((3, size_x, size_z), jnp.float32),
            pltpu.VMEM((channels, size_z), jnp.float32),
            pltpu.VMEM((3, channels, size_z), jnp.float32),
            pltpu.VMEM((2, size_y, channels, size_z), jnp.float32),
            pltpu.VMEM((2, size_x, channels, size_z), jnp.float32),
            pltpu.VMEM((channels, size_z), jnp.float32),
            pltpu.VMEM((2, size_y, channels, size_z), jnp.float32),
            pltpu.VMEM((2, size_x, channels, size_z), jnp.float32),
            pltpu.VMEM((channels, size_z), jnp.float32),
            pltpu.VMEM((devices, 4, slots), jnp.float32),
            pltpu.VMEM((3, slots, slots), jnp.float32),
            pltpu.VMEM((rows, slots, group * slots), jnp.bfloat16),
            pltpu.VMEM((ROUNDS, channels, slots), jnp.bfloat16),
            pltpu.VMEM((ROUNDS, devices, channels, slots), jnp.bfloat16),
            pltpu.VMEM((size_x * size_y, channels, slots), jnp.float32),
            pltpu.SMEM(class_shift.shape, jnp.float32),
            pltpu.VMEM((1, 1), jnp.int32),
            pltpu.VMEM((1, slots), jnp.int32),
            pltpu.VMEM(panel_geometry.shape, jnp.float32),
            pltpu.SemaphoreType.REGULAR((max(1, len(known_stages(rows))),)),
            pltpu.SemaphoreType.DMA((7,)),
            pltpu.SemaphoreType.DMA((1,)),
            pltpu.SemaphoreType.DMA((4 * sum(sides) + crossed,)),
            pltpu.SemaphoreType.DMA((1,)),
            pltpu.SemaphoreType.DMA((1,)),
            pltpu.SemaphoreType.DMA((ROUNDS, rows)),
        ],
        compiler_params=pltpu.CompilerParams(
            collective_id=0, has_side_effects=True, vmem_limit_bytes=grant
        ),
    )(*operands)
    return pl.pallas_call(
        place,
        out_shape=(
            jax.ShapeDtypeStruct(initial_field.shape, jnp.float32),
            jax.ShapeDtypeStruct((channels, slots), jnp.float32),
        ),
        in_specs=[vmem] * 2,
        out_specs=(hbm, hbm),
        scratch_shapes=[pltpu.SemaphoreType.DMA((2,))],
        compiler_params=pltpu.CompilerParams(vmem_limit_bytes=8 * math.prod(brick)),
    )(field, potential)


def solution(mesh):
    placed = (
        P(None, "row", "col", "gz"),
        P(None, "row", "col", "gz"),
        P("row", "col", "gz"),
        P(),
        P(("row", "col", "gz")),
        P(("row", "col", "gz")),
        P(None, ("row", "col", "gz")),
    )
    return jax.shard_map(
        functools.partial(local, tuple(mesh.shape[axis] for axis in AXES)),
        mesh=mesh,
        in_specs=placed,
        out_specs=(P(None, "row", "col", "gz"), P(None, ("row", "col", "gz"))),
        check_vma=False,
    )
```

```python
import functools
import math

import jax
import jax.numpy as jnp
import numpy as np
from jax import lax
from jax.experimental import pallas as pl
from jax.experimental.pallas import tpu as pltpu
from jax.sharding import PartitionSpec as P

ROUNDS = 2

relax_weight = 0.8
wave_number = 25.0
soften = 0.05
coupling = 0.5

MESH = pl.DeviceIdType.MESH
AXES = ("row", "col", "gz")


def cosine_terms(degree=6):
    nodes = 0.125 * (1.0 + np.cos(np.pi * (np.arange(64) + 0.5) / 64))
    fitted = np.polynomial.Polynomial.fit(
        nodes, np.cos(2 * np.pi * np.sqrt(nodes)), degree, domain=[0.0, 0.25]
    )
    return [float(c) for c in fitted.convert().coef]


COSINE = cosine_terms()


def cosine_of_turns(turns):
    fraction = turns - jnp.floor(turns + 0.5)
    square = fraction * fraction
    value = jnp.full_like(square, COSINE[-1])
    for term in reversed(COSINE[:-1]):
        value = value * square + term
    return value


def known_stages(rows):
    stages, reach = [], max(1, rows // 4)
    while reach < rows - 1:
        stages.append(reach)
        reach *= 2
    return stages


def kernel(
    sizes,
    init_hbm, source_hbm, class_hbm, shift_hbm, cell_hbm, live_hbm, geo_hbm,
    field_ref, potential_ref,
    init_v, source_v, forcing_v, class_v, weight_v, state_v,
    x_out, x_in, y_out, y_in, z_out, z_in, xy_in, xz_in, yz_in,
    wx_out, wx_in, wy_out, wy_in, wz_out, wz_in, rim_x, rim_y, rim_z,
    rim_wx, rim_wy, rim_wz, meter,
    geo_all, column_v, tile_v, density_out, density_all, at_cell,
    shift_ref, live_ref, cell_ref, geo_ref,
    known, local_sem, face_send, face_recv, gather_send, geo_recv, density_recv,
):
    rows, cols, depths = sizes
    devices = rows * cols * depths
    group = cols * depths
    channels, size_x, size_y, size_z = init_hbm.shape
    slots = cell_hbm.shape[1]
    classes = shift_ref.shape[0]
    factor = 1.0 / math.sqrt(slots * devices)
    here = tuple(lax.axis_index(axis) for axis in AXES)
    me = (here[0] * cols + here[1]) * depths + here[2]

    def brick_copies(hbm, vmem, sem):
        return [
            pltpu.make_async_copy(hbm.at[e], vmem.at[:, :, e, :], sem) for e in range(channels)
        ]

    def brick_wait(vmem, sem):
        pltpu.make_async_copy(vmem, vmem, sem).wait()

    for copy in brick_copies(init_hbm, init_v, local_sem.at[0]):
        copy.start()

    reach = max(1, rows // 4)
    barrier = pltpu.get_barrier_semaphore()

    def greet(row, first):
        for b in range(cols):
            for c in range(depths):
                if first and b == 0 and c == 0:
                    continue
                pl.semaphore_signal(
                    barrier, inc=1, device_id_type=MESH,
                    device_id=(row, lax.rem(here[1] + b, cols), lax.rem(here[2] + c, depths)),
                )

    greet(here[0], True)
    for away in range(1, reach + 1):
        pl.when(here[0] >= away)(lambda: greet(here[0] - away, False))
        pl.when(here[0] + away < rows)(lambda: greet(here[0] + away, False))
    near_low = jnp.where(here[0] > reach, here[0] - reach, 0)
    near_high = jnp.where(here[0] + reach < rows, here[0] + reach, rows - 1)
    near = (near_high - near_low + 1) * group - 1

    stages = known_stages(rows)

    def pass_on(stage):
        d = stages[stage]

        def tell(row):
            pl.semaphore_signal(
                known.at[stage], inc=1, device_id={"row": row}, device_id_type=MESH
            )

        pl.when((here[0] >= d) & (here[0] < rows - 1))(lambda: tell(here[0] - d))
        pl.when((here[0] + d < rows) & (here[0] > 0))(lambda: tell(here[0] + d))

    def hear(stage):
        d = stages[stage]
        told = jnp.where(here[0] + d < rows - 1, 1, 0) + jnp.where(here[0] > d, 1, 0)
        pl.when(told > 0)(lambda: pl.semaphore_wait(known.at[stage], told))

    copies = [
        pltpu.make_async_copy(class_hbm, class_v, local_sem.at[1]),
        pltpu.make_async_copy(geo_hbm, geo_ref, local_sem.at[3]),
        pltpu.make_async_copy(shift_hbm, shift_ref, local_sem.at[4]),
        pltpu.make_async_copy(cell_hbm, cell_ref, local_sem.at[5]),
        pltpu.make_async_copy(live_hbm, live_ref, local_sem.at[6]),
    ]

    def nth(k):
        below, above = here[0], rows - 1 - here[0]
        near = here[0] + jnp.where(lax.rem(k, 2) == 1, (k + 1) // 2, -(k // 2))
        far = jnp.where(below < above, k, rows - 1 - k)
        return jnp.where((k <= 2 * below) & (k <= 2 * above), near, far)

    def each_other(action):
        def at(row, first):
            for b in reversed(range(cols)):
                for c in reversed(range(depths)):
                    if first and b == 0 and c == 0:
                        continue
                    action((row, lax.rem(here[1] + b, cols), lax.rem(here[2] + c, depths)))

        def others(i, carry):
            at(nth(rows - 1 - i), False)
            return carry

        lax.fori_loop(0, rows - 1, others, 0)
        at(here[0], True)

    for copy in copies:
        copy.start()
    for copy in brick_copies(source_hbm, source_v, local_sem.at[2]):
        copy.start()

    cell_shape, pair_shape = (channels, size_z), (2 * channels, size_z)
    pairs = size_y // 2
    lane = lax.broadcasted_iota(jnp.int32, pair_shape, 1)
    even = (lane & 1) == 0
    at_pair = lane >> 1
    in_line = lax.rem(at_pair, pairs)
    upper = lax.broadcasted_iota(jnp.int32, pair_shape, 0) < channels
    low_plane = at_pair < pairs
    high_plane = (at_pair >= (size_x - 1) * pairs) & (at_pair < size_x * pairs)
    edge = jnp.where((lane == 0) | (lane == size_z - 1), 1.0, 0.0).astype(jnp.bfloat16)
    slab = (size_y * channels, size_z)
    slab_lane = lax.broadcasted_iota(jnp.int32, slab, 1)

    def turn(value, shift):
        return pltpu.roll(value, shift % size_z, 1)

    def swap(value):
        return jnp.concatenate([value[channels:], value[:channels]], axis=0)

    def planes(ref):
        return [[ref[x, y] for y in range(size_y)] for x in range(size_x)]

    def in_pairs(values):
        return [
            [
                jnp.concatenate([line[y], line[y + 1]], axis=0).astype(jnp.bfloat16)
                for y in range(0, size_y, 2)
            ]
            for line in values
        ]

    def pack_deep(paired):
        packed = jnp.zeros(pair_shape, jnp.bfloat16)
        for x in range(size_x):
            for p in range(pairs):
                packed = packed + turn(paired[x][p] * edge, 2 * (x * pairs + p) + 1)
        return packed

    def pack(q, values):
        paired = in_pairs(values)
        for side, x in ((0, 0), (1, size_x - 1)):
            for p in range(pairs):
                x_out[q, side, p] = paired[x][p]
        for side, y in ((0, 0), (1, size_y - 1)):
            for x in range(0, size_x, 2):
                both = jnp.concatenate([values[x][y], values[x + 1][y]], axis=0)
                y_out[q, side, x // 2] = both.astype(y_out.dtype)
        z_out[q] = pack_deep(paired)

    def exists(axis, up):
        return here[axis] < sizes[axis] - 1 if up else here[axis] > 0

    beside = []
    for axis in range(3):
        if sizes[axis] == 2:
            beside.append((axis, 1 - here[axis], 1 - here[axis], None))
        elif sizes[axis] > 2:
            beside.append((axis, 0, here[axis] - 1, exists(axis, 0)))
            beside.append((axis, 1, here[axis] + 1, exists(axis, 1)))
    edges_beside = [(one, two) for one in beside for two in beside if one[0] < two[0]]
    outs, ins = (x_out, y_out, z_out), (x_in, y_in, z_in)
    edge_ins = {(0, 1): xy_in, (0, 2): xz_in, (1, 2): yz_in}

    def when(present, action):
        if present is None:
            action()
        else:
            pl.when(present)(action)

    def start(source, landing, sem, target, present):
        def go():
            pltpu.make_async_remote_copy(
                src_ref=source,
                dst_ref=landing,
                send_sem=face_send.at[0],
                recv_sem=face_recv.at[sem],
                device_id=target,
                device_id_type=MESH,
            ).start()

        when(present, go)

    def start_faces(q):
        for axis, side, place, present in beside:
            source = outs[axis].at[q] if axis == 2 else outs[axis].at[q, side]
            start(source, ins[axis].at[q, 1 - side], q % 3, {AXES[axis]: place}, present)

    def start_edges(q):
        for (a, side_a, place_a, one), (b, side_b, place_b, two) in edges_beside:
            if (a, b) == (0, 1):
                source = y_out.at[q, side_b, side_a * ((size_x - 1) // 2)]
            else:
                source = z_out.at[q]
            landing = edge_ins[a, b].at[q // 3, 1 - side_a, 1 - side_b]
            present = two if one is None else one if two is None else one & two
            start(source, landing, 3, {AXES[a]: place_a, AXES[b]: place_b}, present)

    def start_weights():
        for axis, side, place, present in beside:
            out, into = ((wx_out, wx_in), (wy_out, wy_in), (wz_out, wz_in))[axis]
            source = out if axis == 2 else out.at[side]
            start(source, into.at[1 - side], 4, {AXES[axis]: place}, present)

    def await_bytes(sem, each):
        split = [axis for axis in range(3) if sizes[axis] > 2]
        for case in range(2 ** len(split)):
            counts = [min(count, 2) - 1 for count in sizes]
            condition = None
            for i, axis in enumerate(split):
                both = (case >> i) & 1
                counts[axis] += both
                holds = (here[axis] > 0) & (here[axis] < sizes[axis] - 1)
                holds = holds if both else jnp.logical_not(holds)
                condition = holds if condition is None else condition & holds
            span = meter.at[pl.ds(0, each(counts))]
            when(condition, lambda span=span: pltpu.make_async_copy(span, span, sem).wait())

    def face_cells(n):
        return n[0] * pairs + n[1] * (size_x // 2) + n[2]

    def edge_cells(n):
        return n[0] * n[1] + n[0] * n[2] + n[1] * n[2]

    def weight_cells(n):
        return n[0] * (size_y // channels) + n[1] + n[2]

    none = 3 * ROUNDS
    x_in[none] = jnp.zeros(x_in.shape[1:], x_in.dtype)
    y_in[none] = jnp.zeros(y_in.shape[1:], y_in.dtype)
    z_in[none] = jnp.zeros(z_in.shape[1:], z_in.dtype)
    for into in edge_ins.values():
        into[ROUNDS] = jnp.zeros(into.shape[1:], into.dtype)
    wx_in[2] = jnp.zeros(wx_in.shape[1:], wx_in.dtype)
    wy_in[2] = jnp.zeros(wy_in.shape[1:], wy_in.dtype)
    wz_in[2] = jnp.zeros(wz_in.shape[1:], wz_in.dtype)

    with jax.named_scope("w_init"):
        brick_wait(init_v, local_sem.at[0])

    pack(0, planes(init_v))

    with jax.named_scope("w_barrier"):
        pl.semaphore_wait(barrier, near)
    if stages:
        pass_on(0)
    start_faces(0)

    copies[1].wait()
    eye = lax.broadcasted_iota(jnp.int32, (slots, slots), 0) == lax.broadcasted_iota(
        jnp.int32, (slots, slots), 1
    )
    for i in range(3):
        column = jnp.sum(jnp.where(eye, geo_ref[i : i + 1, :], 0.0), axis=1, keepdims=True)
        column_v[i] = jnp.broadcast_to(column, (slots, slots))
    pltpu.make_async_copy(geo_ref, geo_all.at[me], geo_recv.at[here[0]]).start()


    def start_gather(source, gathered, sem):
        def send(device):
            pltpu.make_async_remote_copy(
                src_ref=source,
                dst_ref=gathered.at[me],
                send_sem=gather_send.at[0],
                recv_sem=sem,
                device_id=device,
                device_id_type=MESH,
            ).start()

        each_other(send)

    def await_gather(gathered, count, sem):
        whole = gathered.at[pl.ds(0, count)]
        pltpu.make_async_copy(whole, whole, sem).wait()

    copies[0].wait()
    copies[2].wait()
    for x in range(size_x):
        kind = class_v[x]
        shift = jnp.zeros(kind.shape, jnp.float32)
        for level in range(classes):
            shift = jnp.where(kind == level, shift_ref[level], shift)
        weight = relax_weight / (6.0 + shift)
        weight_v[x] = jnp.broadcast_to(weight[:, None, :], (size_y, channels, size_z))
        if x == 0:
            wx_out[0] = weight
        if x == size_x - 1:
            wx_out[1] = weight
        if x == 0:
            wy_out[...] = jnp.zeros(wy_out.shape, wy_out.dtype)
        wy_out[0, x : x + 1, :] = weight[0:1]
        wy_out[1, x : x + 1, :] = weight[size_y - 1 : size_y]
    wz_out[...] = pack_deep(in_pairs(planes(weight_v)))
    start_weights()

    copies[3].wait()
    copies[4].wait()
    cell = cell_ref[...]
    bits = size_z.bit_length() - 1
    cell_z = cell & (size_z - 1)
    cell_xy = cell >> bits
    pick_z = lax.broadcasted_iota(jnp.int32, (size_z, slots), 0) == cell_z
    pick_z = jnp.where(pick_z, 1.0, 0.0).astype(jnp.bfloat16)
    for at in range(size_x * size_y):
        at_cell[at] = jnp.broadcast_to(
            jnp.where(cell_xy == at, 1.0, 0.0), (channels, slots)
        )
    live = lax.broadcasted_iota(jnp.int32, (channels, slots), 1) < live_ref[...]
    brick_wait(source_v, local_sem.at[2])
    for x in range(size_x):
        forcing_v[0, x] = weight_v[x] * source_v[x]

    def inside(value, above, below):
        blank = jnp.zeros((1,) + cell_shape, jnp.float32)
        around = jnp.concatenate([value[1:], blank], axis=0)
        around = around + jnp.concatenate([blank, value[:-1]], axis=0)
        for other in (above, below):
            if other is not None:
                around = around + other
        flat = value.reshape(slab)
        beside = jnp.where(slab_lane == size_z - 1, 0.0, turn(flat, size_z - 1))
        beside = beside + jnp.where(slab_lane == 0, 0.0, turn(flat, 1))
        return around + beside.reshape(value.shape)

    def ends(beyond, at):
        both = (turn(beyond, -2 * at) * edge).astype(jnp.float32)
        return both[:channels], both[channels:]

    def inner(source, target, force):
        for x in range(size_x):
            value = source[x]
            around = inside(
                value,
                source[x + 1] if x + 1 < size_x else None,
                source[x - 1] if x > 0 else None,
            )
            target[x] = (1.0 - relax_weight) * value + force[x] + weight_v[x] * around

    def pick(axis, q):
        return (
            jnp.where(here[axis] > 0, q, none),
            jnp.where(here[axis] < sizes[axis] - 1, q, none),
        )

    def half_of_pair(i):
        return slice(channels * (i % 2), channels * (i % 2) + channels)

    def from_x(q, side, y):
        both = x_in[pick(0, q)[side], side, y // 2].astype(jnp.float32)
        return both[half_of_pair(y)]

    def from_y(q, side, x):
        both = y_in[pick(1, q)[side], side, x // 2].astype(jnp.float32)
        return both[half_of_pair(x)]

    def either(low, high):
        return jnp.where(even, low.astype(jnp.float32), high.astype(jnp.float32))

    def from_z(q):
        below, above = pick(2, q)
        return either(z_in[below, 0], z_in[above, 1])

    def beside_ends(natural):
        return jnp.where(even, natural, turn(natural, -2)).astype(jnp.bfloat16)

    def corner(a, b, q, side_a, side_b):
        there = exists(a, side_a) & exists(b, side_b)
        return edge_ins[a, b][jnp.where(there, q // 3, ROUNDS), side_a, side_b]

    def corner_xy(q, side_x, side_y):
        both = corner(0, 1, q, side_x, side_y).astype(jnp.float32)
        return both[half_of_pair(size_x - 1 if side_x == 0 else 0)]

    def corner_z(axis, q, side):
        return either(corner(axis, 2, q, side, 0), corner(axis, 2, q, side, 1))

    def outer(target, q):
        beyond = beside_ends(from_z(q))
        for x in range(size_x):
            for p in range(pairs):
                for y, around in zip((2 * p, 2 * p + 1), ends(beyond, x * pairs + p)):
                    if x == 0:
                        around = around + from_x(q, 0, y)
                    if x == size_x - 1:
                        around = around + from_x(q, 1, y)
                    if y == 0:
                        around = around + from_y(q, 0, x)
                    if y == size_y - 1:
                        around = around + from_y(q, 1, x)
                    target[x, y] = target[x, y] + weight_v[x, y] * around

    def spread_weights():
        for side in (0, 1):
            weight = wx_in[jnp.where(exists(0, side), side, 2)]
            rim_wx[side] = jnp.broadcast_to(weight[:, None, :], (size_y,) + cell_shape)
            weight = wy_in[jnp.where(exists(1, side), side, 2)][:size_x]
            rim_wy[side] = jnp.broadcast_to(weight[:, None, :], (size_x,) + cell_shape)
        rim_wz[...] = either(
            wz_in[jnp.where(exists(2, 0), 0, 2)], wz_in[jnp.where(exists(2, 1), 1, 2)]
        )

    def own_rim(source, q):
        for side in (0, 1):
            rim_x[side] = rim_wx[side] * source[(size_x - 1) * side]
            for x in range(size_x):
                rim_y[side, x] = rim_wy[side, x] * source[x, (size_y - 1) * side]
        own = z_out[q].astype(jnp.float32)
        rim_z[...] = rim_wz[...] * jnp.where(even, turn(own, -1), turn(own, 1))

    def rim(target, q):
        along, across = (size_x - 1) * size_y, 2 * (pairs - 1)
        around = jnp.where(low_plane, turn(corner_z(0, q, 0), -along), 0.0)
        around = around + jnp.where(high_plane, turn(corner_z(0, q, 1), along), 0.0)
        first = upper & (in_line == 0)
        final = jnp.logical_not(upper) & (in_line == pairs - 1)
        around = around + jnp.where(first, swap(turn(corner_z(1, q, 0), -across)), 0.0)
        around = around + jnp.where(final, swap(turn(corner_z(1, q, 1), across)), 0.0)
        beyond = beside_ends(rim_z[...] + rim_wz[...] * around + from_z(q + 1))
        beyond_x = [beside_ends(corner_z(0, q, side)) for side in (0, 1)]
        beyond_y = [beside_ends(corner_z(1, q, side)) for side in (0, 1)]

        def swept_x(side, p):
            found = []
            theirs = (size_x - 1) * (1 - side)
            for y, around in zip((2 * p, 2 * p + 1), ends(beyond_x[side], theirs * pairs + p)):
                if y == 0:
                    around = around + corner_xy(q, side, 0)
                if y == size_y - 1:
                    around = around + corner_xy(q, side, 1)
                found.append(rim_x[side, y] + from_x(q + 1, side, y) + rim_wx[side, y] * around)
            return found

        def swept_y(side, x):
            theirs = (size_y - 1) * (1 - side)
            around = ends(beyond_y[side], x * pairs + theirs // 2)[theirs % 2]
            if x == 0:
                around = around + corner_xy(q, 0, side)
            if x == size_x - 1:
                around = around + corner_xy(q, 1, side)
            return rim_y[side, x] + from_y(q + 1, side, x) + rim_wy[side, x] * around

        for x in range(size_x):
            for p in range(pairs):
                below = swept_x(0, p) if x == 0 else None
                above = swept_x(1, p) if x == size_x - 1 else None
                for i, around in enumerate(ends(beyond, x * pairs + p)):
                    y = 2 * p + i
                    if below:
                        around = around + below[i]
                    if above:
                        around = around + above[i]
                    if y == 0:
                        around = around + swept_y(0, x)
                    if y == size_y - 1:
                        around = around + swept_y(1, x)
                    target[x, y] = target[x, y] + weight_v[x, y] * around

    pieces = 4
    chunk = slots // pieces

    def make_tiles():
        def body(k, carry):
            q = nth(k)
            await_gather(geo_all, group, geo_recv.at[q])
            for j in range(group):
                source = geo_all[q * group + j]
                for piece in range(pieces):
                    span = slice(piece * chunk, (piece + 1) * chunk)
                    delta_x = column_v[0, span, :] - source[0:1, :]
                    delta_y = column_v[1, span, :] - source[1:2, :]
                    delta_z = column_v[2, span, :] - source[2:3, :]
                    square = delta_x * delta_x + delta_y * delta_y + delta_z * delta_z + 1e-30
                    distance = square * lax.rsqrt(square)
                    wave = cosine_of_turns(distance * (wave_number / (2.0 * math.pi)))
                    value = (source[3:4, :] * factor) * wave / (distance + soften)
                    tile_v[q, span, j * slots : (j + 1) * slots] = value.astype(tile_v.dtype)
            return carry

        lax.fori_loop(0, rows, body, 0)

    def apply_tiles(r):
        total = jnp.zeros((channels, slots), jnp.float32)
        for k in range(rows):
            q = nth(k)
            with jax.named_scope(f"w_dens{r}_{k}"):
                await_gather(density_all.at[r], group - (k == 0), density_recv.at[r, q])
            values = jnp.concatenate(
                [density_all[r, q * group + j] for j in range(group)], axis=1
            )
            total = total + lax.dot_general(
                values, tile_v[q], (((1,), (1,)), ((), ())), preferred_element_type=jnp.float32
            )
        return total

    def land(sem, each):
        await_bytes(face_recv.at[sem], each)

    def drain(each):
        await_bytes(face_send.at[0], each)

    def drain_now():
        for q in range(3 * ROUNDS - 2):
            drain(face_cells)
            if q % 3 == 1:
                drain(edge_cells)
        drain(weight_cells)
        await_gather(geo_all, devices - 1, gather_send.at[0])
        for r in range(ROUNDS - 1):
            await_gather(density_all.at[r], devices - 1, gather_send.at[0])

    for r in range(ROUNDS):
        single, double = 3 * r, 3 * r + 1
        before = init_v if r == 0 else state_v.at[2]
        once, mid, after = state_v.at[0], state_v.at[1], state_v.at[2]
        if r == ROUNDS - 1:
            after = field_ref
        force = forcing_v.at[r]
        with jax.named_scope(f"inner{r}"):
            inner(before, once, forcing_v.at[0])
        if r > 0:
            with jax.named_scope("tilesB"):
                make_tiles()
        if r == 0:
            with jax.named_scope("w_known0"):
                for stage in range(len(stages) - 1):
                    hear(stage)
                    pass_on(stage + 1)
        with jax.named_scope(f"w_single{r}"):
            land(0, face_cells)
        with jax.named_scope(f"outer{r}"):
            outer(once, single)
        if r > 0:
            with jax.named_scope(f"apply{r-1}"):
                potential = jnp.where(live, apply_tiles(r - 1), 0.0)
            with jax.named_scope(f"load{r}"):
                half_of = coupling * potential
                big = half_of.astype(jnp.bfloat16).astype(jnp.float32)
                small = half_of - big
                load = jnp.zeros((size_x * size_y * channels, size_z), jnp.float32)
                for part in (big, small):
                    placed = (at_cell[...] * part[None]).astype(jnp.bfloat16)
                    load = load + lax.dot_general(
                        placed.reshape(size_x * size_y * channels, slots), pick_z,
                        (((1,), (1,)), ((), ())), preferred_element_type=jnp.float32,
                    )
                load = load.reshape(size_x, size_y, channels, size_z)
                for x in range(size_x):
                    change = weight_v[x] * load[x]
                    force[x] = forcing_v[0, x] + change
                    once[x] = once[x] + change
        with jax.named_scope(f"pack{r}"):
            pack(double, planes(once))
        start_edges(double)
        start_faces(double)
        with jax.named_scope(f"innerd{r}"):
            inner(once, mid, force)
        with jax.named_scope(f"packd{r}"):
            pack(double + 1, planes(mid))
        start_faces(double + 1)
        if r == 0:
            with jax.named_scope("w_weights"):
                land(4, weight_cells)
                spread_weights()
            with jax.named_scope("w_known"):
                if stages:
                    hear(len(stages) - 1)
            with jax.named_scope("st_geo"):
                start_gather(geo_ref, geo_all, geo_recv.at[here[0]])
        else:
            drain_now()
        own_rim(once, double)
        with jax.named_scope(f"w_double{r}"):
            land(1, face_cells)
        with jax.named_scope(f"outerd{r}"):
            outer(mid, double)
            inner(mid, after, force)
        with jax.named_scope(f"w_edges{r}"):
            land(3, edge_cells)
        with jax.named_scope(f"w_rim{r}"):
            land(2, face_cells)
        with jax.named_scope(f"rim{r}"):
            rim(after, double)
        with jax.named_scope(f"density{r}"):
            flat = after[...].reshape(size_x * size_y * channels, size_z).astype(jnp.bfloat16)
            picked = jnp.dot(flat, pick_z, preferred_element_type=jnp.float32)
            picked = picked.reshape(size_x * size_y, channels, slots)
            density = jnp.sum(picked * at_cell[...], axis=0)
            density = jnp.where(live, density, 0.0).astype(jnp.bfloat16)
            density_out[r] = density
            density_all[r, me] = density
        with jax.named_scope(f"st_dens{r}"):
            start_gather(density_out.at[r], density_all.at[r], density_recv.at[r, here[0]])
        if r < ROUNDS - 1:
            with jax.named_scope(f"pack_s{r}"):
                pack(single + 3, planes(after))
            start_faces(single + 3)
    drain(face_cells)
    drain(edge_cells)
    drain(face_cells)
    with jax.named_scope(f"apply{ROUNDS-1}"):
        potential_ref[...] = jnp.where(live, apply_tiles(ROUNDS - 1), 0.0)

    with jax.named_scope("finish"):
        await_gather(density_all.at[ROUNDS - 1], devices - 1, gather_send.at[0])


def place(field_v, potential_v, field_hbm, potential_hbm, sem):
    channels = field_hbm.shape[0]
    copies = [
        pltpu.make_async_copy(field_v.at[:, :, e, :], field_hbm.at[e], sem.at[0])
        for e in range(channels)
    ]
    copies.append(pltpu.make_async_copy(potential_v, potential_hbm, sem.at[1]))
    for copy in copies:
        copy.start()
    pltpu.make_async_copy(field_v, field_v, sem.at[0]).wait()
    copies[-1].wait()


def local(sizes, initial_field, source_term, cell_class, class_shift, surface_cell, live_count,
          panel_geometry):
    channels, size_x, size_y, size_z = initial_field.shape
    slots = surface_cell.shape[0]
    rows, cols, depths = sizes
    devices, group = rows * cols * depths, cols * depths
    brick = (size_x, size_y, channels, size_z)
    vmem = pl.BlockSpec(memory_space=pltpu.VMEM)
    hbm = pl.BlockSpec(memory_space=pltpu.HBM)
    per_device = slots * (2 * slots + 4 * 8 + ROUNDS * 2 * 2 * channels)
    grant = devices * per_device + 36 * 4 * math.prod(brick)
    operands = [
        pltpu.with_memory_space_constraint(array, pltpu.HBM)
        for array in (
            initial_field, source_term, cell_class, class_shift,
            surface_cell.reshape(1, slots), panel_geometry,
        )
    ]
    operands.insert(5, live_count.reshape(1, 1))
    two, turns = 2 * channels, 3 * ROUNDS
    field, potential = pl.pallas_call(
        functools.partial(kernel, sizes),
        out_shape=(
            jax.ShapeDtypeStruct(brick, jnp.float32),
            jax.ShapeDtypeStruct((channels, slots), jnp.float32),
        ),
        in_specs=[hbm] * 5 + [pl.BlockSpec(memory_space=pl.ANY), hbm],
        out_specs=(vmem, vmem),
        scratch_shapes=[
            pltpu.VMEM(brick, jnp.float32),
            pltpu.VMEM(brick, jnp.float32),
            pltpu.VMEM((ROUNDS,) + brick, jnp.float32),
            pltpu.VMEM((size_x, size_y, size_z), jnp.int32),
            pltpu.VMEM(brick, jnp.float32),
            pltpu.VMEM((3,) + brick, jnp.float32),
            pltpu.VMEM((turns, 2, size_y // 2, two, size_z), jnp.bfloat16),
            pltpu.VMEM((turns + 1, 2, size_y // 2, two, size_z), jnp.bfloat16),
            pltpu.VMEM((turns, 2, size_x // 2, two, size_z), jnp.bfloat16),
            pltpu.VMEM((turns + 1, 2, size_x // 2, two, size_z), jnp.bfloat16),
            pltpu.VMEM((turns, two, size_z), jnp.bfloat16),
            pltpu.VMEM((turns + 1, 2, two, size_z), jnp.bfloat16),
            pltpu.VMEM((ROUNDS + 1, 2, 2, two, size_z), jnp.bfloat16),
            pltpu.VMEM((ROUNDS + 1, 2, 2, two, size_z), jnp.bfloat16),
            pltpu.VMEM((ROUNDS + 1, 2, 2, two, size_z), jnp.bfloat16),
            pltpu.VMEM((2, size_y, size_z), jnp.float32),
            pltpu.VMEM((3, size_y, size_z), jnp.float32),
            pltpu.VMEM((2, channels, size_z), jnp.float32),
            pltpu.VMEM((3, channels, size_z), jnp.float32),
            pltpu.VMEM((two, size_z), jnp.bfloat16),
            pltpu.VMEM((3, two, size_z), jnp.bfloat16),
            pltpu.VMEM((2, size_y, channels, size_z), jnp.float32),
            pltpu.VMEM((2, size_x, channels, size_z), jnp.float32),
            pltpu.VMEM((two, size_z), jnp.float32),
            pltpu.VMEM((2, size_y, channels, size_z), jnp.float32),
            pltpu.VMEM((2, size_x, channels, size_z), jnp.float32),
            pltpu.VMEM((two, size_z), jnp.float32),
            pltpu.VMEM((size_y + size_x + 2, channels, size_z), jnp.float32),
            pltpu.VMEM((devices, 4, slots), jnp.float32),
            pltpu.VMEM((3, slots, slots), jnp.float32),
            pltpu.VMEM((rows, slots, group * slots), jnp.bfloat16),
            pltpu.VMEM((ROUNDS, channels, slots), jnp.bfloat16),
            pltpu.VMEM((ROUNDS, devices, channels, slots), jnp.bfloat16),
            pltpu.VMEM((size_x * size_y, channels, slots), jnp.float32),
            pltpu.SMEM(class_shift.shape, jnp.float32),
            pltpu.VMEM((1, 1), jnp.int32),
            pltpu.VMEM((1, slots), jnp.int32),
            pltpu.VMEM(panel_geometry.shape, jnp.float32),
            pltpu.SemaphoreType.REGULAR((max(1, len(known_stages(rows))),)),
            pltpu.SemaphoreType.DMA((7,)),
            pltpu.SemaphoreType.DMA((1,)),
            pltpu.SemaphoreType.DMA((5,)),
            pltpu.SemaphoreType.DMA((1,)),
            pltpu.SemaphoreType.DMA((rows,)),
            pltpu.SemaphoreType.DMA((ROUNDS, rows)),
        ],
        compiler_params=pltpu.CompilerParams(
            collective_id=0, has_side_effects=True, vmem_limit_bytes=grant
        ),
    )(*operands)
    return pl.pallas_call(
        place,
        out_shape=(
            jax.ShapeDtypeStruct(initial_field.shape, jnp.float32),
            jax.ShapeDtypeStruct((channels, slots), jnp.float32),
        ),
        in_specs=[vmem] * 2,
        out_specs=(hbm, hbm),
        scratch_shapes=[pltpu.SemaphoreType.DMA((2,))],
        compiler_params=pltpu.CompilerParams(vmem_limit_bytes=8 * math.prod(brick)),
    )(field, potential)


def solution(mesh):
    placed = (
        P(None, "row", "col", "gz"),
        P(None, "row", "col", "gz"),
        P("row", "col", "gz"),
        P(),
        P(("row", "col", "gz")),
        P(("row", "col", "gz")),
        P(None, ("row", "col", "gz")),
    )
    return jax.shard_map(
        functools.partial(local, tuple(mesh.shape[axis] for axis in AXES)),
        mesh=mesh,
        in_specs=placed,
        out_specs=(P(None, "row", "col", "gz"), P(None, ("row", "col", "gz"))),
        check_vma=False,
    )
```

```python
import functools
import math

import jax
import jax.numpy as jnp
import numpy as np
from jax import lax
from jax.experimental import pallas as pl
from jax.experimental.pallas import tpu as pltpu
from jax.sharding import PartitionSpec as P

ROUNDS = 2

relax_weight = 0.8
wave_number = 25.0
soften = 0.05
coupling = 0.5

MESH = pl.DeviceIdType.MESH
AXES = ("row", "col", "gz")


def cosine_terms(degree=6):
    nodes = 0.125 * (1.0 + np.cos(np.pi * (np.arange(64) + 0.5) / 64))
    fitted = np.polynomial.Polynomial.fit(
        nodes, np.cos(2 * np.pi * np.sqrt(nodes)), degree, domain=[0.0, 0.25]
    )
    return [float(c) for c in fitted.convert().coef]


COSINE = cosine_terms()


def cosine_of_turns(turns):
    fraction = turns - jnp.floor(turns + 0.5)
    square = fraction * fraction
    value = jnp.full_like(square, COSINE[-1])
    for term in reversed(COSINE[:-1]):
        value = value * square + term
    return value


def known_stages(rows):
    stages, reach = [], max(1, rows // 8)
    while reach < rows - 1:
        stages.append(reach)
        reach *= 2
    return stages


def kernel(
    sizes,
    init_hbm, source_hbm, class_hbm, shift_hbm, cell_hbm, live_hbm, geo_hbm,
    field_ref, potential_ref,
    init_v, source_v, forcing_v, class_v, weight_v, state_v,
    x_out, x_in, y_out, y_in, z_out, z_in, xy_in, xz_in, yz_in,
    wx_out, wx_in, wy_out, wy_in, wz_out, wz_in, rim_x, rim_y, rim_z,
    rim_wx, rim_wy, rim_wz, meter,
    geo_all, column_v, tile_v, density_out, density_all, at_cell,
    shift_ref, live_ref, cell_ref, geo_ref,
    known, local_sem, face_send, face_recv, gather_send, geo_recv, density_recv,
):
    rows, cols, depths = sizes
    devices = rows * cols * depths
    group = cols * depths
    channels, size_x, size_y, size_z = init_hbm.shape
    slots = cell_hbm.shape[1]
    classes = shift_ref.shape[0]
    factor = 1.0 / math.sqrt(slots * devices)
    here = tuple(lax.axis_index(axis) for axis in AXES)
    me = (here[0] * cols + here[1]) * depths + here[2]

    def brick_copies(hbm, vmem, sem):
        return [
            pltpu.make_async_copy(hbm.at[e], vmem.at[:, :, e, :], sem) for e in range(channels)
        ]

    def brick_wait(vmem, sem):
        pltpu.make_async_copy(vmem, vmem, sem).wait()

    for copy in brick_copies(init_hbm, init_v, local_sem.at[0]):
        copy.start()

    reach = max(1, rows // 8)
    barrier = pltpu.get_barrier_semaphore()

    def greet(row, first):
        for b in range(cols):
            for c in range(depths):
                if first and b == 0 and c == 0:
                    continue
                pl.semaphore_signal(
                    barrier, inc=1, device_id_type=MESH,
                    device_id=(row, lax.rem(here[1] + b, cols), lax.rem(here[2] + c, depths)),
                )

    greet(here[0], True)
    for away in range(1, reach + 1):
        pl.when(here[0] >= away)(lambda: greet(here[0] - away, False))
        pl.when(here[0] + away < rows)(lambda: greet(here[0] + away, False))
    near_low = jnp.where(here[0] > reach, here[0] - reach, 0)
    near_high = jnp.where(here[0] + reach < rows, here[0] + reach, rows - 1)
    near = (near_high - near_low + 1) * group - 1

    stages = known_stages(rows)

    def pass_on(stage):
        d = stages[stage]

        def tell(row):
            pl.semaphore_signal(
                known.at[stage], inc=1, device_id={"row": row}, device_id_type=MESH
            )

        pl.when((here[0] >= d) & (here[0] < rows - 1))(lambda: tell(here[0] - d))
        pl.when((here[0] + d < rows) & (here[0] > 0))(lambda: tell(here[0] + d))

    def hear(stage):
        d = stages[stage]
        told = jnp.where(here[0] + d < rows - 1, 1, 0) + jnp.where(here[0] > d, 1, 0)
        pl.when(told > 0)(lambda: pl.semaphore_wait(known.at[stage], told))

    copies = [
        pltpu.make_async_copy(class_hbm, class_v, local_sem.at[1]),
        pltpu.make_async_copy(geo_hbm, geo_ref, local_sem.at[3]),
        pltpu.make_async_copy(shift_hbm, shift_ref, local_sem.at[4]),
        pltpu.make_async_copy(cell_hbm, cell_ref, local_sem.at[5]),
        pltpu.make_async_copy(live_hbm, live_ref, local_sem.at[6]),
    ]

    def nearest(k, own, count):
        below, above = own, count - 1 - own
        near = own + jnp.where(lax.rem(k, 2) == 1, (k + 1) // 2, -(k // 2))
        far = jnp.where(below < above, k, count - 1 - k)
        return jnp.where((k <= 2 * below) & (k <= 2 * above), near, far)

    def nth(k):
        return nearest(k, here[0], rows)

    def each_other(action):
        def at(row, first):
            for b in reversed(range(cols)):
                for c in reversed(range(depths)):
                    if first and b == 0 and c == 0:
                        continue
                    action((row, lax.rem(here[1] + b, cols), lax.rem(here[2] + c, depths)))

        def others(i, carry):
            at(nth(rows - 1 - i), False)
            return carry

        lax.fori_loop(0, rows - 1, others, 0)
        at(here[0], True)

    for copy in copies:
        copy.start()
    for copy in brick_copies(source_hbm, source_v, local_sem.at[2]):
        copy.start()

    cell_shape, pair_shape = (channels, size_z), (2 * channels, size_z)
    pairs = size_y // 2
    lane = lax.broadcasted_iota(jnp.int32, pair_shape, 1)
    even = (lane & 1) == 0
    at_pair = lane >> 1
    in_line = lax.rem(at_pair, pairs)
    upper = lax.broadcasted_iota(jnp.int32, pair_shape, 0) < channels
    low_plane = at_pair < pairs
    high_plane = (at_pair >= (size_x - 1) * pairs) & (at_pair < size_x * pairs)
    edge = jnp.where((lane == 0) | (lane == size_z - 1), 1.0, 0.0).astype(jnp.bfloat16)
    slab = (size_y * channels, size_z)
    slab_lane = lax.broadcasted_iota(jnp.int32, slab, 1)

    def turn(value, shift):
        return pltpu.roll(value, shift % size_z, 1)

    def swap(value):
        return jnp.concatenate([value[channels:], value[:channels]], axis=0)

    def planes(ref):
        return [[ref[x, y] for y in range(size_y)] for x in range(size_x)]

    def in_pairs(values):
        return [
            [
                jnp.concatenate([line[y], line[y + 1]], axis=0).astype(jnp.bfloat16)
                for y in range(0, size_y, 2)
            ]
            for line in values
        ]

    def pack_deep(paired):
        packed = jnp.zeros(pair_shape, jnp.bfloat16)
        for x in range(size_x):
            for p in range(pairs):
                packed = packed + turn(paired[x][p] * edge, 2 * (x * pairs + p) + 1)
        return packed

    def pack(q, values):
        paired = in_pairs(values)
        for side, x in ((0, 0), (1, size_x - 1)):
            for p in range(pairs):
                x_out[q, side, p] = paired[x][p]
        for side, y in ((0, 0), (1, size_y - 1)):
            for x in range(0, size_x, 2):
                both = jnp.concatenate([values[x][y], values[x + 1][y]], axis=0)
                y_out[q, side, x // 2] = both.astype(y_out.dtype)
        z_out[q] = pack_deep(paired)

    def exists(axis, up):
        return here[axis] < sizes[axis] - 1 if up else here[axis] > 0

    beside = []
    for axis in range(3):
        if sizes[axis] == 2:
            beside.append((axis, 1 - here[axis], 1 - here[axis], None))
        elif sizes[axis] > 2:
            beside.append((axis, 0, here[axis] - 1, exists(axis, 0)))
            beside.append((axis, 1, here[axis] + 1, exists(axis, 1)))
    edges_beside = [(one, two) for one in beside for two in beside if one[0] < two[0]]
    outs, ins = (x_out, y_out, z_out), (x_in, y_in, z_in)
    edge_ins = {(0, 1): xy_in, (0, 2): xz_in, (1, 2): yz_in}

    def when(present, action):
        if present is None:
            action()
        else:
            pl.when(present)(action)

    def start(source, landing, sem, target, present):
        def go():
            pltpu.make_async_remote_copy(
                src_ref=source,
                dst_ref=landing,
                send_sem=face_send.at[0],
                recv_sem=face_recv.at[sem],
                device_id=target,
                device_id_type=MESH,
            ).start()

        when(present, go)

    def start_faces(q):
        for axis, side, place, present in beside:
            source = outs[axis].at[q] if axis == 2 else outs[axis].at[q, side]
            start(source, ins[axis].at[q, 1 - side], q % 3, {AXES[axis]: place}, present)

    def start_edges(q):
        for (a, side_a, place_a, one), (b, side_b, place_b, two) in edges_beside:
            if (a, b) == (0, 1):
                source = y_out.at[q, side_b, side_a * ((size_x - 1) // 2)]
            else:
                source = z_out.at[q]
            landing = edge_ins[a, b].at[q // 3, 1 - side_a, 1 - side_b]
            present = two if one is None else one if two is None else one & two
            start(source, landing, 3, {AXES[a]: place_a, AXES[b]: place_b}, present)

    def start_weights():
        for axis, side, place, present in beside:
            out, into = ((wx_out, wx_in), (wy_out, wy_in), (wz_out, wz_in))[axis]
            source = out if axis == 2 else out.at[side]
            start(source, into.at[1 - side], 4, {AXES[axis]: place}, present)

    def await_bytes(sem, each):
        split = [axis for axis in range(3) if sizes[axis] > 2]
        for case in range(2 ** len(split)):
            counts = [min(count, 2) - 1 for count in sizes]
            condition = None
            for i, axis in enumerate(split):
                both = (case >> i) & 1
                counts[axis] += both
                holds = (here[axis] > 0) & (here[axis] < sizes[axis] - 1)
                holds = holds if both else jnp.logical_not(holds)
                condition = holds if condition is None else condition & holds
            span = meter.at[pl.ds(0, each(counts))]
            when(condition, lambda span=span: pltpu.make_async_copy(span, span, sem).wait())

    def face_cells(n):
        return n[0] * pairs + n[1] * (size_x // 2) + n[2]

    def edge_cells(n):
        return n[0] * n[1] + n[0] * n[2] + n[1] * n[2]

    def weight_cells(n):
        return n[0] * (size_y // channels) + n[1] + n[2]

    none = 3 * ROUNDS
    x_in[none] = jnp.zeros(x_in.shape[1:], x_in.dtype)
    y_in[none] = jnp.zeros(y_in.shape[1:], y_in.dtype)
    z_in[none] = jnp.zeros(z_in.shape[1:], z_in.dtype)
    for into in edge_ins.values():
        into[ROUNDS] = jnp.zeros(into.shape[1:], into.dtype)
    wx_in[2] = jnp.zeros(wx_in.shape[1:], wx_in.dtype)
    wy_in[2] = jnp.zeros(wy_in.shape[1:], wy_in.dtype)
    wz_in[2] = jnp.zeros(wz_in.shape[1:], wz_in.dtype)

    with jax.named_scope("w_init"):
        brick_wait(init_v, local_sem.at[0])

    pack(0, planes(init_v))

    with jax.named_scope("w_barrier"):
        pl.semaphore_wait(barrier, near)
    if stages:
        pass_on(0)
    start_faces(0)

    copies[1].wait()
    eye = lax.broadcasted_iota(jnp.int32, (slots, slots), 0) == lax.broadcasted_iota(
        jnp.int32, (slots, slots), 1
    )
    for i in range(3):
        column = jnp.sum(jnp.where(eye, geo_ref[i : i + 1, :], 0.0), axis=1, keepdims=True)
        column_v[i] = jnp.broadcast_to(column, (slots, slots))
    pltpu.make_async_copy(geo_ref, geo_all.at[me], geo_recv.at[here[0]]).start()


    fold = 2 - rows % 2
    layers, layer, part = rows // fold, here[0] // fold, lax.rem(here[0], fold)

    def start_geometry(known_before, known_now):
        def to_row(row, first):
            for b in reversed(range(cols)):
                for c in reversed(range(depths)):
                    if first and b == 0 and c == 0:
                        continue
                    pltpu.make_async_remote_copy(
                        src_ref=geo_ref,
                        dst_ref=geo_all.at[me],
                        send_sem=gather_send.at[0],
                        recv_sem=geo_recv.at[here[0]],
                        device_id=(
                            row, lax.rem(here[1] + b, cols), lax.rem(here[2] + c, depths)
                        ),
                        device_id_type=MESH,
                    ).start()

        if known_before < 0:
            to_row(here[0], True)
        for away in range(max(0, known_before) // fold + 1, min(known_now // fold, layers - 1) + 1):
            away = away * fold
            pl.when(here[0] >= away)(lambda: to_row(here[0] - away, False))
            pl.when(here[0] + away < rows)(lambda: to_row(here[0] + away, False))

    def hand_over(q):
        blocks = geo_all.at[pl.ds(q * group, group)]
        pltpu.make_async_remote_copy(
            src_ref=blocks,
            dst_ref=blocks,
            send_sem=gather_send.at[0],
            recv_sem=geo_recv.at[q],
            device_id={"row": layer * fold + (fold - 1 - part)},
            device_id_type=MESH,
        ).start()

    def start_gather(source, gathered, sem):
        def send(device):
            pltpu.make_async_remote_copy(
                src_ref=source,
                dst_ref=gathered.at[me],
                send_sem=gather_send.at[0],
                recv_sem=sem,
                device_id=device,
                device_id_type=MESH,
            ).start()

        each_other(send)

    def await_gather(gathered, count, sem):
        whole = gathered.at[pl.ds(0, count)]
        pltpu.make_async_copy(whole, whole, sem).wait()

    copies[0].wait()
    copies[2].wait()
    for x in range(size_x):
        kind = class_v[x]
        shift = jnp.zeros(kind.shape, jnp.float32)
        for level in range(classes):
            shift = jnp.where(kind == level, shift_ref[level], shift)
        weight = relax_weight / (6.0 + shift)
        weight_v[x] = jnp.broadcast_to(weight[:, None, :], (size_y, channels, size_z))
        if x == 0:
            wx_out[0] = weight
        if x == size_x - 1:
            wx_out[1] = weight
        if x == 0:
            wy_out[...] = jnp.zeros(wy_out.shape, wy_out.dtype)
        wy_out[0, x : x + 1, :] = weight[0:1]
        wy_out[1, x : x + 1, :] = weight[size_y - 1 : size_y]
    wz_out[...] = pack_deep(in_pairs(planes(weight_v)))
    start_weights()

    copies[3].wait()
    copies[4].wait()
    cell = cell_ref[...]
    bits = size_z.bit_length() - 1
    cell_z = cell & (size_z - 1)
    cell_xy = cell >> bits
    pick_z = lax.broadcasted_iota(jnp.int32, (size_z, slots), 0) == cell_z
    pick_z = jnp.where(pick_z, 1.0, 0.0).astype(jnp.bfloat16)
    for at in range(size_x * size_y):
        at_cell[at] = jnp.broadcast_to(
            jnp.where(cell_xy == at, 1.0, 0.0), (channels, slots)
        )
    live = lax.broadcasted_iota(jnp.int32, (channels, slots), 1) < live_ref[...]
    brick_wait(source_v, local_sem.at[2])
    for x in range(size_x):
        forcing_v[0, x] = weight_v[x] * source_v[x]

    def inside(value, above, below):
        blank = jnp.zeros((1,) + cell_shape, jnp.float32)
        around = jnp.concatenate([value[1:], blank], axis=0)
        around = around + jnp.concatenate([blank, value[:-1]], axis=0)
        for other in (above, below):
            if other is not None:
                around = around + other
        flat = value.reshape(slab)
        beside = jnp.where(slab_lane == size_z - 1, 0.0, turn(flat, size_z - 1))
        beside = beside + jnp.where(slab_lane == 0, 0.0, turn(flat, 1))
        return around + beside.reshape(value.shape)

    def ends(beyond, at):
        both = (turn(beyond, -2 * at) * edge).astype(jnp.float32)
        return both[:channels], both[channels:]

    def inner(source, target, force):
        for x in range(size_x):
            value = source[x]
            around = inside(
                value,
                source[x + 1] if x + 1 < size_x else None,
                source[x - 1] if x > 0 else None,
            )
            target[x] = (1.0 - relax_weight) * value + force[x] + weight_v[x] * around

    def pick(axis, q):
        return (
            jnp.where(here[axis] > 0, q, none),
            jnp.where(here[axis] < sizes[axis] - 1, q, none),
        )

    def half_of_pair(i):
        return slice(channels * (i % 2), channels * (i % 2) + channels)

    def from_x(q, side, y):
        both = x_in[pick(0, q)[side], side, y // 2].astype(jnp.float32)
        return both[half_of_pair(y)]

    def from_y(q, side, x):
        both = y_in[pick(1, q)[side], side, x // 2].astype(jnp.float32)
        return both[half_of_pair(x)]

    def either(low, high):
        return jnp.where(even, low.astype(jnp.float32), high.astype(jnp.float32))

    def from_z(q):
        below, above = pick(2, q)
        return either(z_in[below, 0], z_in[above, 1])

    def beside_ends(natural):
        return jnp.where(even, natural, turn(natural, -2)).astype(jnp.bfloat16)

    def corner(a, b, q, side_a, side_b):
        there = exists(a, side_a) & exists(b, side_b)
        return edge_ins[a, b][jnp.where(there, q // 3, ROUNDS), side_a, side_b]

    def corner_xy(q, side_x, side_y):
        both = corner(0, 1, q, side_x, side_y).astype(jnp.float32)
        return both[half_of_pair(size_x - 1 if side_x == 0 else 0)]

    def corner_z(axis, q, side):
        return either(corner(axis, 2, q, side, 0), corner(axis, 2, q, side, 1))

    def outer(target, q):
        beyond = beside_ends(from_z(q))
        for x in range(size_x):
            for p in range(pairs):
                for y, around in zip((2 * p, 2 * p + 1), ends(beyond, x * pairs + p)):
                    if x == 0:
                        around = around + from_x(q, 0, y)
                    if x == size_x - 1:
                        around = around + from_x(q, 1, y)
                    if y == 0:
                        around = around + from_y(q, 0, x)
                    if y == size_y - 1:
                        around = around + from_y(q, 1, x)
                    target[x, y] = target[x, y] + weight_v[x, y] * around

    def spread_weights():
        for side in (0, 1):
            weight = wx_in[jnp.where(exists(0, side), side, 2)]
            rim_wx[side] = jnp.broadcast_to(weight[:, None, :], (size_y,) + cell_shape)
            weight = wy_in[jnp.where(exists(1, side), side, 2)][:size_x]
            rim_wy[side] = jnp.broadcast_to(weight[:, None, :], (size_x,) + cell_shape)
        rim_wz[...] = either(
            wz_in[jnp.where(exists(2, 0), 0, 2)], wz_in[jnp.where(exists(2, 1), 1, 2)]
        )

    def own_rim(source, q):
        for side in (0, 1):
            rim_x[side] = rim_wx[side] * source[(size_x - 1) * side]
            for x in range(size_x):
                rim_y[side, x] = rim_wy[side, x] * source[x, (size_y - 1) * side]
        own = z_out[q].astype(jnp.float32)
        rim_z[...] = rim_wz[...] * jnp.where(even, turn(own, -1), turn(own, 1))

    def rim(target, q):
        along, across = (size_x - 1) * size_y, 2 * (pairs - 1)
        around = jnp.where(low_plane, turn(corner_z(0, q, 0), -along), 0.0)
        around = around + jnp.where(high_plane, turn(corner_z(0, q, 1), along), 0.0)
        first = upper & (in_line == 0)
        final = jnp.logical_not(upper) & (in_line == pairs - 1)
        around = around + jnp.where(first, swap(turn(corner_z(1, q, 0), -across)), 0.0)
        around = around + jnp.where(final, swap(turn(corner_z(1, q, 1), across)), 0.0)
        beyond = beside_ends(rim_z[...] + rim_wz[...] * around + from_z(q + 1))
        beyond_x = [beside_ends(corner_z(0, q, side)) for side in (0, 1)]
        beyond_y = [beside_ends(corner_z(1, q, side)) for side in (0, 1)]

        def swept_x(side, p):
            found = []
            theirs = (size_x - 1) * (1 - side)
            for y, around in zip((2 * p, 2 * p + 1), ends(beyond_x[side], theirs * pairs + p)):
                if y == 0:
                    around = around + corner_xy(q, side, 0)
                if y == size_y - 1:
                    around = around + corner_xy(q, side, 1)
                found.append(rim_x[side, y] + from_x(q + 1, side, y) + rim_wx[side, y] * around)
            return found

        def swept_y(side, x):
            theirs = (size_y - 1) * (1 - side)
            around = ends(beyond_y[side], x * pairs + theirs // 2)[theirs % 2]
            if x == 0:
                around = around + corner_xy(q, 0, side)
            if x == size_x - 1:
                around = around + corner_xy(q, 1, side)
            return rim_y[side, x] + from_y(q + 1, side, x) + rim_wy[side, x] * around

        for x in range(size_x):
            for p in range(pairs):
                below = swept_x(0, p) if x == 0 else None
                above = swept_x(1, p) if x == size_x - 1 else None
                for i, around in enumerate(ends(beyond, x * pairs + p)):
                    y = 2 * p + i
                    if below:
                        around = around + below[i]
                    if above:
                        around = around + above[i]
                    if y == 0:
                        around = around + swept_y(0, x)
                    if y == size_y - 1:
                        around = around + swept_y(1, x)
                    target[x, y] = target[x, y] + weight_v[x, y] * around

    pieces = 4
    chunk = slots // pieces

    def make_tiles():
        def body(i, carry):
            a, k = i // layers, lax.rem(i, layers)
            q = nearest(k, layer, layers) * fold + lax.rem(part + a, fold)
            await_gather(geo_all, group, geo_recv.at[q])
            if fold > 1:
                pl.when(a == 0)(lambda: hand_over(q))
            for j in range(group):
                source = geo_all[q * group + j]
                for piece in range(pieces):
                    span = slice(piece * chunk, (piece + 1) * chunk)
                    delta_x = column_v[0, span, :] - source[0:1, :]
                    delta_y = column_v[1, span, :] - source[1:2, :]
                    delta_z = column_v[2, span, :] - source[2:3, :]
                    square = delta_x * delta_x + delta_y * delta_y + delta_z * delta_z + 1e-30
                    distance = square * lax.rsqrt(square)
                    wave = cosine_of_turns(distance * (wave_number / (2.0 * math.pi)))
                    value = (source[3:4, :] * factor) * wave / (distance + soften)
                    tile_v[q, span, j * slots : (j + 1) * slots] = value.astype(tile_v.dtype)
            return carry

        lax.fori_loop(0, rows, body, 0)

    def apply_tiles(r):
        total = jnp.zeros((channels, slots), jnp.float32)
        for k in range(rows):
            q = nth(k)
            with jax.named_scope(f"w_dens{r}_{k}"):
                await_gather(density_all.at[r], group - (k == 0), density_recv.at[r, q])
            values = jnp.concatenate(
                [density_all[r, q * group + j] for j in range(group)], axis=1
            )
            total = total + lax.dot_general(
                values, tile_v[q], (((1,), (1,)), ((), ())), preferred_element_type=jnp.float32
            )
        return total

    def land(sem, each):
        await_bytes(face_recv.at[sem], each)

    def drain(each):
        await_bytes(face_send.at[0], each)

    def drain_now():
        for q in range(3 * ROUNDS - 2):
            drain(face_cells)
            if q % 3 == 1:
                drain(edge_cells)
        drain(weight_cells)
        await_gather(geo_all, devices - 1, gather_send.at[0])
        for r in range(ROUNDS - 1):
            await_gather(density_all.at[r], devices - 1, gather_send.at[0])

    knowledge = ([rows, rows] + stages)[-2:] if len(stages) != 1 else stages * 2
    for r in range(ROUNDS):
        single, double = 3 * r, 3 * r + 1
        before = init_v if r == 0 else state_v.at[2]
        once, mid, after = state_v.at[0], state_v.at[1], state_v.at[2]
        if r == ROUNDS - 1:
            after = field_ref
        force = forcing_v.at[r]
        with jax.named_scope(f"inner{r}"):
            inner(before, once, forcing_v.at[0])
        if r > 0:
            with jax.named_scope("tilesB"):
                make_tiles()
        if r == 0:
            with jax.named_scope("w_known0"):
                for stage in range(len(stages) - 2):
                    hear(stage)
                    pass_on(stage + 1)
                start_geometry(-1, knowledge[0])
        with jax.named_scope(f"w_single{r}"):
            land(0, face_cells)
        if r == 0 and len(stages) > 1:
            hear(len(stages) - 2)
            pass_on(len(stages) - 1)
            start_geometry(knowledge[0], knowledge[1])
        with jax.named_scope(f"outer{r}"):
            outer(once, single)
        if r > 0:
            with jax.named_scope(f"apply{r-1}"):
                potential = jnp.where(live, apply_tiles(r - 1), 0.0)
            with jax.named_scope(f"load{r}"):
                half_of = coupling * potential
                big = half_of.astype(jnp.bfloat16).astype(jnp.float32)
                small = half_of - big
                placed = jnp.concatenate(
                    [(at_cell[...] * part[None]).astype(jnp.bfloat16) for part in (big, small)],
                    axis=2,
                ).reshape(size_x * size_y * channels, 2 * slots)
                load = lax.dot_general(
                    placed, jnp.concatenate([pick_z, pick_z], axis=1),
                    (((1,), (1,)), ((), ())), preferred_element_type=jnp.float32,
                )
                load = load.reshape(size_x, size_y, channels, size_z)
                for x in range(size_x):
                    change = weight_v[x] * load[x]
                    force[x] = forcing_v[0, x] + change
                    once[x] = once[x] + change
        with jax.named_scope(f"pack{r}"):
            pack(double, planes(once))
        start_edges(double)
        start_faces(double)
        with jax.named_scope(f"innerd{r}"):
            inner(once, mid, force)
        with jax.named_scope(f"packd{r}"):
            pack(double + 1, planes(mid))
        start_faces(double + 1)
        if r == 0:
            with jax.named_scope("w_weights"):
                land(4, weight_cells)
                spread_weights()
            with jax.named_scope("w_known"):
                if stages:
                    hear(len(stages) - 1)
            with jax.named_scope("st_geo"):
                start_geometry(knowledge[1], rows)
        else:
            drain_now()
        own_rim(once, double)
        with jax.named_scope(f"w_double{r}"):
            land(1, face_cells)
        with jax.named_scope(f"outerd{r}"):
            outer(mid, double)
            inner(mid, after, force)
        with jax.named_scope(f"w_edges{r}"):
            land(3, edge_cells)
        with jax.named_scope(f"w_rim{r}"):
            land(2, face_cells)
        with jax.named_scope(f"rim{r}"):
            rim(after, double)
        with jax.named_scope(f"density{r}"):
            flat = after[...].reshape(size_x * size_y * channels, size_z).astype(jnp.bfloat16)
            picked = jnp.dot(flat, pick_z, preferred_element_type=jnp.float32)
            picked = picked.reshape(size_x * size_y, channels, slots)
            density = jnp.sum(picked * at_cell[...], axis=0)
            density = jnp.where(live, density, 0.0).astype(jnp.bfloat16)
            density_out[r] = density
            density_all[r, me] = density
        with jax.named_scope(f"st_dens{r}"):
            start_gather(density_out.at[r], density_all.at[r], density_recv.at[r, here[0]])
        if r < ROUNDS - 1:
            with jax.named_scope(f"pack_s{r}"):
                pack(single + 3, planes(after))
            start_faces(single + 3)
    drain(face_cells)
    drain(edge_cells)
    drain(face_cells)
    with jax.named_scope(f"apply{ROUNDS-1}"):
        potential_ref[...] = jnp.where(live, apply_tiles(ROUNDS - 1), 0.0)

    with jax.named_scope("finish"):
        await_gather(density_all.at[ROUNDS - 1], devices - 1, gather_send.at[0])


def place(field_v, potential_v, field_hbm, potential_hbm, sem):
    channels = field_hbm.shape[0]
    copies = [
        pltpu.make_async_copy(field_v.at[:, :, e, :], field_hbm.at[e], sem.at[0])
        for e in range(channels)
    ]
    copies.append(pltpu.make_async_copy(potential_v, potential_hbm, sem.at[1]))
    for copy in copies:
        copy.start()
    pltpu.make_async_copy(field_v, field_v, sem.at[0]).wait()
    copies[-1].wait()


def local(sizes, initial_field, source_term, cell_class, class_shift, surface_cell, live_count,
          panel_geometry):
    channels, size_x, size_y, size_z = initial_field.shape
    slots = surface_cell.shape[0]
    rows, cols, depths = sizes
    devices, group = rows * cols * depths, cols * depths
    brick = (size_x, size_y, channels, size_z)
    vmem = pl.BlockSpec(memory_space=pltpu.VMEM)
    hbm = pl.BlockSpec(memory_space=pltpu.HBM)
    per_device = slots * (2 * slots + 4 * 8 + ROUNDS * 2 * 2 * channels)
    grant = devices * per_device + 36 * 4 * math.prod(brick)
    operands = [
        pltpu.with_memory_space_constraint(array, pltpu.HBM)
        for array in (
            initial_field, source_term, cell_class, class_shift,
            surface_cell.reshape(1, slots), panel_geometry,
        )
    ]
    operands.insert(5, live_count.reshape(1, 1))
    two, turns = 2 * channels, 3 * ROUNDS
    field, potential = pl.pallas_call(
        functools.partial(kernel, sizes),
        out_shape=(
            jax.ShapeDtypeStruct(brick, jnp.float32),
            jax.ShapeDtypeStruct((channels, slots), jnp.float32),
        ),
        in_specs=[hbm] * 5 + [pl.BlockSpec(memory_space=pl.ANY), hbm],
        out_specs=(vmem, vmem),
        scratch_shapes=[
            pltpu.VMEM(brick, jnp.float32),
            pltpu.VMEM(brick, jnp.float32),
            pltpu.VMEM((ROUNDS,) + brick, jnp.float32),
            pltpu.VMEM((size_x, size_y, size_z), jnp.int32),
            pltpu.VMEM(brick, jnp.float32),
            pltpu.VMEM((3,) + brick, jnp.float32),
            pltpu.VMEM((turns, 2, size_y // 2, two, size_z), jnp.bfloat16),
            pltpu.VMEM((turns + 1, 2, size_y // 2, two, size_z), jnp.bfloat16),
            pltpu.VMEM((turns, 2, size_x // 2, two, size_z), jnp.bfloat16),
            pltpu.VMEM((turns + 1, 2, size_x // 2, two, size_z), jnp.bfloat16),
            pltpu.VMEM((turns, two, size_z), jnp.bfloat16),
            pltpu.VMEM((turns + 1, 2, two, size_z), jnp.bfloat16),
            pltpu.VMEM((ROUNDS + 1, 2, 2, two, size_z), jnp.bfloat16),
            pltpu.VMEM((ROUNDS + 1, 2, 2, two, size_z), jnp.bfloat16),
            pltpu.VMEM((ROUNDS + 1, 2, 2, two, size_z), jnp.bfloat16),
            pltpu.VMEM((2, size_y, size_z), jnp.float32),
            pltpu.VMEM((3, size_y, size_z), jnp.float32),
            pltpu.VMEM((2, channels, size_z), jnp.float32),
            pltpu.VMEM((3, channels, size_z), jnp.float32),
            pltpu.VMEM((two, size_z), jnp.bfloat16),
            pltpu.VMEM((3, two, size_z), jnp.bfloat16),
            pltpu.VMEM((2, size_y, channels, size_z), jnp.float32),
            pltpu.VMEM((2, size_x, channels, size_z), jnp.float32),
            pltpu.VMEM((two, size_z), jnp.float32),
            pltpu.VMEM((2, size_y, channels, size_z), jnp.float32),
            pltpu.VMEM((2, size_x, channels, size_z), jnp.float32),
            pltpu.VMEM((two, size_z), jnp.float32),
            pltpu.VMEM((size_y + size_x + 2, channels, size_z), jnp.float32),
            pltpu.VMEM((devices, 4, slots), jnp.float32),
            pltpu.VMEM((3, slots, slots), jnp.float32),
            pltpu.VMEM((rows, slots, group * slots), jnp.bfloat16),
            pltpu.VMEM((ROUNDS, channels, slots), jnp.bfloat16),
            pltpu.VMEM((ROUNDS, devices, channels, slots), jnp.bfloat16),
            pltpu.VMEM((size_x * size_y, channels, slots), jnp.float32),
            pltpu.SMEM(class_shift.shape, jnp.float32),
            pltpu.VMEM((1, 1), jnp.int32),
            pltpu.VMEM((1, slots), jnp.int32),
            pltpu.VMEM(panel_geometry.shape, jnp.float32),
            pltpu.SemaphoreType.REGULAR((max(1, len(known_stages(rows))),)),
            pltpu.SemaphoreType.DMA((7,)),
            pltpu.SemaphoreType.DMA((1,)),
            pltpu.SemaphoreType.DMA((5,)),
            pltpu.SemaphoreType.DMA((1,)),
            pltpu.SemaphoreType.DMA((rows,)),
            pltpu.SemaphoreType.DMA((ROUNDS, rows)),
        ],
        compiler_params=pltpu.CompilerParams(
            collective_id=0, has_side_effects=True, vmem_limit_bytes=grant
        ),
    )(*operands)
    return pl.pallas_call(
        place,
        out_shape=(
            jax.ShapeDtypeStruct(initial_field.shape, jnp.float32),
            jax.ShapeDtypeStruct((channels, slots), jnp.float32),
        ),
        in_specs=[vmem] * 2,
        out_specs=(hbm, hbm),
        scratch_shapes=[pltpu.SemaphoreType.DMA((2,))],
        compiler_params=pltpu.CompilerParams(vmem_limit_bytes=8 * math.prod(brick)),
    )(field, potential)


def solution(mesh):
    placed = (
        P(None, "row", "col", "gz"),
        P(None, "row", "col", "gz"),
        P("row", "col", "gz"),
        P(),
        P(("row", "col", "gz")),
        P(("row", "col", "gz")),
        P(None, ("row", "col", "gz")),
    )
    return jax.shard_map(
        functools.partial(local, tuple(mesh.shape[axis] for axis in AXES)),
        mesh=mesh,
        in_specs=placed,
        out_specs=(P(None, "row", "col", "gz"), P(None, ("row", "col", "gz"))),
        check_vma=False,
    )
```

```python
import functools
import math

import jax
import jax.numpy as jnp
import numpy as np
from jax import lax
from jax.experimental import pallas as pl
from jax.experimental.pallas import tpu as pltpu
from jax.sharding import PartitionSpec as P

ROUNDS = 2

relax_weight = 0.8
wave_number = 25.0
soften = 0.05
coupling = 0.5

MESH = pl.DeviceIdType.MESH
AXES = ("row", "col", "gz")


def cosine_terms(degree=6):
    nodes = 0.125 * (1.0 + np.cos(np.pi * (np.arange(64) + 0.5) / 64))
    fitted = np.polynomial.Polynomial.fit(
        nodes, np.cos(2 * np.pi * np.sqrt(nodes)), degree, domain=[0.0, 0.25]
    )
    return [float(c) for c in fitted.convert().coef]


COSINE = cosine_terms()


def cosine_of_turns(turns):
    fraction = turns - jnp.floor(turns + 0.5)
    square = fraction * fraction
    value = jnp.full_like(square, COSINE[-1])
    for term in reversed(COSINE[:-1]):
        value = value * square + term
    return value


def relays(sizes):
    rows, cols, depths = sizes
    if cols != 2 or depths != 2 or rows < 2 or rows % 2:
        return []
    stages, far = [[(-1, 0, 0), (1, 0, 0), (0, 1, 0), (0, 0, 1)]], 2
    while far < rows:
        stages.append([(-far, 0, 0), (far, 0, 0)] + ([(0, 1, 1)] if far == 2 else []))
        far *= 2
    stages.append([(0, 1, 1)])

    def at(device, offset):
        r, c, d = (x + o for x, o in zip(device, offset))
        return (r, c % 2, d % 2) if 0 <= r < rows else None

    everyone = [(r, c, d) for r in range(rows) for c in range(2) for d in range(2)]
    known = {x: {x} | {at(x, o) for o in stages[0]} for x in everyone}
    for i, stage in enumerate(stages):
        told = {x: set(known[x]) for x in everyone}
        for x in everyone:
            for offset in stage:
                target = at(x, offset)
                if target is not None:
                    if target not in known[x]:
                        return []
                    told[target] |= known[x]
        known = told
        for x in everyone:
            ahead = {at(x, (r, c, d)) for r in (-1, 0, 1) for c in (0, 1) for d in (0, 1) if abs(r) + c + d < 3}
            ahead |= {at(x, (r, 0, 0)) for r in (-2, 2)}
            if i == len(stages) - 2:
                ahead = {y for y in everyone if (y[0] - x[0]) % 2 == 0}
            if i == len(stages) - 1:
                ahead = set(everyone)
            if not ahead - {None} <= known[x] | {None}:
                return []
    return stages


def kernel(
    sizes,
    init_hbm, source_hbm, class_hbm, shift_hbm, cell_hbm, live_hbm, geo_hbm,
    field_ref, potential_ref,
    init_v, source_v, forcing_v, class_v, weight_v, state_v,
    x_out, x_in, y_out, y_in, z_out, z_in, xy_in, xz_in, yz_in,
    wx_out, wx_in, wy_out, wy_in, wz_out, wz_in, rim_x, rim_y, rim_z,
    rim_wx, rim_wy, rim_wz, meter,
    geo_all, column_v, tile_v, density_out, density_all, at_cell,
    shift_ref, live_ref, cell_ref, geo_ref,
    known, local_sem, face_send, face_recv, gather_send, geo_recv, density_recv,
):
    rows, cols, depths = sizes
    devices = rows * cols * depths
    group = cols * depths
    channels, size_x, size_y, size_z = init_hbm.shape
    slots = cell_hbm.shape[1]
    classes = shift_ref.shape[0]
    factor = 1.0 / math.sqrt(slots * devices)
    here = tuple(lax.axis_index(axis) for axis in AXES)
    me = (here[0] * cols + here[1]) * depths + here[2]

    def brick_copies(hbm, vmem, sem):
        return [
            pltpu.make_async_copy(hbm.at[e], vmem.at[:, :, e, :], sem) for e in range(channels)
        ]

    def brick_wait(vmem, sem):
        pltpu.make_async_copy(vmem, vmem, sem).wait()

    for copy in brick_copies(init_hbm, init_v, local_sem.at[0]):
        copy.start()

    stages = relays(sizes)
    barrier = pltpu.get_barrier_semaphore()

    def offset_place(offset):
        return (
            here[0] + offset[0],
            1 - here[1] if offset[1] else here[1],
            1 - here[2] if offset[2] else here[2],
        )

    def reaches(offset):
        if offset[0] == 0:
            return None
        return here[0] >= -offset[0] if offset[0] < 0 else here[0] + offset[0] < rows

    def tell(sem, offset):
        def go():
            pl.semaphore_signal(
                sem, inc=1, device_id=offset_place(offset), device_id_type=MESH
            )

        present = reaches(offset)
        if present is None:
            go()
        else:
            pl.when(present)(go)

    def tellers(stage):
        return sum(
            1 if reaches(offset) is None else jnp.where(reaches(offset), 1, 0)
            for offset in stages[stage]
        )

    def pass_on(stage):
        for offset in stages[stage]:
            tell(known.at[stage], offset)

    def hear(stage):
        pl.semaphore_wait(known.at[stage], tellers(stage))

    if stages:
        for offset in stages[0]:
            tell(barrier, offset)
        near = tellers(0)
    else:
        near = devices - 1

    copies = [
        pltpu.make_async_copy(class_hbm, class_v, local_sem.at[1]),
        pltpu.make_async_copy(geo_hbm, geo_ref, local_sem.at[3]),
        pltpu.make_async_copy(shift_hbm, shift_ref, local_sem.at[4]),
        pltpu.make_async_copy(cell_hbm, cell_ref, local_sem.at[5]),
        pltpu.make_async_copy(live_hbm, live_ref, local_sem.at[6]),
    ]

    def nearest(k, own, count):
        below, above = own, count - 1 - own
        near = own + jnp.where(lax.rem(k, 2) == 1, (k + 1) // 2, -(k // 2))
        far = jnp.where(below < above, k, count - 1 - k)
        return jnp.where((k <= 2 * below) & (k <= 2 * above), near, far)

    def nth(k):
        return nearest(k, here[0], rows)

    def each_other(action):
        def at(row, first):
            for b in reversed(range(cols)):
                for c in reversed(range(depths)):
                    if first and b == 0 and c == 0:
                        continue
                    action((row, lax.rem(here[1] + b, cols), lax.rem(here[2] + c, depths)))

        def others(i, carry):
            at(nth(rows - 1 - i), False)
            return carry

        lax.fori_loop(0, rows - 1, others, 0)
        at(here[0], True)

    if not stages:
        each_other(
            lambda device: pl.semaphore_signal(
                barrier, inc=1, device_id=device, device_id_type=MESH
            )
        )
    for copy in copies:
        copy.start()
    for copy in brick_copies(source_hbm, source_v, local_sem.at[2]):
        copy.start()

    cell_shape, pair_shape = (channels, size_z), (2 * channels, size_z)
    pairs = size_y // 2
    lane = lax.broadcasted_iota(jnp.int32, pair_shape, 1)
    even = (lane & 1) == 0
    at_pair = lane >> 1
    in_line = lax.rem(at_pair, pairs)
    upper = lax.broadcasted_iota(jnp.int32, pair_shape, 0) < channels
    low_plane = at_pair < pairs
    high_plane = (at_pair >= (size_x - 1) * pairs) & (at_pair < size_x * pairs)
    edge = jnp.where((lane == 0) | (lane == size_z - 1), 1.0, 0.0).astype(jnp.bfloat16)
    slab = (size_y * channels, size_z)
    slab_lane = lax.broadcasted_iota(jnp.int32, slab, 1)

    def turn(value, shift):
        return pltpu.roll(value, shift % size_z, 1)

    def swap(value):
        return jnp.concatenate([value[channels:], value[:channels]], axis=0)

    def planes(ref):
        return [[ref[x, y] for y in range(size_y)] for x in range(size_x)]

    def in_pairs(values):
        return [
            [
                jnp.concatenate([line[y], line[y + 1]], axis=0).astype(jnp.bfloat16)
                for y in range(0, size_y, 2)
            ]
            for line in values
        ]

    def pack_deep(paired):
        packed = jnp.zeros(pair_shape, jnp.bfloat16)
        for x in range(size_x):
            for p in range(pairs):
                packed = packed + turn(paired[x][p] * edge, 2 * (x * pairs + p) + 1)
        return packed

    def pack(q, values):
        paired = in_pairs(values)
        for side, x in ((0, 0), (1, size_x - 1)):
            for p in range(pairs):
                x_out[q, side, p] = paired[x][p]
        for side, y in ((0, 0), (1, size_y - 1)):
            for x in range(0, size_x, 2):
                both = jnp.concatenate([values[x][y], values[x + 1][y]], axis=0)
                y_out[q, side, x // 2] = both.astype(y_out.dtype)
        z_out[q] = pack_deep(paired)

    def exists(axis, up):
        return here[axis] < sizes[axis] - 1 if up else here[axis] > 0

    beside = []
    for axis in range(3):
        if sizes[axis] == 2:
            beside.append((axis, 1 - here[axis], 1 - here[axis], None))
        elif sizes[axis] > 2:
            beside.append((axis, 0, here[axis] - 1, exists(axis, 0)))
            beside.append((axis, 1, here[axis] + 1, exists(axis, 1)))
    edges_beside = [(one, two) for one in beside for two in beside if one[0] < two[0]]
    outs, ins = (x_out, y_out, z_out), (x_in, y_in, z_in)
    edge_ins = {(0, 1): xy_in, (0, 2): xz_in, (1, 2): yz_in}

    def when(present, action):
        if present is None:
            action()
        else:
            pl.when(present)(action)

    def start(source, landing, sem, target, present):
        def go():
            pltpu.make_async_remote_copy(
                src_ref=source,
                dst_ref=landing,
                send_sem=face_send.at[0],
                recv_sem=face_recv.at[sem],
                device_id=target,
                device_id_type=MESH,
            ).start()

        when(present, go)

    def start_faces(q):
        for axis, side, place, present in beside:
            source = outs[axis].at[q] if axis == 2 else outs[axis].at[q, side]
            start(source, ins[axis].at[q, 1 - side], q % 3, {AXES[axis]: place}, present)

    def start_edges(q):
        for (a, side_a, place_a, one), (b, side_b, place_b, two) in edges_beside:
            if (a, b) == (0, 1):
                source = y_out.at[q, side_b, side_a * ((size_x - 1) // 2)]
            else:
                source = z_out.at[q]
            landing = edge_ins[a, b].at[q // 3, 1 - side_a, 1 - side_b]
            present = two if one is None else one if two is None else one & two
            start(source, landing, 3, {AXES[a]: place_a, AXES[b]: place_b}, present)

    def start_weights():
        for axis, side, place, present in beside:
            out, into = ((wx_out, wx_in), (wy_out, wy_in), (wz_out, wz_in))[axis]
            source = out if axis == 2 else out.at[side]
            start(source, into.at[1 - side], 4, {AXES[axis]: place}, present)

    def await_bytes(sem, each):
        split = [axis for axis in range(3) if sizes[axis] > 2]
        for case in range(2 ** len(split)):
            counts = [min(count, 2) - 1 for count in sizes]
            condition = None
            for i, axis in enumerate(split):
                both = (case >> i) & 1
                counts[axis] += both
                holds = (here[axis] > 0) & (here[axis] < sizes[axis] - 1)
                holds = holds if both else jnp.logical_not(holds)
                condition = holds if condition is None else condition & holds
            span = meter.at[pl.ds(0, each(counts))]
            when(condition, lambda span=span: pltpu.make_async_copy(span, span, sem).wait())

    def face_cells(n):
        return n[0] * pairs + n[1] * (size_x // 2) + n[2]

    def edge_cells(n):
        return n[0] * n[1] + n[0] * n[2] + n[1] * n[2]

    def weight_cells(n):
        return n[0] * (size_y // channels) + n[1] + n[2]

    none = 3 * ROUNDS
    x_in[none] = jnp.zeros(x_in.shape[1:], x_in.dtype)
    y_in[none] = jnp.zeros(y_in.shape[1:], y_in.dtype)
    z_in[none] = jnp.zeros(z_in.shape[1:], z_in.dtype)
    for into in edge_ins.values():
        into[ROUNDS] = jnp.zeros(into.shape[1:], into.dtype)
    wx_in[2] = jnp.zeros(wx_in.shape[1:], wx_in.dtype)
    wy_in[2] = jnp.zeros(wy_in.shape[1:], wy_in.dtype)
    wz_in[2] = jnp.zeros(wz_in.shape[1:], wz_in.dtype)

    with jax.named_scope("w_init"):
        brick_wait(init_v, local_sem.at[0])

    pack(0, planes(init_v))

    with jax.named_scope("w_barrier"):
        pl.semaphore_wait(barrier, near)
    if stages:
        pass_on(0)
    start_faces(0)

    copies[1].wait()
    eye = lax.broadcasted_iota(jnp.int32, (slots, slots), 0) == lax.broadcasted_iota(
        jnp.int32, (slots, slots), 1
    )
    for i in range(3):
        column = jnp.sum(jnp.where(eye, geo_ref[i : i + 1, :], 0.0), axis=1, keepdims=True)
        column_v[i] = jnp.broadcast_to(column, (slots, slots))
    pltpu.make_async_copy(geo_ref, geo_all.at[me], geo_recv.at[here[0]]).start()


    fold = 2 - rows % 2
    layers, layer, part = rows // fold, here[0] // fold, lax.rem(here[0], fold)

    def send_geometry(row, b, c):
        pltpu.make_async_remote_copy(
            src_ref=geo_ref,
            dst_ref=geo_all.at[me],
            send_sem=gather_send.at[0],
            recv_sem=geo_recv.at[here[0]],
            device_id=(row, lax.rem(here[1] + b, cols), lax.rem(here[2] + c, depths)),
            device_id_type=MESH,
        ).start()

    others_beside = [(b, c) for b in range(cols) for c in range(depths)]

    def start_geometry(near_part, far_part):
        if near_part:
            for b, c in others_beside[1:]:
                send_geometry(here[0], b, c)
        for away in reversed(range(fold, rows, fold)):
            targets = []
            if near_part and away == fold or far_part and away > fold:
                targets += others_beside[:1]
            if far_part:
                targets += others_beside[1:]

            def to_row(row, targets=targets):
                for b, c in targets:
                    send_geometry(row, b, c)

            if targets:
                pl.when(here[0] >= away)(lambda: to_row(here[0] - away))
                pl.when(here[0] + away < rows)(lambda: to_row(here[0] + away))

    def hand_over(q):
        blocks = geo_all.at[pl.ds(q * group, group)]
        pltpu.make_async_remote_copy(
            src_ref=blocks,
            dst_ref=blocks,
            send_sem=gather_send.at[0],
            recv_sem=geo_recv.at[q],
            device_id={"row": layer * fold + (fold - 1 - part)},
            device_id_type=MESH,
        ).start()

    def start_gather(source, gathered, sem):
        def send(device):
            pltpu.make_async_remote_copy(
                src_ref=source,
                dst_ref=gathered.at[me],
                send_sem=gather_send.at[0],
                recv_sem=sem,
                device_id=device,
                device_id_type=MESH,
            ).start()

        each_other(send)

    def await_gather(gathered, count, sem):
        whole = gathered.at[pl.ds(0, count)]
        pltpu.make_async_copy(whole, whole, sem).wait()

    copies[0].wait()
    copies[2].wait()
    for x in range(size_x):
        kind = class_v[x]
        shift = jnp.zeros(kind.shape, jnp.float32)
        for level in range(classes):
            shift = jnp.where(kind == level, shift_ref[level], shift)
        weight = relax_weight / (6.0 + shift)
        weight_v[x] = jnp.broadcast_to(weight[:, None, :], (size_y, channels, size_z))
        if x == 0:
            wx_out[0] = weight
        if x == size_x - 1:
            wx_out[1] = weight
        if x == 0:
            wy_out[...] = jnp.zeros(wy_out.shape, wy_out.dtype)
        wy_out[0, x : x + 1, :] = weight[0:1]
        wy_out[1, x : x + 1, :] = weight[size_y - 1 : size_y]
    wz_out[...] = pack_deep(in_pairs(planes(weight_v)))
    start_weights()

    copies[3].wait()
    copies[4].wait()
    cell = cell_ref[...]
    bits = size_z.bit_length() - 1
    cell_z = cell & (size_z - 1)
    cell_xy = cell >> bits
    pick_z = lax.broadcasted_iota(jnp.int32, (size_z, slots), 0) == cell_z
    pick_z = jnp.where(pick_z, 1.0, 0.0).astype(jnp.bfloat16)
    for at in range(size_x * size_y):
        at_cell[at] = jnp.broadcast_to(
            jnp.where(cell_xy == at, 1.0, 0.0), (channels, slots)
        )
    live = lax.broadcasted_iota(jnp.int32, (channels, slots), 1) < live_ref[...]
    brick_wait(source_v, local_sem.at[2])
    for x in range(size_x):
        forcing_v[0, x] = weight_v[x] * source_v[x]

    def inside(value, above, below):
        blank = jnp.zeros((1,) + cell_shape, jnp.float32)
        around = jnp.concatenate([value[1:], blank], axis=0)
        around = around + jnp.concatenate([blank, value[:-1]], axis=0)
        for other in (above, below):
            if other is not None:
                around = around + other
        flat = value.reshape(slab)
        beside = jnp.where(slab_lane == size_z - 1, 0.0, turn(flat, size_z - 1))
        beside = beside + jnp.where(slab_lane == 0, 0.0, turn(flat, 1))
        return around + beside.reshape(value.shape)

    def ends(beyond, at):
        both = (turn(beyond, -2 * at) * edge).astype(jnp.float32)
        return both[:channels], both[channels:]

    def inner(source, target, force):
        for x in range(size_x):
            value = source[x]
            around = inside(
                value,
                source[x + 1] if x + 1 < size_x else None,
                source[x - 1] if x > 0 else None,
            )
            target[x] = (1.0 - relax_weight) * value + force[x] + weight_v[x] * around

    def pick(axis, q):
        return (
            jnp.where(here[axis] > 0, q, none),
            jnp.where(here[axis] < sizes[axis] - 1, q, none),
        )

    def half_of_pair(i):
        return slice(channels * (i % 2), channels * (i % 2) + channels)

    def from_x(q, side, y):
        both = x_in[pick(0, q)[side], side, y // 2].astype(jnp.float32)
        return both[half_of_pair(y)]

    def from_y(q, side, x):
        both = y_in[pick(1, q)[side], side, x // 2].astype(jnp.float32)
        return both[half_of_pair(x)]

    def either(low, high):
        return jnp.where(even, low.astype(jnp.float32), high.astype(jnp.float32))

    def from_z(q):
        below, above = pick(2, q)
        return either(z_in[below, 0], z_in[above, 1])

    def beside_ends(natural):
        return jnp.where(even, natural, turn(natural, -2)).astype(jnp.bfloat16)

    def corner(a, b, q, side_a, side_b):
        there = exists(a, side_a) & exists(b, side_b)
        return edge_ins[a, b][jnp.where(there, q // 3, ROUNDS), side_a, side_b]

    def corner_xy(q, side_x, side_y):
        both = corner(0, 1, q, side_x, side_y).astype(jnp.float32)
        return both[half_of_pair(size_x - 1 if side_x == 0 else 0)]

    def corner_z(axis, q, side):
        return either(corner(axis, 2, q, side, 0), corner(axis, 2, q, side, 1))

    def outer(target, q):
        beyond = beside_ends(from_z(q))
        for x in range(size_x):
            for p in range(pairs):
                for y, around in zip((2 * p, 2 * p + 1), ends(beyond, x * pairs + p)):
                    if x == 0:
                        around = around + from_x(q, 0, y)
                    if x == size_x - 1:
                        around = around + from_x(q, 1, y)
                    if y == 0:
                        around = around + from_y(q, 0, x)
                    if y == size_y - 1:
                        around = around + from_y(q, 1, x)
                    target[x, y] = target[x, y] + weight_v[x, y] * around

    def spread_weights():
        for side in (0, 1):
            weight = wx_in[jnp.where(exists(0, side), side, 2)]
            rim_wx[side] = jnp.broadcast_to(weight[:, None, :], (size_y,) + cell_shape)
            weight = wy_in[jnp.where(exists(1, side), side, 2)][:size_x]
            rim_wy[side] = jnp.broadcast_to(weight[:, None, :], (size_x,) + cell_shape)
        rim_wz[...] = either(
            wz_in[jnp.where(exists(2, 0), 0, 2)], wz_in[jnp.where(exists(2, 1), 1, 2)]
        )

    def own_rim(source, q):
        for side in (0, 1):
            rim_x[side] = rim_wx[side] * source[(size_x - 1) * side]
            for x in range(size_x):
                rim_y[side, x] = rim_wy[side, x] * source[x, (size_y - 1) * side]
        own = z_out[q].astype(jnp.float32)
        rim_z[...] = rim_wz[...] * jnp.where(even, turn(own, -1), turn(own, 1))

    def rim(target, q):
        along, across = (size_x - 1) * size_y, 2 * (pairs - 1)
        around = jnp.where(low_plane, turn(corner_z(0, q, 0), -along), 0.0)
        around = around + jnp.where(high_plane, turn(corner_z(0, q, 1), along), 0.0)
        first = upper & (in_line == 0)
        final = jnp.logical_not(upper) & (in_line == pairs - 1)
        around = around + jnp.where(first, swap(turn(corner_z(1, q, 0), -across)), 0.0)
        around = around + jnp.where(final, swap(turn(corner_z(1, q, 1), across)), 0.0)
        beyond = beside_ends(rim_z[...] + rim_wz[...] * around + from_z(q + 1))
        beyond_x = [beside_ends(corner_z(0, q, side)) for side in (0, 1)]
        beyond_y = [beside_ends(corner_z(1, q, side)) for side in (0, 1)]

        def swept_x(side, p):
            found = []
            theirs = (size_x - 1) * (1 - side)
            for y, around in zip((2 * p, 2 * p + 1), ends(beyond_x[side], theirs * pairs + p)):
                if y == 0:
                    around = around + corner_xy(q, side, 0)
                if y == size_y - 1:
                    around = around + corner_xy(q, side, 1)
                found.append(rim_x[side, y] + from_x(q + 1, side, y) + rim_wx[side, y] * around)
            return found

        def swept_y(side, x):
            theirs = (size_y - 1) * (1 - side)
            around = ends(beyond_y[side], x * pairs + theirs // 2)[theirs % 2]
            if x == 0:
                around = around + corner_xy(q, 0, side)
            if x == size_x - 1:
                around = around + corner_xy(q, 1, side)
            return rim_y[side, x] + from_y(q + 1, side, x) + rim_wy[side, x] * around

        for x in range(size_x):
            for p in range(pairs):
                below = swept_x(0, p) if x == 0 else None
                above = swept_x(1, p) if x == size_x - 1 else None
                for i, around in enumerate(ends(beyond, x * pairs + p)):
                    y = 2 * p + i
                    if below:
                        around = around + below[i]
                    if above:
                        around = around + above[i]
                    if y == 0:
                        around = around + swept_y(0, x)
                    if y == size_y - 1:
                        around = around + swept_y(1, x)
                    target[x, y] = target[x, y] + weight_v[x, y] * around

    pieces = 4
    chunk = slots // pieces

    def make_tiles():
        def body(i, carry):
            a, k = i // layers, lax.rem(i, layers)
            q = nearest(k, layer, layers) * fold + lax.rem(part + a, fold)
            await_gather(geo_all, group, geo_recv.at[q])
            if fold > 1:
                pl.when(a == 0)(lambda: hand_over(q))
            for j in range(group):
                source = geo_all[q * group + j]
                for piece in range(pieces):
                    span = slice(piece * chunk, (piece + 1) * chunk)
                    delta_x = column_v[0, span, :] - source[0:1, :]
                    delta_y = column_v[1, span, :] - source[1:2, :]
                    delta_z = column_v[2, span, :] - source[2:3, :]
                    square = delta_x * delta_x + delta_y * delta_y + delta_z * delta_z + 1e-30
                    distance = square * lax.rsqrt(square)
                    wave = cosine_of_turns(distance * (wave_number / (2.0 * math.pi)))
                    value = (source[3:4, :] * factor) * wave / (distance + soften)
                    tile_v[q, span, j * slots : (j + 1) * slots] = value.astype(tile_v.dtype)
            return carry

        lax.fori_loop(0, rows, body, 0)

    def apply_tiles(r):
        total = jnp.zeros((channels, slots), jnp.float32)
        for k in range(rows):
            q = nth(k)
            with jax.named_scope(f"w_dens{r}_{k}"):
                await_gather(density_all.at[r], group - (k == 0), density_recv.at[r, q])
            values = jnp.concatenate(
                [density_all[r, q * group + j] for j in range(group)], axis=1
            )
            total = total + lax.dot_general(
                values, tile_v[q], (((1,), (1,)), ((), ())), preferred_element_type=jnp.float32
            )
        return total

    def land(sem, each):
        await_bytes(face_recv.at[sem], each)

    def drain(each):
        await_bytes(face_send.at[0], each)

    def drain_now():
        for q in range(3 * ROUNDS - 2):
            drain(face_cells)
            if q % 3 == 1:
                drain(edge_cells)
        drain(weight_cells)
        await_gather(geo_all, devices - 1, gather_send.at[0])
        for r in range(ROUNDS - 1):
            await_gather(density_all.at[r], devices - 1, gather_send.at[0])

    for r in range(ROUNDS):
        single, double = 3 * r, 3 * r + 1
        before = init_v if r == 0 else state_v.at[2]
        once, mid, after = state_v.at[0], state_v.at[1], state_v.at[2]
        if r == ROUNDS - 1:
            after = field_ref
        force = forcing_v.at[r]
        with jax.named_scope(f"inner{r}"):
            inner(before, once, forcing_v.at[0])
        if r > 0:
            with jax.named_scope("tilesB"):
                make_tiles()
        if r == 0:
            with jax.named_scope("w_known0"):
                if stages:
                    hear(0)
                    pass_on(1)
                start_geometry(True, not stages)
        with jax.named_scope(f"w_single{r}"):
            land(0, face_cells)
        if r == 0 and stages:
            for stage in range(1, len(stages) - 2):
                hear(stage)
                pass_on(stage + 1)
        with jax.named_scope(f"outer{r}"):
            outer(once, single)
        if r > 0:
            with jax.named_scope(f"apply{r-1}"):
                potential = jnp.where(live, apply_tiles(r - 1), 0.0)
            with jax.named_scope(f"load{r}"):
                half_of = coupling * potential
                big = half_of.astype(jnp.bfloat16).astype(jnp.float32)
                small = half_of - big
                placed = jnp.concatenate(
                    [(at_cell[...] * part[None]).astype(jnp.bfloat16) for part in (big, small)],
                    axis=2,
                ).reshape(size_x * size_y * channels, 2 * slots)
                load = lax.dot_general(
                    placed, jnp.concatenate([pick_z, pick_z], axis=1),
                    (((1,), (1,)), ((), ())), preferred_element_type=jnp.float32,
                )
                load = load.reshape(size_x, size_y, channels, size_z)
                for x in range(size_x):
                    change = weight_v[x] * load[x]
                    force[x] = forcing_v[0, x] + change
                    once[x] = once[x] + change
        with jax.named_scope(f"pack{r}"):
            pack(double, planes(once))
        start_edges(double)
        start_faces(double)
        with jax.named_scope(f"innerd{r}"):
            inner(once, mid, force)
        with jax.named_scope(f"packd{r}"):
            pack(double + 1, planes(mid))
        start_faces(double + 1)
        if r == 0:
            with jax.named_scope("w_weights"):
                land(4, weight_cells)
                spread_weights()
            with jax.named_scope("w_known"):
                if stages:
                    hear(len(stages) - 2)
                    pass_on(len(stages) - 1)
            with jax.named_scope("st_geo"):
                if stages:
                    start_geometry(False, True)
        else:
            drain_now()
        own_rim(once, double)
        with jax.named_scope(f"w_double{r}"):
            land(1, face_cells)
        with jax.named_scope(f"outerd{r}"):
            outer(mid, double)
            inner(mid, after, force)
        with jax.named_scope(f"w_edges{r}"):
            land(3, edge_cells)
        with jax.named_scope(f"w_rim{r}"):
            land(2, face_cells)
        with jax.named_scope(f"rim{r}"):
            rim(after, double)
        with jax.named_scope(f"density{r}"):
            flat = after[...].reshape(size_x * size_y * channels, size_z).astype(jnp.bfloat16)
            picked = jnp.dot(flat, pick_z, preferred_element_type=jnp.float32)
            picked = picked.reshape(size_x * size_y, channels, slots)
            density = jnp.sum(picked * at_cell[...], axis=0)
            density = jnp.where(live, density, 0.0).astype(jnp.bfloat16)
            density_out[r] = density
            density_all[r, me] = density
        if r == 0 and stages:
            hear(len(stages) - 1)
        with jax.named_scope(f"st_dens{r}"):
            start_gather(density_out.at[r], density_all.at[r], density_recv.at[r, here[0]])
        if r < ROUNDS - 1:
            with jax.named_scope(f"pack_s{r}"):
                pack(single + 3, planes(after))
            start_faces(single + 3)
    drain(face_cells)
    drain(edge_cells)
    drain(face_cells)
    with jax.named_scope(f"apply{ROUNDS-1}"):
        potential_ref[...] = jnp.where(live, apply_tiles(ROUNDS - 1), 0.0)

    with jax.named_scope("finish"):
        await_gather(density_all.at[ROUNDS - 1], devices - 1, gather_send.at[0])


def place(field_v, potential_v, field_hbm, potential_hbm, sem):
    channels = field_hbm.shape[0]
    copies = [
        pltpu.make_async_copy(field_v.at[:, :, e, :], field_hbm.at[e], sem.at[0])
        for e in range(channels)
    ]
    copies.append(pltpu.make_async_copy(potential_v, potential_hbm, sem.at[1]))
    for copy in copies:
        copy.start()
    pltpu.make_async_copy(field_v, field_v, sem.at[0]).wait()
    copies[-1].wait()


def local(sizes, initial_field, source_term, cell_class, class_shift, surface_cell, live_count,
          panel_geometry):
    channels, size_x, size_y, size_z = initial_field.shape
    slots = surface_cell.shape[0]
    rows, cols, depths = sizes
    devices, group = rows * cols * depths, cols * depths
    brick = (size_x, size_y, channels, size_z)
    vmem = pl.BlockSpec(memory_space=pltpu.VMEM)
    hbm = pl.BlockSpec(memory_space=pltpu.HBM)
    per_device = slots * (2 * slots + 4 * 8 + ROUNDS * 2 * 2 * channels)
    grant = devices * per_device + 36 * 4 * math.prod(brick)
    operands = [
        pltpu.with_memory_space_constraint(array, pltpu.HBM)
        for array in (
            initial_field, source_term, cell_class, class_shift,
            surface_cell.reshape(1, slots), panel_geometry,
        )
    ]
    operands.insert(5, live_count.reshape(1, 1))
    two, turns = 2 * channels, 3 * ROUNDS
    field, potential = pl.pallas_call(
        functools.partial(kernel, sizes),
        out_shape=(
            jax.ShapeDtypeStruct(brick, jnp.float32),
            jax.ShapeDtypeStruct((channels, slots), jnp.float32),
        ),
        in_specs=[hbm] * 5 + [pl.BlockSpec(memory_space=pl.ANY), hbm],
        out_specs=(vmem, vmem),
        scratch_shapes=[
            pltpu.VMEM(brick, jnp.float32),
            pltpu.VMEM(brick, jnp.float32),
            pltpu.VMEM((ROUNDS,) + brick, jnp.float32),
            pltpu.VMEM((size_x, size_y, size_z), jnp.int32),
            pltpu.VMEM(brick, jnp.float32),
            pltpu.VMEM((3,) + brick, jnp.float32),
            pltpu.VMEM((turns, 2, size_y // 2, two, size_z), jnp.bfloat16),
            pltpu.VMEM((turns + 1, 2, size_y // 2, two, size_z), jnp.bfloat16),
            pltpu.VMEM((turns, 2, size_x // 2, two, size_z), jnp.bfloat16),
            pltpu.VMEM((turns + 1, 2, size_x // 2, two, size_z), jnp.bfloat16),
            pltpu.VMEM((turns, two, size_z), jnp.bfloat16),
            pltpu.VMEM((turns + 1, 2, two, size_z), jnp.bfloat16),
            pltpu.VMEM((ROUNDS + 1, 2, 2, two, size_z), jnp.bfloat16),
            pltpu.VMEM((ROUNDS + 1, 2, 2, two, size_z), jnp.bfloat16),
            pltpu.VMEM((ROUNDS + 1, 2, 2, two, size_z), jnp.bfloat16),
            pltpu.VMEM((2, size_y, size_z), jnp.float32),
            pltpu.VMEM((3, size_y, size_z), jnp.float32),
            pltpu.VMEM((2, channels, size_z), jnp.float32),
            pltpu.VMEM((3, channels, size_z), jnp.float32),
            pltpu.VMEM((two, size_z), jnp.bfloat16),
            pltpu.VMEM((3, two, size_z), jnp.bfloat16),
            pltpu.VMEM((2, size_y, channels, size_z), jnp.float32),
            pltpu.VMEM((2, size_x, channels, size_z), jnp.float32),
            pltpu.VMEM((two, size_z), jnp.float32),
            pltpu.VMEM((2, size_y, channels, size_z), jnp.float32),
            pltpu.VMEM((2, size_x, channels, size_z), jnp.float32),
            pltpu.VMEM((two, size_z), jnp.float32),
            pltpu.VMEM((size_y + size_x + 2, channels, size_z), jnp.float32),
            pltpu.VMEM((devices, 4, slots), jnp.float32),
            pltpu.VMEM((3, slots, slots), jnp.float32),
            pltpu.VMEM((rows, slots, group * slots), jnp.bfloat16),
            pltpu.VMEM((ROUNDS, channels, slots), jnp.bfloat16),
            pltpu.VMEM((ROUNDS, devices, channels, slots), jnp.bfloat16),
            pltpu.VMEM((size_x * size_y, channels, slots), jnp.float32),
            pltpu.SMEM(class_shift.shape, jnp.float32),
            pltpu.VMEM((1, 1), jnp.int32),
            pltpu.VMEM((1, slots), jnp.int32),
            pltpu.VMEM(panel_geometry.shape, jnp.float32),
            pltpu.SemaphoreType.REGULAR((max(1, len(relays(sizes))),)),
            pltpu.SemaphoreType.DMA((7,)),
            pltpu.SemaphoreType.DMA((1,)),
            pltpu.SemaphoreType.DMA((5,)),
            pltpu.SemaphoreType.DMA((1,)),
            pltpu.SemaphoreType.DMA((rows,)),
            pltpu.SemaphoreType.DMA((ROUNDS, rows)),
        ],
        compiler_params=pltpu.CompilerParams(
            collective_id=0, has_side_effects=True, vmem_limit_bytes=grant
        ),
    )(*operands)
    return pl.pallas_call(
        place,
        out_shape=(
            jax.ShapeDtypeStruct(initial_field.shape, jnp.float32),
            jax.ShapeDtypeStruct((channels, slots), jnp.float32),
        ),
        in_specs=[vmem] * 2,
        out_specs=(hbm, hbm),
        scratch_shapes=[pltpu.SemaphoreType.DMA((2,))],
        compiler_params=pltpu.CompilerParams(vmem_limit_bytes=8 * math.prod(brick)),
    )(field, potential)


def solution(mesh):
    placed = (
        P(None, "row", "col", "gz"),
        P(None, "row", "col", "gz"),
        P("row", "col", "gz"),
        P(),
        P(("row", "col", "gz")),
        P(("row", "col", "gz")),
        P(None, ("row", "col", "gz")),
    )
    return jax.shard_map(
        functools.partial(local, tuple(mesh.shape[axis] for axis in AXES)),
        mesh=mesh,
        in_specs=placed,
        out_specs=(P(None, "row", "col", "gz"), P(None, ("row", "col", "gz"))),
        check_vma=False,
    )
```

```python
import functools
import math

import jax
import jax.numpy as jnp
import numpy as np
from jax import lax
from jax.experimental import pallas as pl
from jax.experimental.pallas import tpu as pltpu
from jax.sharding import PartitionSpec as P

ROUNDS = 2

relax_weight = 0.8
wave_number = 25.0
soften = 0.05
coupling = 0.5

MESH = pl.DeviceIdType.MESH
AXES = ("row", "col", "gz")


def cosine_terms(degree=6):
    nodes = 0.125 * (1.0 + np.cos(np.pi * (np.arange(64) + 0.5) / 64))
    fitted = np.polynomial.Polynomial.fit(
        nodes, np.cos(2 * np.pi * np.sqrt(nodes)), degree, domain=[0.0, 0.25]
    )
    return [float(c) for c in fitted.convert().coef]


COSINE = cosine_terms()


def cosine_of_turns(turns):
    fraction = turns - jnp.floor(turns + 0.5)
    square = fraction * fraction
    value = jnp.full_like(square, COSINE[-1])
    for term in reversed(COSINE[:-1]):
        value = value * square + term
    return value


def relays(sizes):
    rows, cols, depths = sizes
    if cols != 2 or depths != 2 or rows < 2 or rows % 2:
        return []
    stages, far = [[(-1, 0, 0), (1, 0, 0), (0, 1, 0), (0, 0, 1)]], 2
    while far < rows:
        stages.append([(-far, 0, 0), (far, 0, 0)] + ([(0, 1, 1)] if far == 2 else []))
        far *= 2
    stages.append([(0, 1, 1)])

    def at(device, offset):
        r, c, d = (x + o for x, o in zip(device, offset))
        return (r, c % 2, d % 2) if 0 <= r < rows else None

    everyone = [(r, c, d) for r in range(rows) for c in range(2) for d in range(2)]
    known = {x: {x} | {at(x, o) for o in stages[0]} for x in everyone}
    for i, stage in enumerate(stages):
        told = {x: set(known[x]) for x in everyone}
        for x in everyone:
            for offset in stage:
                target = at(x, offset)
                if target is not None:
                    if target not in known[x]:
                        return []
                    told[target] |= known[x]
        known = told
        for x in everyone:
            ahead = {at(x, (r, c, d)) for r in (-1, 0, 1) for c in (0, 1) for d in (0, 1) if abs(r) + c + d < 3}
            ahead |= {at(x, (r, 0, 0)) for r in (-2, 2)}
            if i > 0:
                ahead |= {at(x, (r, c, d)) for r in (-2, 2) for c in (0, 1) for d in (0, 1)}
                ahead |= {at(x, (r, 0, 0)) for r in (-4, 4)}
            if i == len(stages) - 2:
                ahead = {y for y in everyone if (y[0] - x[0]) % 2 == 0}
            if i == len(stages) - 1:
                ahead = set(everyone)
            if not ahead - {None} <= known[x] | {None}:
                return []
    return stages


def kernel(
    sizes,
    init_hbm, source_hbm, class_hbm, shift_hbm, cell_hbm, live_hbm, geo_hbm,
    field_ref, potential_ref,
    init_v, source_v, forcing_v, class_v, weight_v, state_v,
    x_out, x_in, y_out, y_in, z_out, z_in, xy_in, xz_in, yz_in,
    wx_out, wx_in, wy_out, wy_in, wz_out, wz_in, rim_x, rim_y, rim_z,
    rim_wx, rim_wy, rim_wz, meter,
    geo_all, column_v, tile_v, density_out, density_all, at_cell,
    shift_ref, live_ref, cell_ref, geo_ref,
    known, local_sem, face_send, face_recv, gather_send, geo_recv, density_recv,
):
    rows, cols, depths = sizes
    devices = rows * cols * depths
    group = cols * depths
    channels, size_x, size_y, size_z = init_hbm.shape
    slots = cell_hbm.shape[1]
    classes = shift_ref.shape[0]
    factor = 1.0 / math.sqrt(slots * devices)
    here = tuple(lax.axis_index(axis) for axis in AXES)
    me = (here[0] * cols + here[1]) * depths + here[2]

    def brick_copies(hbm, vmem, sem):
        return [
            pltpu.make_async_copy(hbm.at[e], vmem.at[:, :, e, :], sem) for e in range(channels)
        ]

    def brick_wait(vmem, sem):
        pltpu.make_async_copy(vmem, vmem, sem).wait()

    stages = relays(sizes)
    barrier = pltpu.get_barrier_semaphore()

    def offset_place(offset):
        return (
            here[0] + offset[0],
            1 - here[1] if offset[1] else here[1],
            1 - here[2] if offset[2] else here[2],
        )

    def reaches(offset):
        if offset[0] == 0:
            return None
        return here[0] >= -offset[0] if offset[0] < 0 else here[0] + offset[0] < rows

    def tell(sem, offset):
        def go():
            pl.semaphore_signal(
                sem, inc=1, device_id=offset_place(offset), device_id_type=MESH
            )

        present = reaches(offset)
        if present is None:
            go()
        else:
            pl.when(present)(go)

    def tellers(stage):
        return sum(
            1 if reaches(offset) is None else jnp.where(reaches(offset), 1, 0)
            for offset in stages[stage]
        )

    def pass_on(stage):
        for offset in stages[stage]:
            tell(known.at[stage], offset)

    def hear(stage):
        pl.semaphore_wait(known.at[stage], tellers(stage))

    if stages:
        for offset in stages[0]:
            tell(barrier, offset)
        near = tellers(0)
    else:
        near = devices - 1

    for copy in brick_copies(init_hbm, init_v, local_sem.at[0]):
        copy.start()

    copies = [
        pltpu.make_async_copy(class_hbm, class_v, local_sem.at[1]),
        pltpu.make_async_copy(geo_hbm, geo_ref, local_sem.at[3]),
        pltpu.make_async_copy(shift_hbm, shift_ref, local_sem.at[4]),
        pltpu.make_async_copy(cell_hbm, cell_ref, local_sem.at[5]),
        pltpu.make_async_copy(live_hbm, live_ref, local_sem.at[6]),
    ]

    def nearest(k, own, count):
        below, above = own, count - 1 - own
        near = own + jnp.where(lax.rem(k, 2) == 1, (k + 1) // 2, -(k // 2))
        far = jnp.where(below < above, k, count - 1 - k)
        return jnp.where((k <= 2 * below) & (k <= 2 * above), near, far)

    def nth(k):
        return nearest(k, here[0], rows)

    def each_other(action):
        def at(row, first):
            for b in reversed(range(cols)):
                for c in reversed(range(depths)):
                    if first and b == 0 and c == 0:
                        continue
                    action((row, lax.rem(here[1] + b, cols), lax.rem(here[2] + c, depths)))

        def others(i, carry):
            at(nth(rows - 1 - i), False)
            return carry

        lax.fori_loop(0, rows - 1, others, 0)
        at(here[0], True)

    if not stages:
        each_other(
            lambda device: pl.semaphore_signal(
                barrier, inc=1, device_id=device, device_id_type=MESH
            )
        )
    for copy in copies:
        copy.start()
    for copy in brick_copies(source_hbm, source_v, local_sem.at[2]):
        copy.start()

    cell_shape, pair_shape = (channels, size_z), (2 * channels, size_z)
    pairs = size_y // 2
    lane = lax.broadcasted_iota(jnp.int32, pair_shape, 1)
    even = (lane & 1) == 0
    at_pair = lane >> 1
    in_line = lax.rem(at_pair, pairs)
    upper = lax.broadcasted_iota(jnp.int32, pair_shape, 0) < channels
    low_plane = at_pair < pairs
    high_plane = (at_pair >= (size_x - 1) * pairs) & (at_pair < size_x * pairs)
    edge = jnp.where((lane == 0) | (lane == size_z - 1), 1.0, 0.0).astype(jnp.bfloat16)
    slab = (size_y * channels, size_z)
    slab_lane = lax.broadcasted_iota(jnp.int32, slab, 1)

    def turn(value, shift):
        return pltpu.roll(value, shift % size_z, 1)

    def swap(value):
        return jnp.concatenate([value[channels:], value[:channels]], axis=0)

    def planes(ref):
        return [[ref[x, y] for y in range(size_y)] for x in range(size_x)]

    def in_pairs(values):
        return [
            [
                jnp.concatenate([line[y], line[y + 1]], axis=0).astype(jnp.bfloat16)
                for y in range(0, size_y, 2)
            ]
            for line in values
        ]

    def pack_deep(paired):
        packed = jnp.zeros(pair_shape, jnp.bfloat16)
        for x in range(size_x):
            for p in range(pairs):
                packed = packed + turn(paired[x][p] * edge, 2 * (x * pairs + p) + 1)
        return packed

    def pack(q, values):
        paired = in_pairs(values)
        for side, x in ((0, 0), (1, size_x - 1)):
            for p in range(pairs):
                x_out[q, side, p] = paired[x][p]
        for side, y in ((0, 0), (1, size_y - 1)):
            for x in range(0, size_x, 2):
                both = jnp.concatenate([values[x][y], values[x + 1][y]], axis=0)
                y_out[q, side, x // 2] = both.astype(y_out.dtype)
        z_out[q] = pack_deep(paired)

    def exists(axis, up):
        return here[axis] < sizes[axis] - 1 if up else here[axis] > 0

    beside = []
    for axis in range(3):
        if sizes[axis] == 2:
            beside.append((axis, 1 - here[axis], 1 - here[axis], None))
        elif sizes[axis] > 2:
            beside.append((axis, 0, here[axis] - 1, exists(axis, 0)))
            beside.append((axis, 1, here[axis] + 1, exists(axis, 1)))
    edges_beside = [(one, two) for one in beside for two in beside if one[0] < two[0]]
    outs, ins = (x_out, y_out, z_out), (x_in, y_in, z_in)
    edge_ins = {(0, 1): xy_in, (0, 2): xz_in, (1, 2): yz_in}

    def when(present, action):
        if present is None:
            action()
        else:
            pl.when(present)(action)

    def start(source, landing, sem, target, present):
        def go():
            pltpu.make_async_remote_copy(
                src_ref=source,
                dst_ref=landing,
                send_sem=face_send.at[0],
                recv_sem=face_recv.at[sem],
                device_id=target,
                device_id_type=MESH,
            ).start()

        when(present, go)

    def start_faces(q):
        for axis, side, place, present in beside:
            source = outs[axis].at[q] if axis == 2 else outs[axis].at[q, side]
            start(source, ins[axis].at[q, 1 - side], q % 3, {AXES[axis]: place}, present)

    def start_edges(q):
        for (a, side_a, place_a, one), (b, side_b, place_b, two) in edges_beside:
            if (a, b) == (0, 1):
                source = y_out.at[q, side_b, side_a * ((size_x - 1) // 2)]
            else:
                source = z_out.at[q]
            landing = edge_ins[a, b].at[q // 3, 1 - side_a, 1 - side_b]
            present = two if one is None else one if two is None else one & two
            start(source, landing, 3, {AXES[a]: place_a, AXES[b]: place_b}, present)

    def start_weights():
        for axis, side, place, present in beside:
            out, into = ((wx_out, wx_in), (wy_out, wy_in), (wz_out, wz_in))[axis]
            source = out if axis == 2 else out.at[side]
            start(source, into.at[1 - side], 4, {AXES[axis]: place}, present)

    def await_bytes(sem, each):
        split = [axis for axis in range(3) if sizes[axis] > 2]
        for case in range(2 ** len(split)):
            counts = [min(count, 2) - 1 for count in sizes]
            condition = None
            for i, axis in enumerate(split):
                both = (case >> i) & 1
                counts[axis] += both
                holds = (here[axis] > 0) & (here[axis] < sizes[axis] - 1)
                holds = holds if both else jnp.logical_not(holds)
                condition = holds if condition is None else condition & holds
            span = meter.at[pl.ds(0, each(counts))]
            when(condition, lambda span=span: pltpu.make_async_copy(span, span, sem).wait())

    def face_cells(n):
        return n[0] * pairs + n[1] * (size_x // 2) + n[2]

    def edge_cells(n):
        return n[0] * n[1] + n[0] * n[2] + n[1] * n[2]

    def weight_cells(n):
        return n[0] * (size_y // channels) + n[1] + n[2]

    none = 3 * ROUNDS
    x_in[none] = jnp.zeros(x_in.shape[1:], x_in.dtype)
    y_in[none] = jnp.zeros(y_in.shape[1:], y_in.dtype)
    z_in[none] = jnp.zeros(z_in.shape[1:], z_in.dtype)
    for into in edge_ins.values():
        into[ROUNDS] = jnp.zeros(into.shape[1:], into.dtype)
    wx_in[2] = jnp.zeros(wx_in.shape[1:], wx_in.dtype)
    wy_in[2] = jnp.zeros(wy_in.shape[1:], wy_in.dtype)
    wz_in[2] = jnp.zeros(wz_in.shape[1:], wz_in.dtype)

    with jax.named_scope("w_init"):
        brick_wait(init_v, local_sem.at[0])

    pack(0, planes(init_v))

    with jax.named_scope("w_barrier"):
        pl.semaphore_wait(barrier, near)
    if stages:
        pass_on(0)
    start_faces(0)

    copies[1].wait()
    eye = lax.broadcasted_iota(jnp.int32, (slots, slots), 0) == lax.broadcasted_iota(
        jnp.int32, (slots, slots), 1
    )
    for i in range(3):
        column = jnp.sum(jnp.where(eye, geo_ref[i : i + 1, :], 0.0), axis=1, keepdims=True)
        column_v[i] = jnp.broadcast_to(column, (slots, slots))
    pltpu.make_async_copy(geo_ref, geo_all.at[me], geo_recv.at[here[0]]).start()


    fold = 2 - rows % 2
    layers, layer, part = rows // fold, here[0] // fold, lax.rem(here[0], fold)

    def send_geometry(row, b, c):
        pltpu.make_async_remote_copy(
            src_ref=geo_ref,
            dst_ref=geo_all.at[me],
            send_sem=gather_send.at[0],
            recv_sem=geo_recv.at[here[0]],
            device_id=(row, lax.rem(here[1] + b, cols), lax.rem(here[2] + c, depths)),
            device_id_type=MESH,
        ).start()

    others_beside = [(b, c) for b in range(cols) for c in range(depths)]

    def start_geometry(*parts):
        if 0 in parts:
            for b, c in others_beside[1:]:
                send_geometry(here[0], b, c)
        for away in reversed(range(fold, rows, fold)):
            step = min(away // fold, 3)
            targets = others_beside[:1] if step - 1 in parts else []
            targets = targets + (others_beside[1:] if min(step, 2) in parts else [])

            def to_row(row, targets=targets):
                for b, c in targets:
                    send_geometry(row, b, c)

            if targets:
                pl.when(here[0] >= away)(lambda: to_row(here[0] - away))
                pl.when(here[0] + away < rows)(lambda: to_row(here[0] + away))

    def hand_over(q):
        blocks = geo_all.at[pl.ds(q * group, group)]
        pltpu.make_async_remote_copy(
            src_ref=blocks,
            dst_ref=blocks,
            send_sem=gather_send.at[0],
            recv_sem=geo_recv.at[q],
            device_id={"row": layer * fold + (fold - 1 - part)},
            device_id_type=MESH,
        ).start()

    def start_gather(source, gathered, sem):
        def send(device):
            pltpu.make_async_remote_copy(
                src_ref=source,
                dst_ref=gathered.at[me],
                send_sem=gather_send.at[0],
                recv_sem=sem,
                device_id=device,
                device_id_type=MESH,
            ).start()

        each_other(send)

    def await_gather(gathered, count, sem):
        whole = gathered.at[pl.ds(0, count)]
        pltpu.make_async_copy(whole, whole, sem).wait()

    copies[0].wait()
    copies[2].wait()
    for x in range(size_x):
        kind = class_v[x]
        shift = jnp.zeros(kind.shape, jnp.float32)
        for level in range(classes):
            shift = jnp.where(kind == level, shift_ref[level], shift)
        weight = relax_weight / (6.0 + shift)
        weight_v[x] = jnp.broadcast_to(weight[:, None, :], (size_y, channels, size_z))
        if x == 0:
            wx_out[0] = weight
        if x == size_x - 1:
            wx_out[1] = weight
        if x == 0:
            wy_out[...] = jnp.zeros(wy_out.shape, wy_out.dtype)
        wy_out[0, x : x + 1, :] = weight[0:1]
        wy_out[1, x : x + 1, :] = weight[size_y - 1 : size_y]
    wz_out[...] = pack_deep(in_pairs(planes(weight_v)))
    start_weights()

    copies[3].wait()
    copies[4].wait()
    cell = cell_ref[...]
    bits = size_z.bit_length() - 1
    cell_z = cell & (size_z - 1)
    cell_xy = cell >> bits
    pick_z = lax.broadcasted_iota(jnp.int32, (size_z, slots), 0) == cell_z
    pick_z = jnp.where(pick_z, 1.0, 0.0).astype(jnp.bfloat16)
    for at in range(size_x * size_y):
        at_cell[at] = jnp.broadcast_to(
            jnp.where(cell_xy == at, 1.0, 0.0), (channels, slots)
        )
    live = lax.broadcasted_iota(jnp.int32, (channels, slots), 1) < live_ref[...]
    brick_wait(source_v, local_sem.at[2])
    for x in range(size_x):
        forcing_v[0, x] = weight_v[x] * source_v[x]

    def inside(value, above, below):
        blank = jnp.zeros((1,) + cell_shape, jnp.float32)
        around = jnp.concatenate([value[1:], blank], axis=0)
        around = around + jnp.concatenate([blank, value[:-1]], axis=0)
        for other in (above, below):
            if other is not None:
                around = around + other
        flat = value.reshape(slab)
        beside = jnp.where(slab_lane == size_z - 1, 0.0, turn(flat, size_z - 1))
        beside = beside + jnp.where(slab_lane == 0, 0.0, turn(flat, 1))
        return around + beside.reshape(value.shape)

    def ends(beyond, at):
        both = (turn(beyond, -2 * at) * edge).astype(jnp.float32)
        return both[:channels], both[channels:]

    def inner(source, target, force):
        for x in range(size_x):
            value = source[x]
            around = inside(
                value,
                source[x + 1] if x + 1 < size_x else None,
                source[x - 1] if x > 0 else None,
            )
            target[x] = (1.0 - relax_weight) * value + force[x] + weight_v[x] * around

    def pick(axis, q):
        return (
            jnp.where(here[axis] > 0, q, none),
            jnp.where(here[axis] < sizes[axis] - 1, q, none),
        )

    def half_of_pair(i):
        return slice(channels * (i % 2), channels * (i % 2) + channels)

    def from_x(q, side, y):
        both = x_in[pick(0, q)[side], side, y // 2].astype(jnp.float32)
        return both[half_of_pair(y)]

    def from_y(q, side, x):
        both = y_in[pick(1, q)[side], side, x // 2].astype(jnp.float32)
        return both[half_of_pair(x)]

    def either(low, high):
        return jnp.where(even, low.astype(jnp.float32), high.astype(jnp.float32))

    def from_z(q):
        below, above = pick(2, q)
        return either(z_in[below, 0], z_in[above, 1])

    def beside_ends(natural):
        return jnp.where(even, natural, turn(natural, -2)).astype(jnp.bfloat16)

    def corner(a, b, q, side_a, side_b):
        there = exists(a, side_a) & exists(b, side_b)
        return edge_ins[a, b][jnp.where(there, q // 3, ROUNDS), side_a, side_b]

    def corner_xy(q, side_x, side_y):
        both = corner(0, 1, q, side_x, side_y).astype(jnp.float32)
        return both[half_of_pair(size_x - 1 if side_x == 0 else 0)]

    def corner_z(axis, q, side):
        return either(corner(axis, 2, q, side, 0), corner(axis, 2, q, side, 1))

    def outer(target, q):
        beyond = beside_ends(from_z(q))
        for x in range(size_x):
            for p in range(pairs):
                for y, around in zip((2 * p, 2 * p + 1), ends(beyond, x * pairs + p)):
                    if x == 0:
                        around = around + from_x(q, 0, y)
                    if x == size_x - 1:
                        around = around + from_x(q, 1, y)
                    if y == 0:
                        around = around + from_y(q, 0, x)
                    if y == size_y - 1:
                        around = around + from_y(q, 1, x)
                    target[x, y] = target[x, y] + weight_v[x, y] * around

    def spread_weights():
        for side in (0, 1):
            weight = wx_in[jnp.where(exists(0, side), side, 2)]
            rim_wx[side] = jnp.broadcast_to(weight[:, None, :], (size_y,) + cell_shape)
            weight = wy_in[jnp.where(exists(1, side), side, 2)][:size_x]
            rim_wy[side] = jnp.broadcast_to(weight[:, None, :], (size_x,) + cell_shape)
        rim_wz[...] = either(
            wz_in[jnp.where(exists(2, 0), 0, 2)], wz_in[jnp.where(exists(2, 1), 1, 2)]
        )

    def own_rim(source, q):
        for side in (0, 1):
            rim_x[side] = rim_wx[side] * source[(size_x - 1) * side]
            for x in range(size_x):
                rim_y[side, x] = rim_wy[side, x] * source[x, (size_y - 1) * side]
        own = z_out[q].astype(jnp.float32)
        rim_z[...] = rim_wz[...] * jnp.where(even, turn(own, -1), turn(own, 1))

    def rim(target, q):
        along, across = (size_x - 1) * size_y, 2 * (pairs - 1)
        around = jnp.where(low_plane, turn(corner_z(0, q, 0), -along), 0.0)
        around = around + jnp.where(high_plane, turn(corner_z(0, q, 1), along), 0.0)
        first = upper & (in_line == 0)
        final = jnp.logical_not(upper) & (in_line == pairs - 1)
        around = around + jnp.where(first, swap(turn(corner_z(1, q, 0), -across)), 0.0)
        around = around + jnp.where(final, swap(turn(corner_z(1, q, 1), across)), 0.0)
        beyond = beside_ends(rim_z[...] + rim_wz[...] * around + from_z(q + 1))
        beyond_x = [beside_ends(corner_z(0, q, side)) for side in (0, 1)]
        beyond_y = [beside_ends(corner_z(1, q, side)) for side in (0, 1)]

        def swept_x(side, p):
            found = []
            theirs = (size_x - 1) * (1 - side)
            for y, around in zip((2 * p, 2 * p + 1), ends(beyond_x[side], theirs * pairs + p)):
                if y == 0:
                    around = around + corner_xy(q, side, 0)
                if y == size_y - 1:
                    around = around + corner_xy(q, side, 1)
                found.append(rim_x[side, y] + from_x(q + 1, side, y) + rim_wx[side, y] * around)
            return found

        def swept_y(side, x):
            theirs = (size_y - 1) * (1 - side)
            around = ends(beyond_y[side], x * pairs + theirs // 2)[theirs % 2]
            if x == 0:
                around = around + corner_xy(q, 0, side)
            if x == size_x - 1:
                around = around + corner_xy(q, 1, side)
            return rim_y[side, x] + from_y(q + 1, side, x) + rim_wy[side, x] * around

        cells = []
        for x in range(size_x):
            for p in range(pairs):
                below = swept_x(0, p) if x == 0 else None
                above = swept_x(1, p) if x == size_x - 1 else None
                for i, around in enumerate(ends(beyond, x * pairs + p)):
                    y = 2 * p + i
                    if below:
                        around = around + below[i]
                    if above:
                        around = around + above[i]
                    if y == 0:
                        around = around + swept_y(0, x)
                    if y == size_y - 1:
                        around = around + swept_y(1, x)
                    cell = target[x, y] + weight_v[x, y] * around
                    target[x, y] = cell
                    cells.append(cell)
        return cells

    def sum_up(found):
        sums = [block * at_cell[at] for at, block in enumerate(found)]
        while len(sums) > 1:
            sums = [a + b for a, b in zip(sums[::2], sums[1::2])]
        return sums[0]

    pieces = 4
    chunk = slots // pieces

    def make_tiles():
        def body(i, carry):
            a, k = i // layers, lax.rem(i, layers)
            q = nearest(k, layer, layers) * fold + lax.rem(part + a, fold)
            await_gather(geo_all, group, geo_recv.at[q])
            if fold > 1:
                pl.when(a == 0)(lambda: hand_over(q))
            for j in range(group):
                source = geo_all[q * group + j]
                for piece in range(pieces):
                    span = slice(piece * chunk, (piece + 1) * chunk)
                    delta_x = column_v[0, span, :] - source[0:1, :]
                    delta_y = column_v[1, span, :] - source[1:2, :]
                    delta_z = column_v[2, span, :] - source[2:3, :]
                    square = delta_x * delta_x + delta_y * delta_y + delta_z * delta_z + 1e-30
                    distance = square * lax.rsqrt(square)
                    wave = cosine_of_turns(distance * (wave_number / (2.0 * math.pi)))
                    value = (source[3:4, :] * factor) * wave / (distance + soften)
                    tile_v[q, span, j * slots : (j + 1) * slots] = value.astype(tile_v.dtype)
            return carry

        lax.fori_loop(0, rows, body, 0)

    def apply_tiles(r):
        total = jnp.zeros((channels, slots), jnp.float32)
        for k in range(rows):
            q = nth(k)
            with jax.named_scope(f"w_dens{r}_{k}"):
                await_gather(density_all.at[r], group - (k == 0), density_recv.at[r, q])
            values = jnp.concatenate(
                [density_all[r, q * group + j] for j in range(group)], axis=1
            )
            total = total + lax.dot_general(
                values, tile_v[q], (((1,), (1,)), ((), ())), preferred_element_type=jnp.float32
            )
        return total

    def land(sem, each):
        await_bytes(face_recv.at[sem], each)

    def drain(each):
        await_bytes(face_send.at[0], each)

    def drain_now():
        for q in range(3 * ROUNDS - 2):
            drain(face_cells)
            if q % 3 == 1:
                drain(edge_cells)
        drain(weight_cells)
        await_gather(geo_all, devices - 1, gather_send.at[0])
        for r in range(ROUNDS - 1):
            await_gather(density_all.at[r], devices - 1, gather_send.at[0])

    for r in range(ROUNDS):
        single, double = 3 * r, 3 * r + 1
        before = init_v if r == 0 else state_v.at[2]
        once, mid, after = state_v.at[0], state_v.at[1], state_v.at[2]
        if r == ROUNDS - 1:
            after = field_ref
        force = forcing_v.at[r]
        with jax.named_scope(f"inner{r}"):
            inner(before, once, forcing_v.at[0])
        if r > 0:
            with jax.named_scope("tilesB"):
                make_tiles()
        if r == 0:
            with jax.named_scope("w_known0"):
                early = stages[1:-2]
                if stages:
                    hear(0)
                    pass_on(1)
                    start_geometry(0)
                    if early:
                        hear(1)
                        pass_on(2)
                        start_geometry(1)
                else:
                    start_geometry(0, 1, 2)
        with jax.named_scope(f"w_single{r}"):
            land(0, face_cells)
        if r == 0 and stages:
            for stage in range(2, len(stages) - 2):
                hear(stage)
                pass_on(stage + 1)
        with jax.named_scope(f"outer{r}"):
            outer(once, single)
        if r > 0:
            with jax.named_scope(f"apply{r-1}"):
                potential = jnp.where(live, apply_tiles(r - 1), 0.0)
            with jax.named_scope(f"load{r}"):
                half_of = coupling * potential
                big = half_of.astype(jnp.bfloat16).astype(jnp.float32)
                small = half_of - big
                placed = jnp.concatenate(
                    [(at_cell[...] * part[None]).astype(jnp.bfloat16) for part in (big, small)],
                    axis=2,
                ).reshape(size_x * size_y * channels, 2 * slots)
                load = lax.dot_general(
                    placed, jnp.concatenate([pick_z, pick_z], axis=1),
                    (((1,), (1,)), ((), ())), preferred_element_type=jnp.float32,
                )
                load = load.reshape(size_x, size_y, channels, size_z)
                for x in range(size_x):
                    change = weight_v[x] * load[x]
                    force[x] = forcing_v[0, x] + change
                    once[x] = once[x] + change
        with jax.named_scope(f"pack{r}"):
            pack(double, planes(once))
        start_edges(double)
        start_faces(double)
        with jax.named_scope(f"innerd{r}"):
            inner(once, mid, force)
        with jax.named_scope(f"packd{r}"):
            pack(double + 1, planes(mid))
        start_faces(double + 1)
        if r == 0:
            with jax.named_scope("w_weights"):
                land(4, weight_cells)
                spread_weights()
            with jax.named_scope("w_known"):
                if stages:
                    hear(len(stages) - 2)
                    pass_on(len(stages) - 1)
            with jax.named_scope("st_geo"):
                if stages:
                    start_geometry(*((2,) if early else (1, 2)))
        else:
            drain_now()
        own_rim(once, double)
        with jax.named_scope(f"w_double{r}"):
            land(1, face_cells)
        with jax.named_scope(f"outerd{r}"):
            outer(mid, double)
            inner(mid, after, force)
        with jax.named_scope(f"w_edges{r}"):
            land(3, edge_cells)
        with jax.named_scope(f"w_rim{r}"):
            land(2, face_cells)
        with jax.named_scope(f"rim{r}"):
            cells = rim(after, double)
            parts = [jnp.dot(jnp.concatenate(cells[x * size_y : (x + 1) * size_y], axis=0).astype(jnp.bfloat16), pick_z, preferred_element_type=jnp.float32) for x in range(size_x)]
            density = sum_up([found[channels * i : channels * (i + 1)] for found in parts for i in range(found.shape[0] // channels)])
            density = jnp.where(live, density, 0.0).astype(jnp.bfloat16)
            density_out[r] = density
            density_all[r, me] = density
        if r == 0 and stages:
            hear(len(stages) - 1)
        with jax.named_scope(f"st_dens{r}"):
            start_gather(density_out.at[r], density_all.at[r], density_recv.at[r, here[0]])
        if r < ROUNDS - 1:
            with jax.named_scope(f"pack_s{r}"):
                pack(single + 3, planes(after))
            start_faces(single + 3)
    drain(face_cells)
    drain(edge_cells)
    drain(face_cells)
    with jax.named_scope(f"apply{ROUNDS-1}"):
        potential_ref[...] = jnp.where(live, apply_tiles(ROUNDS - 1), 0.0)

    with jax.named_scope("finish"):
        await_gather(density_all.at[ROUNDS - 1], devices - 1, gather_send.at[0])


def place(field_v, potential_v, field_hbm, potential_hbm, sem):
    channels = field_hbm.shape[0]
    copies = [
        pltpu.make_async_copy(field_v.at[:, :, e, :], field_hbm.at[e], sem.at[0])
        for e in range(channels)
    ]
    copies.append(pltpu.make_async_copy(potential_v, potential_hbm, sem.at[1]))
    for copy in copies:
        copy.start()
    pltpu.make_async_copy(field_v, field_v, sem.at[0]).wait()
    copies[-1].wait()


def local(sizes, initial_field, source_term, cell_class, class_shift, surface_cell, live_count,
          panel_geometry):
    channels, size_x, size_y, size_z = initial_field.shape
    slots = surface_cell.shape[0]
    rows, cols, depths = sizes
    devices, group = rows * cols * depths, cols * depths
    brick = (size_x, size_y, channels, size_z)
    vmem = pl.BlockSpec(memory_space=pltpu.VMEM)
    hbm = pl.BlockSpec(memory_space=pltpu.HBM)
    per_device = slots * (2 * slots + 4 * 8 + ROUNDS * 2 * 2 * channels)
    grant = devices * per_device + 36 * 4 * math.prod(brick)
    operands = [
        pltpu.with_memory_space_constraint(array, pltpu.HBM)
        for array in (
            initial_field, source_term, cell_class, class_shift,
            surface_cell.reshape(1, slots), panel_geometry,
        )
    ]
    operands.insert(5, live_count.reshape(1, 1))
    two, turns = 2 * channels, 3 * ROUNDS
    field, potential = pl.pallas_call(
        functools.partial(kernel, sizes),
        out_shape=(
            jax.ShapeDtypeStruct(brick, jnp.float32),
            jax.ShapeDtypeStruct((channels, slots), jnp.float32),
        ),
        in_specs=[hbm] * 5 + [pl.BlockSpec(memory_space=pl.ANY), hbm],
        out_specs=(vmem, vmem),
        scratch_shapes=[
            pltpu.VMEM(brick, jnp.float32),
            pltpu.VMEM(brick, jnp.float32),
            pltpu.VMEM((ROUNDS,) + brick, jnp.float32),
            pltpu.VMEM((size_x, size_y, size_z), jnp.int32),
            pltpu.VMEM(brick, jnp.float32),
            pltpu.VMEM((3,) + brick, jnp.float32),
            pltpu.VMEM((turns, 2, size_y // 2, two, size_z), jnp.bfloat16),
            pltpu.VMEM((turns + 1, 2, size_y // 2, two, size_z), jnp.bfloat16),
            pltpu.VMEM((turns, 2, size_x // 2, two, size_z), jnp.bfloat16),
            pltpu.VMEM((turns + 1, 2, size_x // 2, two, size_z), jnp.bfloat16),
            pltpu.VMEM((turns, two, size_z), jnp.bfloat16),
            pltpu.VMEM((turns + 1, 2, two, size_z), jnp.bfloat16),
            pltpu.VMEM((ROUNDS + 1, 2, 2, two, size_z), jnp.bfloat16),
            pltpu.VMEM((ROUNDS + 1, 2, 2, two, size_z), jnp.bfloat16),
            pltpu.VMEM((ROUNDS + 1, 2, 2, two, size_z), jnp.bfloat16),
            pltpu.VMEM((2, size_y, size_z), jnp.float32),
            pltpu.VMEM((3, size_y, size_z), jnp.float32),
            pltpu.VMEM((2, channels, size_z), jnp.float32),
            pltpu.VMEM((3, channels, size_z), jnp.float32),
            pltpu.VMEM((two, size_z), jnp.bfloat16),
            pltpu.VMEM((3, two, size_z), jnp.bfloat16),
            pltpu.VMEM((2, size_y, channels, size_z), jnp.float32),
            pltpu.VMEM((2, size_x, channels, size_z), jnp.float32),
            pltpu.VMEM((two, size_z), jnp.float32),
            pltpu.VMEM((2, size_y, channels, size_z), jnp.float32),
            pltpu.VMEM((2, size_x, channels, size_z), jnp.float32),
            pltpu.VMEM((two, size_z), jnp.float32),
            pltpu.VMEM((size_y + size_x + 2, channels, size_z), jnp.float32),
            pltpu.VMEM((devices, 4, slots), jnp.float32),
            pltpu.VMEM((3, slots, slots), jnp.float32),
            pltpu.VMEM((rows, slots, group * slots), jnp.bfloat16),
            pltpu.VMEM((ROUNDS, channels, slots), jnp.bfloat16),
            pltpu.VMEM((ROUNDS, devices, channels, slots), jnp.bfloat16),
            pltpu.VMEM((size_x * size_y, channels, slots), jnp.float32),
            pltpu.SMEM(class_shift.shape, jnp.float32),
            pltpu.VMEM((1, 1), jnp.int32),
            pltpu.VMEM((1, slots), jnp.int32),
            pltpu.VMEM(panel_geometry.shape, jnp.float32),
            pltpu.SemaphoreType.REGULAR((max(1, len(relays(sizes))),)),
            pltpu.SemaphoreType.DMA((7,)),
            pltpu.SemaphoreType.DMA((1,)),
            pltpu.SemaphoreType.DMA((5,)),
            pltpu.SemaphoreType.DMA((1,)),
            pltpu.SemaphoreType.DMA((rows,)),
            pltpu.SemaphoreType.DMA((ROUNDS, rows)),
        ],
        compiler_params=pltpu.CompilerParams(
            collective_id=0, has_side_effects=True, vmem_limit_bytes=grant
        ),
    )(*operands)
    return pl.pallas_call(
        place,
        out_shape=(
            jax.ShapeDtypeStruct(initial_field.shape, jnp.float32),
            jax.ShapeDtypeStruct((channels, slots), jnp.float32),
        ),
        in_specs=[vmem] * 2,
        out_specs=(hbm, hbm),
        scratch_shapes=[pltpu.SemaphoreType.DMA((2,))],
        compiler_params=pltpu.CompilerParams(vmem_limit_bytes=8 * math.prod(brick)),
    )(field, potential)


def solution(mesh):
    placed = (
        P(None, "row", "col", "gz"),
        P(None, "row", "col", "gz"),
        P("row", "col", "gz"),
        P(),
        P(("row", "col", "gz")),
        P(("row", "col", "gz")),
        P(None, ("row", "col", "gz")),
    )
    return jax.shard_map(
        functools.partial(local, tuple(mesh.shape[axis] for axis in AXES)),
        mesh=mesh,
        in_specs=placed,
        out_specs=(P(None, "row", "col", "gz"), P(None, ("row", "col", "gz"))),
        check_vma=False,
    )
```

```python
import functools
import math

import jax
import jax.numpy as jnp
import numpy as np
from jax import lax
from jax.experimental import pallas as pl
from jax.experimental.pallas import tpu as pltpu
from jax.sharding import PartitionSpec as P

ROUNDS = 2

relax_weight = 0.8
wave_number = 25.0
soften = 0.05
coupling = 0.5

MESH = pl.DeviceIdType.MESH
AXES = ("row", "col", "gz")


def cosine_terms(degree=6):
    nodes = 0.125 * (1.0 + np.cos(np.pi * (np.arange(64) + 0.5) / 64))
    fitted = np.polynomial.Polynomial.fit(
        nodes, np.cos(2 * np.pi * np.sqrt(nodes)), degree, domain=[0.0, 0.25]
    )
    return [float(c) for c in fitted.convert().coef]


COSINE = cosine_terms()


def cosine_of_turns(turns):
    fraction = turns - jnp.floor(turns + 0.5)
    square = fraction * fraction
    value = jnp.full_like(square, COSINE[-1])
    for term in reversed(COSINE[:-1]):
        value = value * square + term
    return value


def relays(sizes):
    rows, cols, depths = sizes
    if cols != 2 or depths != 2 or rows < 2 or rows % 2:
        return []
    stages, far = [[(-1, 0, 0), (1, 0, 0), (0, 1, 0), (0, 0, 1)]], 2
    while far < rows:
        stages.append([(-far, 0, 0), (far, 0, 0)] + ([(0, 1, 1)] if far == 2 else []))
        far *= 2
    stages.append([(0, 1, 1)])

    def at(device, offset):
        r, c, d = (x + o for x, o in zip(device, offset))
        return (r, c % 2, d % 2) if 0 <= r < rows else None

    everyone = [(r, c, d) for r in range(rows) for c in range(2) for d in range(2)]
    known = {x: {x} | {at(x, o) for o in stages[0]} for x in everyone}
    for i, stage in enumerate(stages):
        told = {x: set(known[x]) for x in everyone}
        for x in everyone:
            for offset in stage:
                target = at(x, offset)
                if target is not None:
                    if target not in known[x]:
                        return []
                    told[target] |= known[x]
        known = told
        for x in everyone:
            ahead = {at(x, (r, c, d)) for r in (-1, 0, 1) for c in (0, 1) for d in (0, 1) if abs(r) + c + d < 3}
            ahead |= {at(x, (r, 0, 0)) for r in (-2, 2)}
            if i > 0:
                ahead |= {at(x, (r, c, d)) for r in (-2, 2) for c in (0, 1) for d in (0, 1)}
                ahead |= {at(x, (r, 0, 0)) for r in (-4, 4)}
            if i == len(stages) - 2:
                ahead = {y for y in everyone if (y[0] - x[0]) % 2 == 0}
            if i == len(stages) - 1:
                ahead = set(everyone)
            if not ahead - {None} <= known[x] | {None}:
                return []
    return stages


def kernel(
    sizes,
    init_hbm, source_hbm, class_hbm, shift_hbm, cell_hbm, live_hbm, geo_hbm,
    field_ref, potential_ref,
    init_v, source_v, forcing_v, class_v, weight_v, state_v,
    x_out, x_in, y_out, y_in, z_out, z_in, xy_in, xz_in, yz_in,
    wx_out, wx_in, wy_out, wy_in, wz_out, wz_in, rim_x, rim_y, rim_z,
    rim_wx, rim_wy, rim_wz, meter,
    geo_all, column_v, tile_v, density_out, density_all, at_cell,
    shift_ref, live_ref, cell_ref, geo_ref,
    known, local_sem, face_send, face_recv, gather_send, geo_relay, geo_recv, density_recv,
):
    rows, cols, depths = sizes
    devices = rows * cols * depths
    group = cols * depths
    channels, size_x, size_y, size_z = init_hbm.shape
    slots = cell_hbm.shape[1]
    classes = shift_ref.shape[0]
    factor = 1.0 / math.sqrt(slots * devices)
    here = tuple(lax.axis_index(axis) for axis in AXES)
    me = (here[0] * cols + here[1]) * depths + here[2]

    def brick_copies(hbm, vmem, sem):
        return [
            pltpu.make_async_copy(hbm.at[e], vmem.at[:, :, e, :], sem) for e in range(channels)
        ]

    def brick_wait(vmem, sem):
        pltpu.make_async_copy(vmem, vmem, sem).wait()

    stages = relays(sizes)
    barrier = pltpu.get_barrier_semaphore()

    def offset_place(offset):
        return (
            here[0] + offset[0],
            1 - here[1] if offset[1] else here[1],
            1 - here[2] if offset[2] else here[2],
        )

    def reaches(offset):
        if offset[0] == 0:
            return None
        return here[0] >= -offset[0] if offset[0] < 0 else here[0] + offset[0] < rows

    def tell(sem, offset):
        def go():
            pl.semaphore_signal(
                sem, inc=1, device_id=offset_place(offset), device_id_type=MESH
            )

        present = reaches(offset)
        if present is None:
            go()
        else:
            pl.when(present)(go)

    def tellers(stage):
        return sum(
            1 if reaches(offset) is None else jnp.where(reaches(offset), 1, 0)
            for offset in stages[stage]
        )

    def pass_on(stage):
        for offset in stages[stage]:
            tell(known.at[stage], offset)

    def hear(stage):
        pl.semaphore_wait(known.at[stage], tellers(stage))

    if stages:
        for offset in stages[0]:
            tell(barrier, offset)
        near = tellers(0)
    else:
        near = devices - 1

    for copy in brick_copies(init_hbm, init_v, local_sem.at[0]):
        copy.start()

    copies = [
        pltpu.make_async_copy(class_hbm, class_v, local_sem.at[1]),
        pltpu.make_async_copy(geo_hbm, geo_ref, local_sem.at[3]),
        pltpu.make_async_copy(shift_hbm, shift_ref, local_sem.at[4]),
        pltpu.make_async_copy(cell_hbm, cell_ref, local_sem.at[5]),
        pltpu.make_async_copy(live_hbm, live_ref, local_sem.at[6]),
    ]

    def nearest(k, own, count):
        below, above = own, count - 1 - own
        near = own + jnp.where(lax.rem(k, 2) == 1, (k + 1) // 2, -(k // 2))
        far = jnp.where(below < above, k, count - 1 - k)
        return jnp.where((k <= 2 * below) & (k <= 2 * above), near, far)

    def nth(k):
        return nearest(k, here[0], rows)

    def each_other(action):
        def at(row, first):
            for b in reversed(range(cols)):
                for c in reversed(range(depths)):
                    if first and b == 0 and c == 0:
                        continue
                    action((row, lax.rem(here[1] + b, cols), lax.rem(here[2] + c, depths)))

        def others(i, carry):
            at(nth(rows - 1 - i), False)
            return carry

        lax.fori_loop(0, rows - 1, others, 0)
        at(here[0], True)

    if not stages:
        each_other(
            lambda device: pl.semaphore_signal(
                barrier, inc=1, device_id=device, device_id_type=MESH
            )
        )
    for copy in copies:
        copy.start()
    for copy in brick_copies(source_hbm, source_v, local_sem.at[2]):
        copy.start()

    cell_shape, pair_shape = (channels, size_z), (2 * channels, size_z)
    pairs = size_y // 2
    lane = lax.broadcasted_iota(jnp.int32, pair_shape, 1)
    even = (lane & 1) == 0
    at_pair = lane >> 1
    in_line = lax.rem(at_pair, pairs)
    upper = lax.broadcasted_iota(jnp.int32, pair_shape, 0) < channels
    low_plane = at_pair < pairs
    high_plane = (at_pair >= (size_x - 1) * pairs) & (at_pair < size_x * pairs)
    edge = jnp.where((lane == 0) | (lane == size_z - 1), 1.0, 0.0).astype(jnp.bfloat16)
    slab = (size_y * channels, size_z)
    slab_lane = lax.broadcasted_iota(jnp.int32, slab, 1)

    def turn(value, shift):
        return pltpu.roll(value, shift % size_z, 1)

    def swap(value):
        return jnp.concatenate([value[channels:], value[:channels]], axis=0)

    def planes(ref):
        return [[ref[x, y] for y in range(size_y)] for x in range(size_x)]

    def in_pairs(values):
        return [
            [
                jnp.concatenate([line[y], line[y + 1]], axis=0).astype(jnp.bfloat16)
                for y in range(0, size_y, 2)
            ]
            for line in values
        ]

    def pack_deep(paired):
        packed = jnp.zeros(pair_shape, jnp.bfloat16)
        for x in range(size_x):
            for p in range(pairs):
                packed = packed + turn(paired[x][p] * edge, 2 * (x * pairs + p) + 1)
        return packed

    def pack(q, values):
        paired = in_pairs(values)
        for side, x in ((0, 0), (1, size_x - 1)):
            for p in range(pairs):
                x_out[q, side, p] = paired[x][p]
        for side, y in ((0, 0), (1, size_y - 1)):
            for x in range(0, size_x, 2):
                both = jnp.concatenate([values[x][y], values[x + 1][y]], axis=0)
                y_out[q, side, x // 2] = both.astype(y_out.dtype)
        z_out[q] = pack_deep(paired)

    def exists(axis, up):
        return here[axis] < sizes[axis] - 1 if up else here[axis] > 0

    beside = []
    for axis in range(3):
        if sizes[axis] == 2:
            beside.append((axis, 1 - here[axis], 1 - here[axis], None))
        elif sizes[axis] > 2:
            beside.append((axis, 0, here[axis] - 1, exists(axis, 0)))
            beside.append((axis, 1, here[axis] + 1, exists(axis, 1)))
    edges_beside = [(one, two) for one in beside for two in beside if one[0] < two[0]]
    outs, ins = (x_out, y_out, z_out), (x_in, y_in, z_in)
    edge_ins = {(0, 1): xy_in, (0, 2): xz_in, (1, 2): yz_in}

    def when(present, action):
        if present is None:
            action()
        else:
            pl.when(present)(action)

    def start(source, landing, sem, target, present):
        def go():
            pltpu.make_async_remote_copy(
                src_ref=source,
                dst_ref=landing,
                send_sem=face_send.at[0],
                recv_sem=face_recv.at[sem],
                device_id=target,
                device_id_type=MESH,
            ).start()

        when(present, go)

    def start_faces(q):
        for axis, side, place, present in beside:
            source = outs[axis].at[q] if axis == 2 else outs[axis].at[q, side]
            start(source, ins[axis].at[q, 1 - side], q % 3, {AXES[axis]: place}, present)

    def start_edges(q):
        for (a, side_a, place_a, one), (b, side_b, place_b, two) in edges_beside:
            if (a, b) == (0, 1):
                source = y_out.at[q, side_b, side_a * ((size_x - 1) // 2)]
            else:
                source = z_out.at[q]
            landing = edge_ins[a, b].at[q // 3, 1 - side_a, 1 - side_b]
            present = two if one is None else one if two is None else one & two
            start(source, landing, 3, {AXES[a]: place_a, AXES[b]: place_b}, present)

    def start_weights():
        for axis, side, place, present in beside:
            out, into = ((wx_out, wx_in), (wy_out, wy_in), (wz_out, wz_in))[axis]
            source = out if axis == 2 else out.at[side]
            start(source, into.at[1 - side], 4, {AXES[axis]: place}, present)

    def await_bytes(sem, each):
        split = [axis for axis in range(3) if sizes[axis] > 2]
        for case in range(2 ** len(split)):
            counts = [min(count, 2) - 1 for count in sizes]
            condition = None
            for i, axis in enumerate(split):
                both = (case >> i) & 1
                counts[axis] += both
                holds = (here[axis] > 0) & (here[axis] < sizes[axis] - 1)
                holds = holds if both else jnp.logical_not(holds)
                condition = holds if condition is None else condition & holds
            span = meter.at[pl.ds(0, each(counts))]
            when(condition, lambda span=span: pltpu.make_async_copy(span, span, sem).wait())

    def face_cells(n):
        return n[0] * pairs + n[1] * (size_x // 2) + n[2]

    def edge_cells(n):
        return n[0] * n[1] + n[0] * n[2] + n[1] * n[2]

    def weight_cells(n):
        return n[0] * (size_y // channels) + n[1] + n[2]

    none = 3 * ROUNDS
    x_in[none] = jnp.zeros(x_in.shape[1:], x_in.dtype)
    y_in[none] = jnp.zeros(y_in.shape[1:], y_in.dtype)
    z_in[none] = jnp.zeros(z_in.shape[1:], z_in.dtype)
    for into in edge_ins.values():
        into[ROUNDS] = jnp.zeros(into.shape[1:], into.dtype)
    wx_in[2] = jnp.zeros(wx_in.shape[1:], wx_in.dtype)
    wy_in[2] = jnp.zeros(wy_in.shape[1:], wy_in.dtype)
    wz_in[2] = jnp.zeros(wz_in.shape[1:], wz_in.dtype)

    with jax.named_scope("w_init"):
        brick_wait(init_v, local_sem.at[0])

    pack(0, planes(init_v))

    with jax.named_scope("w_barrier"):
        pl.semaphore_wait(barrier, near)
    if stages:
        pass_on(0)
    start_faces(0)

    copies[1].wait()
    eye = lax.broadcasted_iota(jnp.int32, (slots, slots), 0) == lax.broadcasted_iota(
        jnp.int32, (slots, slots), 1
    )
    for i in range(3):
        column = jnp.sum(jnp.where(eye, geo_ref[i : i + 1, :], 0.0), axis=1, keepdims=True)
        column_v[i] = jnp.broadcast_to(column, (slots, slots))
    pltpu.make_async_copy(geo_ref, geo_all.at[me], geo_recv.at[here[0]]).start()


    fold = 2 - rows % 2
    layers, layer, part = rows // fold, here[0] // fold, lax.rem(here[0], fold)

    handed_on = len(stages) > 3 and layers <= 4

    def send_geometry(row, b, c, sem=None):
        pltpu.make_async_remote_copy(
            src_ref=geo_ref,
            dst_ref=geo_all.at[me],
            send_sem=gather_send.at[0],
            recv_sem=geo_recv.at[here[0]] if sem is None else sem,
            device_id=(row, lax.rem(here[1] + b, cols), lax.rem(here[2] + c, depths)),
            device_id_type=MESH,
        ).start()

    others_beside = [(b, c) for b in range(cols) for c in range(depths)]

    def start_geometry(*parts):
        if 0 in parts:
            for b, c in others_beside[1:]:
                send_geometry(here[0], b, c)
        for away in reversed(range(fold, rows, fold)):
            step = min(away // fold, 3)
            down = others_beside[:1] if step - 1 in parts else []
            down = down + (others_beside[1:] if min(step, 2) in parts else [])
            up, sem = down, None
            if handed_on and step > 1:
                up, sem = (others_beside[:1] if step == 2 and 1 in parts else []), geo_relay.at[0]

            def to_row(row, targets, sem):
                for b, c in targets:
                    send_geometry(row, b, c, sem)

            if down:
                pl.when(here[0] >= away)(
                    functools.partial(to_row, here[0] - away, down, None)
                )
            if up:
                pl.when(here[0] + away < rows)(
                    functools.partial(to_row, here[0] + away, up, sem)
                )

    def hand_on():
        def pass_block(q, onward):
            block = geo_all.at[(q * cols + here[1]) * depths + here[2]]
            pltpu.make_async_copy(block, block, geo_relay.at[0]).wait()

            def send(row, b, c):
                pltpu.make_async_remote_copy(
                    src_ref=block,
                    dst_ref=block,
                    send_sem=gather_send.at[0],
                    recv_sem=geo_recv.at[q],
                    device_id=(
                        row, lax.rem(here[1] + b, cols), lax.rem(here[2] + c, depths)
                    ),
                    device_id_type=MESH,
                ).start()

            def send_onward():
                for b, c in others_beside:
                    send(onward, b, c)

            pl.when(onward < rows)(send_onward)
            for b, c in others_beside[1:]:
                send(here[0], b, c)

        two = 2 * fold
        pl.when(here[0] >= two)(lambda: pass_block(here[0] - two, here[0] + fold))

    def drain_geometry():
        def spent(count, present=None):
            when(present, lambda: await_gather(geo_all, count, gather_send.at[0]))

        if not handed_on:
            spent(devices - 1)
            return
        spent(layers * group)
        spent(group - 1)
        for n in range(1, layers):
            spent(group, here[0] >= n * fold)
            if n < 3:
                spent(group if n == 1 else 1, here[0] + n * fold < rows)
        two = 2 * fold
        spent(group - 1, here[0] >= two)
        spent(group, (here[0] >= two) & (here[0] + fold < rows))

    def hand_over(q):
        blocks = geo_all.at[pl.ds(q * group, group)]
        pltpu.make_async_remote_copy(
            src_ref=blocks,
            dst_ref=blocks,
            send_sem=gather_send.at[0],
            recv_sem=geo_recv.at[q],
            device_id={"row": layer * fold + (fold - 1 - part)},
            device_id_type=MESH,
        ).start()

    def start_gather(source, gathered, sem):
        def send(device):
            pltpu.make_async_remote_copy(
                src_ref=source,
                dst_ref=gathered.at[me],
                send_sem=gather_send.at[0],
                recv_sem=sem,
                device_id=device,
                device_id_type=MESH,
            ).start()

        each_other(send)

    def await_gather(gathered, count, sem):
        whole = gathered.at[pl.ds(0, count)]
        pltpu.make_async_copy(whole, whole, sem).wait()

    copies[0].wait()
    copies[2].wait()
    for x in range(size_x):
        kind = class_v[x]
        shift = jnp.zeros(kind.shape, jnp.float32)
        for level in range(classes):
            shift = jnp.where(kind == level, shift_ref[level], shift)
        weight = relax_weight / (6.0 + shift)
        weight_v[x] = jnp.broadcast_to(weight[:, None, :], (size_y, channels, size_z))
        if x == 0:
            wx_out[0] = weight
        if x == size_x - 1:
            wx_out[1] = weight
        if x == 0:
            wy_out[...] = jnp.zeros(wy_out.shape, wy_out.dtype)
        wy_out[0, x : x + 1, :] = weight[0:1]
        wy_out[1, x : x + 1, :] = weight[size_y - 1 : size_y]
    wz_out[...] = pack_deep(in_pairs(planes(weight_v)))
    start_weights()

    copies[3].wait()
    copies[4].wait()
    cell = cell_ref[...]
    bits = size_z.bit_length() - 1
    cell_z = cell & (size_z - 1)
    cell_xy = cell >> bits
    pick_z = lax.broadcasted_iota(jnp.int32, (size_z, slots), 0) == cell_z
    pick_z = jnp.where(pick_z, 1.0, 0.0).astype(jnp.bfloat16)
    for at in range(size_x * size_y):
        at_cell[at] = jnp.broadcast_to(
            jnp.where(cell_xy == at, 1.0, 0.0), (channels, slots)
        )
    live = lax.broadcasted_iota(jnp.int32, (channels, slots), 1) < live_ref[...]
    brick_wait(source_v, local_sem.at[2])
    for x in range(size_x):
        forcing_v[0, x] = weight_v[x] * source_v[x]

    def inside(value, above, below):
        blank = jnp.zeros((1,) + cell_shape, jnp.float32)
        around = jnp.concatenate([value[1:], blank], axis=0)
        around = around + jnp.concatenate([blank, value[:-1]], axis=0)
        for other in (above, below):
            if other is not None:
                around = around + other
        flat = value.reshape(slab)
        beside = jnp.where(slab_lane == size_z - 1, 0.0, turn(flat, size_z - 1))
        beside = beside + jnp.where(slab_lane == 0, 0.0, turn(flat, 1))
        return around + beside.reshape(value.shape)

    def ends(beyond, at):
        both = (turn(beyond, -2 * at) * edge).astype(jnp.float32)
        return both[:channels], both[channels:]

    def inner(source, target, force):
        for x in range(size_x):
            value = source[x]
            around = inside(
                value,
                source[x + 1] if x + 1 < size_x else None,
                source[x - 1] if x > 0 else None,
            )
            target[x] = (1.0 - relax_weight) * value + force[x] + weight_v[x] * around

    def pick(axis, q):
        return (
            jnp.where(here[axis] > 0, q, none),
            jnp.where(here[axis] < sizes[axis] - 1, q, none),
        )

    def half_of_pair(i):
        return slice(channels * (i % 2), channels * (i % 2) + channels)

    def from_x(q, side, y):
        both = x_in[pick(0, q)[side], side, y // 2].astype(jnp.float32)
        return both[half_of_pair(y)]

    def from_y(q, side, x):
        both = y_in[pick(1, q)[side], side, x // 2].astype(jnp.float32)
        return both[half_of_pair(x)]

    def either(low, high):
        return jnp.where(even, low.astype(jnp.float32), high.astype(jnp.float32))

    def from_z(q):
        below, above = pick(2, q)
        return either(z_in[below, 0], z_in[above, 1])

    def beside_ends(natural):
        return jnp.where(even, natural, turn(natural, -2)).astype(jnp.bfloat16)

    def corner(a, b, q, side_a, side_b):
        there = exists(a, side_a) & exists(b, side_b)
        return edge_ins[a, b][jnp.where(there, q // 3, ROUNDS), side_a, side_b]

    def corner_xy(q, side_x, side_y):
        both = corner(0, 1, q, side_x, side_y).astype(jnp.float32)
        return both[half_of_pair(size_x - 1 if side_x == 0 else 0)]

    def corner_z(axis, q, side):
        return either(corner(axis, 2, q, side, 0), corner(axis, 2, q, side, 1))

    def outer(target, q):
        beyond = beside_ends(from_z(q))
        for x in range(size_x):
            for p in range(pairs):
                for y, around in zip((2 * p, 2 * p + 1), ends(beyond, x * pairs + p)):
                    if x == 0:
                        around = around + from_x(q, 0, y)
                    if x == size_x - 1:
                        around = around + from_x(q, 1, y)
                    if y == 0:
                        around = around + from_y(q, 0, x)
                    if y == size_y - 1:
                        around = around + from_y(q, 1, x)
                    target[x, y] = target[x, y] + weight_v[x, y] * around

    def spread_weights():
        for side in (0, 1):
            weight = wx_in[jnp.where(exists(0, side), side, 2)]
            rim_wx[side] = jnp.broadcast_to(weight[:, None, :], (size_y,) + cell_shape)
            weight = wy_in[jnp.where(exists(1, side), side, 2)][:size_x]
            rim_wy[side] = jnp.broadcast_to(weight[:, None, :], (size_x,) + cell_shape)
        rim_wz[...] = either(
            wz_in[jnp.where(exists(2, 0), 0, 2)], wz_in[jnp.where(exists(2, 1), 1, 2)]
        )

    def own_rim(source, q):
        for side in (0, 1):
            rim_x[side] = rim_wx[side] * source[(size_x - 1) * side]
            for x in range(size_x):
                rim_y[side, x] = rim_wy[side, x] * source[x, (size_y - 1) * side]
        own = z_out[q].astype(jnp.float32)
        rim_z[...] = rim_wz[...] * jnp.where(even, turn(own, -1), turn(own, 1))

    def rim(target, q):
        along, across = (size_x - 1) * size_y, 2 * (pairs - 1)
        around = jnp.where(low_plane, turn(corner_z(0, q, 0), -along), 0.0)
        around = around + jnp.where(high_plane, turn(corner_z(0, q, 1), along), 0.0)
        first = upper & (in_line == 0)
        final = jnp.logical_not(upper) & (in_line == pairs - 1)
        around = around + jnp.where(first, swap(turn(corner_z(1, q, 0), -across)), 0.0)
        around = around + jnp.where(final, swap(turn(corner_z(1, q, 1), across)), 0.0)
        beyond = beside_ends(rim_z[...] + rim_wz[...] * around + from_z(q + 1))
        beyond_x = [beside_ends(corner_z(0, q, side)) for side in (0, 1)]
        beyond_y = [beside_ends(corner_z(1, q, side)) for side in (0, 1)]

        def swept_x(side, p):
            found = []
            theirs = (size_x - 1) * (1 - side)
            for y, around in zip((2 * p, 2 * p + 1), ends(beyond_x[side], theirs * pairs + p)):
                if y == 0:
                    around = around + corner_xy(q, side, 0)
                if y == size_y - 1:
                    around = around + corner_xy(q, side, 1)
                found.append(rim_x[side, y] + from_x(q + 1, side, y) + rim_wx[side, y] * around)
            return found

        def swept_y(side, x):
            theirs = (size_y - 1) * (1 - side)
            around = ends(beyond_y[side], x * pairs + theirs // 2)[theirs % 2]
            if x == 0:
                around = around + corner_xy(q, 0, side)
            if x == size_x - 1:
                around = around + corner_xy(q, 1, side)
            return rim_y[side, x] + from_y(q + 1, side, x) + rim_wy[side, x] * around

        cells = []
        for x in range(size_x):
            for p in range(pairs):
                below = swept_x(0, p) if x == 0 else None
                above = swept_x(1, p) if x == size_x - 1 else None
                for i, around in enumerate(ends(beyond, x * pairs + p)):
                    y = 2 * p + i
                    if below:
                        around = around + below[i]
                    if above:
                        around = around + above[i]
                    if y == 0:
                        around = around + swept_y(0, x)
                    if y == size_y - 1:
                        around = around + swept_y(1, x)
                    cell = target[x, y] + weight_v[x, y] * around
                    target[x, y] = cell
                    cells.append(cell)
        return cells

    def sum_up(found):
        sums = [block * at_cell[at] for at, block in enumerate(found)]
        while len(sums) > 1:
            sums = [a + b for a, b in zip(sums[::2], sums[1::2])]
        return sums[0]

    pieces = 4
    chunk = slots // pieces

    def make_tiles():
        def body(i, carry):
            a, k = i // layers, lax.rem(i, layers)
            q = nearest(k, layer, layers) * fold + lax.rem(part + a, fold)
            if handed_on:
                away = q // fold - layer
                relayed = (a == 0) & (away == -2)
                pl.when(relayed)(lambda: await_gather(geo_all, group - 1, geo_recv.at[q]))
                pl.when(jnp.logical_not(relayed))(
                    lambda: await_gather(geo_all, group, geo_recv.at[q])
                )
            else:
                await_gather(geo_all, group, geo_recv.at[q])
            if fold > 1:
                pl.when(a == 0)(lambda: hand_over(q))
            for j in range(group):
                source = geo_all[q * group + j]
                for piece in range(pieces):
                    span = slice(piece * chunk, (piece + 1) * chunk)
                    delta_x = column_v[0, span, :] - source[0:1, :]
                    delta_y = column_v[1, span, :] - source[1:2, :]
                    delta_z = column_v[2, span, :] - source[2:3, :]
                    square = delta_x * delta_x + delta_y * delta_y + delta_z * delta_z + 1e-30
                    distance = square * lax.rsqrt(square)
                    wave = cosine_of_turns(distance * (wave_number / (2.0 * math.pi)))
                    value = (source[3:4, :] * factor) * wave / (distance + soften)
                    tile_v[q, span, j * slots : (j + 1) * slots] = value.astype(tile_v.dtype)
            return carry

        lax.fori_loop(0, rows, body, 0)

    def apply_tiles(r):
        total = jnp.zeros((channels, slots), jnp.float32)
        for k in range(rows):
            q = nth(k)
            with jax.named_scope(f"w_dens{r}_{k}"):
                await_gather(density_all.at[r], group - (k == 0), density_recv.at[r, q])
            values = jnp.concatenate(
                [density_all[r, q * group + j] for j in range(group)], axis=1
            )
            total = total + lax.dot_general(
                values, tile_v[q], (((1,), (1,)), ((), ())), preferred_element_type=jnp.float32
            )
        return total

    def land(sem, each):
        await_bytes(face_recv.at[sem], each)

    def drain(each):
        await_bytes(face_send.at[0], each)

    def drain_now():
        for q in range(3 * ROUNDS - 2):
            drain(face_cells)
            if q % 3 == 1:
                drain(edge_cells)
        drain(weight_cells)
        drain_geometry()
        for r in range(ROUNDS - 1):
            await_gather(density_all.at[r], devices - 1, gather_send.at[0])

    for r in range(ROUNDS):
        single, double = 3 * r, 3 * r + 1
        before = init_v if r == 0 else state_v.at[2]
        once, mid, after = state_v.at[0], state_v.at[1], state_v.at[2]
        if r == ROUNDS - 1:
            after = field_ref
        force = forcing_v.at[r]
        with jax.named_scope(f"inner{r}"):
            inner(before, once, forcing_v.at[0])
        if r > 0:
            with jax.named_scope("tilesB"):
                make_tiles()
        if r == 0:
            with jax.named_scope("w_known0"):
                early = stages[1:-2]
                if stages:
                    hear(0)
                    pass_on(1)
                    start_geometry(0)
                    if early:
                        hear(1)
                        pass_on(2)
                        start_geometry(1)
                else:
                    start_geometry(0, 1, 2)
        with jax.named_scope(f"w_single{r}"):
            land(0, face_cells)
        if r == 0 and stages:
            for stage in range(2, len(stages) - 2):
                hear(stage)
                pass_on(stage + 1)
        with jax.named_scope(f"outer{r}"):
            outer(once, single)
        if r > 0:
            with jax.named_scope(f"apply{r-1}"):
                potential = jnp.where(live, apply_tiles(r - 1), 0.0)
            with jax.named_scope(f"load{r}"):
                half_of = coupling * potential
                big = half_of.astype(jnp.bfloat16).astype(jnp.float32)
                small = half_of - big
                placed = jnp.concatenate(
                    [(at_cell[...] * part[None]).astype(jnp.bfloat16) for part in (big, small)],
                    axis=2,
                ).reshape(size_x * size_y * channels, 2 * slots)
                load = lax.dot_general(
                    placed, jnp.concatenate([pick_z, pick_z], axis=1),
                    (((1,), (1,)), ((), ())), preferred_element_type=jnp.float32,
                )
                load = load.reshape(size_x, size_y, channels, size_z)
                for x in range(size_x):
                    change = weight_v[x] * load[x]
                    force[x] = forcing_v[0, x] + change
                    once[x] = once[x] + change
        with jax.named_scope(f"pack{r}"):
            pack(double, planes(once))
        start_edges(double)
        start_faces(double)
        with jax.named_scope(f"innerd{r}"):
            inner(once, mid, force)
        with jax.named_scope(f"packd{r}"):
            pack(double + 1, planes(mid))
        start_faces(double + 1)
        if r == 0:
            with jax.named_scope("w_weights"):
                land(4, weight_cells)
                spread_weights()
            with jax.named_scope("w_known"):
                if stages:
                    hear(len(stages) - 2)
                    pass_on(len(stages) - 1)
            with jax.named_scope("st_geo"):
                if stages:
                    start_geometry(*((2,) if early else (1, 2)))
                if handed_on:
                    hand_on()
        else:
            drain_now()
        own_rim(once, double)
        with jax.named_scope(f"w_double{r}"):
            land(1, face_cells)
        with jax.named_scope(f"outerd{r}"):
            outer(mid, double)
            inner(mid, after, force)
        with jax.named_scope(f"w_edges{r}"):
            land(3, edge_cells)
        with jax.named_scope(f"w_rim{r}"):
            land(2, face_cells)
        with jax.named_scope(f"rim{r}"):
            cells = rim(after, double)
            parts = [jnp.dot(jnp.concatenate(cells[x * size_y : (x + 1) * size_y], axis=0).astype(jnp.bfloat16), pick_z, preferred_element_type=jnp.float32) for x in range(size_x)]
            density = sum_up([found[channels * i : channels * (i + 1)] for found in parts for i in range(found.shape[0] // channels)])
            density = jnp.where(live, density, 0.0).astype(jnp.bfloat16)
            density_out[r] = density
            density_all[r, me] = density
        if r == 0 and stages:
            hear(len(stages) - 1)
        with jax.named_scope(f"st_dens{r}"):
            start_gather(density_out.at[r], density_all.at[r], density_recv.at[r, here[0]])
        if r < ROUNDS - 1:
            with jax.named_scope(f"pack_s{r}"):
                pack(single + 3, planes(after))
            start_faces(single + 3)
    drain(face_cells)
    drain(edge_cells)
    drain(face_cells)
    with jax.named_scope(f"apply{ROUNDS-1}"):
        potential_ref[...] = jnp.where(live, apply_tiles(ROUNDS - 1), 0.0)

    with jax.named_scope("finish"):
        await_gather(density_all.at[ROUNDS - 1], devices - 1, gather_send.at[0])


def place(field_v, potential_v, field_hbm, potential_hbm, sem):
    channels = field_hbm.shape[0]
    copies = [
        pltpu.make_async_copy(field_v.at[:, :, e, :], field_hbm.at[e], sem.at[0])
        for e in range(channels)
    ]
    copies.append(pltpu.make_async_copy(potential_v, potential_hbm, sem.at[1]))
    for copy in copies:
        copy.start()
    pltpu.make_async_copy(field_v, field_v, sem.at[0]).wait()
    copies[-1].wait()


def local(sizes, initial_field, source_term, cell_class, class_shift, surface_cell, live_count,
          panel_geometry):
    channels, size_x, size_y, size_z = initial_field.shape
    slots = surface_cell.shape[0]
    rows, cols, depths = sizes
    devices, group = rows * cols * depths, cols * depths
    brick = (size_x, size_y, channels, size_z)
    vmem = pl.BlockSpec(memory_space=pltpu.VMEM)
    hbm = pl.BlockSpec(memory_space=pltpu.HBM)
    per_device = slots * (2 * slots + 4 * 8 + ROUNDS * 2 * 2 * channels)
    grant = devices * per_device + 36 * 4 * math.prod(brick)
    operands = [
        pltpu.with_memory_space_constraint(array, pltpu.HBM)
        for array in (
            initial_field, source_term, cell_class, class_shift,
            surface_cell.reshape(1, slots), panel_geometry,
        )
    ]
    operands.insert(5, live_count.reshape(1, 1))
    two, turns = 2 * channels, 3 * ROUNDS
    field, potential = pl.pallas_call(
        functools.partial(kernel, sizes),
        out_shape=(
            jax.ShapeDtypeStruct(brick, jnp.float32),
            jax.ShapeDtypeStruct((channels, slots), jnp.float32),
        ),
        in_specs=[hbm] * 5 + [pl.BlockSpec(memory_space=pl.ANY), hbm],
        out_specs=(vmem, vmem),
        scratch_shapes=[
            pltpu.VMEM(brick, jnp.float32),
            pltpu.VMEM(brick, jnp.float32),
            pltpu.VMEM((ROUNDS,) + brick, jnp.float32),
            pltpu.VMEM((size_x, size_y, size_z), jnp.int32),
            pltpu.VMEM(brick, jnp.float32),
            pltpu.VMEM((3,) + brick, jnp.float32),
            pltpu.VMEM((turns, 2, size_y // 2, two, size_z), jnp.bfloat16),
            pltpu.VMEM((turns + 1, 2, size_y // 2, two, size_z), jnp.bfloat16),
            pltpu.VMEM((turns, 2, size_x // 2, two, size_z), jnp.bfloat16),
            pltpu.VMEM((turns + 1, 2, size_x // 2, two, size_z), jnp.bfloat16),
            pltpu.VMEM((turns, two, size_z), jnp.bfloat16),
            pltpu.VMEM((turns + 1, 2, two, size_z), jnp.bfloat16),
            pltpu.VMEM((ROUNDS + 1, 2, 2, two, size_z), jnp.bfloat16),
            pltpu.VMEM((ROUNDS + 1, 2, 2, two, size_z), jnp.bfloat16),
            pltpu.VMEM((ROUNDS + 1, 2, 2, two, size_z), jnp.bfloat16),
            pltpu.VMEM((2, size_y, size_z), jnp.float32),
            pltpu.VMEM((3, size_y, size_z), jnp.float32),
            pltpu.VMEM((2, channels, size_z), jnp.float32),
            pltpu.VMEM((3, channels, size_z), jnp.float32),
            pltpu.VMEM((two, size_z), jnp.bfloat16),
            pltpu.VMEM((3, two, size_z), jnp.bfloat16),
            pltpu.VMEM((2, size_y, channels, size_z), jnp.float32),
            pltpu.VMEM((2, size_x, channels, size_z), jnp.float32),
            pltpu.VMEM((two, size_z), jnp.float32),
            pltpu.VMEM((2, size_y, channels, size_z), jnp.float32),
            pltpu.VMEM((2, size_x, channels, size_z), jnp.float32),
            pltpu.VMEM((two, size_z), jnp.float32),
            pltpu.VMEM((size_y + size_x + 2, channels, size_z), jnp.float32),
            pltpu.VMEM((devices, 4, slots), jnp.float32),
            pltpu.VMEM((3, slots, slots), jnp.float32),
            pltpu.VMEM((rows, slots, group * slots), jnp.bfloat16),
            pltpu.VMEM((ROUNDS, channels, slots), jnp.bfloat16),
            pltpu.VMEM((ROUNDS, devices, channels, slots), jnp.bfloat16),
            pltpu.VMEM((size_x * size_y, channels, slots), jnp.float32),
            pltpu.SMEM(class_shift.shape, jnp.float32),
            pltpu.VMEM((1, 1), jnp.int32),
            pltpu.VMEM((1, slots), jnp.int32),
            pltpu.VMEM(panel_geometry.shape, jnp.float32),
            pltpu.SemaphoreType.REGULAR((max(1, len(relays(sizes))),)),
            pltpu.SemaphoreType.DMA((7,)),
            pltpu.SemaphoreType.DMA((1,)),
            pltpu.SemaphoreType.DMA((5,)),
            pltpu.SemaphoreType.DMA((1,)),
            pltpu.SemaphoreType.DMA((1,)),
            pltpu.SemaphoreType.DMA((rows,)),
            pltpu.SemaphoreType.DMA((ROUNDS, rows)),
        ],
        compiler_params=pltpu.CompilerParams(
            collective_id=0, has_side_effects=True, vmem_limit_bytes=grant
        ),
    )(*operands)
    return pl.pallas_call(
        place,
        out_shape=(
            jax.ShapeDtypeStruct(initial_field.shape, jnp.float32),
            jax.ShapeDtypeStruct((channels, slots), jnp.float32),
        ),
        in_specs=[vmem] * 2,
        out_specs=(hbm, hbm),
        scratch_shapes=[pltpu.SemaphoreType.DMA((2,))],
        compiler_params=pltpu.CompilerParams(vmem_limit_bytes=8 * math.prod(brick)),
    )(field, potential)


def solution(mesh):
    placed = (
        P(None, "row", "col", "gz"),
        P(None, "row", "col", "gz"),
        P("row", "col", "gz"),
        P(),
        P(("row", "col", "gz")),
        P(("row", "col", "gz")),
        P(None, ("row", "col", "gz")),
    )
    return jax.shard_map(
        functools.partial(local, tuple(mesh.shape[axis] for axis in AXES)),
        mesh=mesh,
        in_specs=placed,
        out_specs=(P(None, "row", "col", "gz"), P(None, ("row", "col", "gz"))),
        check_vma=False,
    )
```

```python
import functools
import math

import jax
import jax.numpy as jnp
import numpy as np
from jax import lax
from jax.experimental import pallas as pl
from jax.experimental.pallas import tpu as pltpu
from jax.sharding import PartitionSpec as P

ROUNDS = 2

relax_weight = 0.8
wave_number = 25.0
soften = 0.05
coupling = 0.5

MESH = pl.DeviceIdType.MESH
AXES = ("row", "col", "gz")


def cosine_terms(degree=6):
    nodes = 0.125 * (1.0 + np.cos(np.pi * (np.arange(64) + 0.5) / 64))
    fitted = np.polynomial.Polynomial.fit(
        nodes, np.cos(2 * np.pi * np.sqrt(nodes)), degree, domain=[0.0, 0.25]
    )
    return [float(c) for c in fitted.convert().coef]


COSINE = cosine_terms()


def cosine_of_turns(turns):
    fraction = turns - jnp.floor(turns + 0.5)
    square = fraction * fraction
    value = jnp.full_like(square, COSINE[-1])
    for term in reversed(COSINE[:-1]):
        value = value * square + term
    return value


def relays(sizes):
    rows, cols, depths = sizes
    if cols != 2 or depths != 2 or rows < 2 or rows % 2:
        return []
    stages, far = [[(-1, 0, 0), (1, 0, 0), (0, 1, 0), (0, 0, 1)]], 2
    while far < rows:
        stages.append([(-far, 0, 0), (far, 0, 0)] + ([(0, 1, 1)] if far == 2 else []))
        far *= 2
    stages.append([(0, 1, 1)])

    def at(device, offset):
        r, c, d = (x + o for x, o in zip(device, offset))
        return (r, c % 2, d % 2) if 0 <= r < rows else None

    everyone = [(r, c, d) for r in range(rows) for c in range(2) for d in range(2)]
    known = {x: {x} | {at(x, o) for o in stages[0]} for x in everyone}
    for i, stage in enumerate(stages):
        told = {x: set(known[x]) for x in everyone}
        for x in everyone:
            for offset in stage:
                target = at(x, offset)
                if target is not None:
                    if target not in known[x]:
                        return []
                    told[target] |= known[x]
        known = told
        for x in everyone:
            ahead = {at(x, (r, c, d)) for r in (-1, 0, 1) for c in (0, 1) for d in (0, 1) if abs(r) + c + d < 3}
            ahead |= {at(x, (r, 0, 0)) for r in (-2, 2)}
            if i > 0:
                ahead |= {at(x, (r, c, d)) for r in (-2, 2) for c in (0, 1) for d in (0, 1)}
                ahead |= {at(x, (r, 0, 0)) for r in (-4, 4)}
            if i == len(stages) - 2:
                ahead = {y for y in everyone if (y[0] - x[0]) % 2 == 0}
            if i == len(stages) - 1:
                ahead = set(everyone)
            if not ahead - {None} <= known[x] | {None}:
                return []
    return stages


def kernel(
    sizes,
    init_hbm, source_hbm, class_hbm, shift_hbm, cell_hbm, live_hbm, geo_hbm,
    field_ref, potential_ref,
    init_v, source_v, forcing_v, class_v, weight_v, state_v,
    x_out, x_in, y_out, y_in, z_out, z_in, xy_in, xz_in, yz_in,
    wx_out, wx_in, wy_out, wy_in, wz_out, wz_in, rim_x, rim_y, rim_z,
    rim_wx, rim_wy, rim_wz, meter,
    geo_all, column_v, tile_v, density_out, density_all, at_cell,
    shift_ref, live_ref, cell_ref, geo_ref,
    known, local_sem, face_send, face_recv, gather_send, geo_relay, geo_recv, density_recv,
):
    rows, cols, depths = sizes
    devices = rows * cols * depths
    group = cols * depths
    channels, size_x, size_y, size_z = init_hbm.shape
    slots = cell_hbm.shape[1]
    classes = shift_ref.shape[0]
    factor = 1.0 / math.sqrt(slots * devices)
    per_turn = wave_number / (2.0 * math.pi)
    here = tuple(lax.axis_index(axis) for axis in AXES)
    me = (here[0] * cols + here[1]) * depths + here[2]

    def brick_copies(hbm, vmem, sem):
        return [
            pltpu.make_async_copy(hbm.at[e], vmem.at[:, :, e, :], sem) for e in range(channels)
        ]

    def brick_wait(vmem, sem):
        pltpu.make_async_copy(vmem, vmem, sem).wait()

    stages = relays(sizes)
    barrier = pltpu.get_barrier_semaphore()

    def offset_place(offset):
        return (
            here[0] + offset[0],
            1 - here[1] if offset[1] else here[1],
            1 - here[2] if offset[2] else here[2],
        )

    def reaches(offset):
        if offset[0] == 0:
            return None
        return here[0] >= -offset[0] if offset[0] < 0 else here[0] + offset[0] < rows

    def tell(sem, offset):
        def go():
            pl.semaphore_signal(
                sem, inc=1, device_id=offset_place(offset), device_id_type=MESH
            )

        present = reaches(offset)
        if present is None:
            go()
        else:
            pl.when(present)(go)

    def tellers(stage):
        return sum(
            1 if reaches(offset) is None else jnp.where(reaches(offset), 1, 0)
            for offset in stages[stage]
        )

    def pass_on(stage):
        for offset in stages[stage]:
            tell(known.at[stage], offset)

    def hear(stage):
        pl.semaphore_wait(known.at[stage], tellers(stage))

    if stages:
        for offset in stages[0]:
            tell(barrier, offset)
        near = tellers(0)
    else:
        near = devices - 1

    for copy in brick_copies(init_hbm, init_v, local_sem.at[0]):
        copy.start()

    copies = [
        pltpu.make_async_copy(class_hbm, class_v, local_sem.at[1]),
        pltpu.make_async_copy(geo_hbm, geo_ref, local_sem.at[3]),
        pltpu.make_async_copy(shift_hbm, shift_ref, local_sem.at[4]),
        pltpu.make_async_copy(cell_hbm, cell_ref, local_sem.at[5]),
        pltpu.make_async_copy(live_hbm, live_ref, local_sem.at[6]),
    ]

    def nearest(k, own, count):
        below, above = own, count - 1 - own
        near = own + jnp.where(lax.rem(k, 2) == 1, (k + 1) // 2, -(k // 2))
        far = jnp.where(below < above, k, count - 1 - k)
        return jnp.where((k <= 2 * below) & (k <= 2 * above), near, far)

    def nth(k):
        return nearest(k, here[0], rows)

    def each_other(action):
        def at(row, first):
            for b in reversed(range(cols)):
                for c in reversed(range(depths)):
                    if first and b == 0 and c == 0:
                        continue
                    action((row, lax.rem(here[1] + b, cols), lax.rem(here[2] + c, depths)))

        def others(i, carry):
            at(nth(rows - 1 - i), False)
            return carry

        lax.fori_loop(0, rows - 1, others, 0)
        at(here[0], True)

    if not stages:
        each_other(
            lambda device: pl.semaphore_signal(
                barrier, inc=1, device_id=device, device_id_type=MESH
            )
        )
    for copy in copies:
        copy.start()
    for copy in brick_copies(source_hbm, source_v, local_sem.at[2]):
        copy.start()

    cell_shape, pair_shape = (channels, size_z), (2 * channels, size_z)
    pairs = size_y // 2
    lane = lax.broadcasted_iota(jnp.int32, pair_shape, 1)
    even = (lane & 1) == 0
    at_pair = lane >> 1
    in_line = lax.rem(at_pair, pairs)
    upper = lax.broadcasted_iota(jnp.int32, pair_shape, 0) < channels
    low_plane = at_pair < pairs
    high_plane = (at_pair >= (size_x - 1) * pairs) & (at_pair < size_x * pairs)
    edge = jnp.where((lane == 0) | (lane == size_z - 1), 1.0, 0.0).astype(jnp.bfloat16)
    slab = (size_y * channels, size_z)
    slab_lane = lax.broadcasted_iota(jnp.int32, slab, 1)

    def turn(value, shift):
        return pltpu.roll(value, shift % size_z, 1)

    def swap(value):
        return jnp.concatenate([value[channels:], value[:channels]], axis=0)

    def planes(ref):
        return [[ref[x, y] for y in range(size_y)] for x in range(size_x)]

    def in_pairs(values):
        return [
            [
                jnp.concatenate([line[y], line[y + 1]], axis=0).astype(jnp.bfloat16)
                for y in range(0, size_y, 2)
            ]
            for line in values
        ]

    def pack_deep(paired):
        packed = jnp.zeros(pair_shape, jnp.bfloat16)
        for x in range(size_x):
            for p in range(pairs):
                packed = packed + turn(paired[x][p] * edge, 2 * (x * pairs + p) + 1)
        return packed

    def pack(q, values):
        paired = in_pairs(values)
        for side, x in ((0, 0), (1, size_x - 1)):
            for p in range(pairs):
                x_out[q, side, p] = paired[x][p]
        for side, y in ((0, 0), (1, size_y - 1)):
            for x in range(0, size_x, 2):
                both = jnp.concatenate([values[x][y], values[x + 1][y]], axis=0)
                y_out[q, side, x // 2] = both.astype(y_out.dtype)
        z_out[q] = pack_deep(paired)

    def exists(axis, up):
        return here[axis] < sizes[axis] - 1 if up else here[axis] > 0

    beside = []
    for axis in range(3):
        if sizes[axis] == 2:
            beside.append((axis, 1 - here[axis], 1 - here[axis], None))
        elif sizes[axis] > 2:
            beside.append((axis, 0, here[axis] - 1, exists(axis, 0)))
            beside.append((axis, 1, here[axis] + 1, exists(axis, 1)))
    edges_beside = [(one, two) for one in beside for two in beside if one[0] < two[0]]
    outs, ins = (x_out, y_out, z_out), (x_in, y_in, z_in)
    edge_ins = {(0, 1): xy_in, (0, 2): xz_in, (1, 2): yz_in}

    def when(present, action):
        if present is None:
            action()
        else:
            pl.when(present)(action)

    def start(source, landing, sem, target, present):
        def go():
            pltpu.make_async_remote_copy(
                src_ref=source,
                dst_ref=landing,
                send_sem=face_send.at[0],
                recv_sem=face_recv.at[sem],
                device_id=target,
                device_id_type=MESH,
            ).start()

        when(present, go)

    def start_faces(q):
        for axis, side, place, present in beside:
            source = outs[axis].at[q] if axis == 2 else outs[axis].at[q, side]
            start(source, ins[axis].at[q, 1 - side], q % 3, {AXES[axis]: place}, present)

    def start_edges(q):
        for (a, side_a, place_a, one), (b, side_b, place_b, two) in edges_beside:
            if (a, b) == (0, 1):
                source = y_out.at[q, side_b, side_a * ((size_x - 1) // 2)]
            else:
                source = z_out.at[q]
            landing = edge_ins[a, b].at[q // 3, 1 - side_a, 1 - side_b]
            present = two if one is None else one if two is None else one & two
            start(source, landing, 3, {AXES[a]: place_a, AXES[b]: place_b}, present)

    def start_weights():
        for axis, side, place, present in beside:
            out, into = ((wx_out, wx_in), (wy_out, wy_in), (wz_out, wz_in))[axis]
            source = out if axis == 2 else out.at[side]
            start(source, into.at[1 - side], 4, {AXES[axis]: place}, present)

    def await_bytes(sem, each):
        split = [axis for axis in range(3) if sizes[axis] > 2]
        for case in range(2 ** len(split)):
            counts = [min(count, 2) - 1 for count in sizes]
            condition = None
            for i, axis in enumerate(split):
                both = (case >> i) & 1
                counts[axis] += both
                holds = (here[axis] > 0) & (here[axis] < sizes[axis] - 1)
                holds = holds if both else jnp.logical_not(holds)
                condition = holds if condition is None else condition & holds
            span = meter.at[pl.ds(0, each(counts))]
            when(condition, lambda span=span: pltpu.make_async_copy(span, span, sem).wait())

    def face_cells(n):
        return n[0] * pairs + n[1] * (size_x // 2) + n[2]

    def edge_cells(n):
        return n[0] * n[1] + n[0] * n[2] + n[1] * n[2]

    def weight_cells(n):
        return n[0] * (size_y // channels) + n[1] + n[2]

    none = 3 * ROUNDS
    x_in[none] = jnp.zeros(x_in.shape[1:], x_in.dtype)
    y_in[none] = jnp.zeros(y_in.shape[1:], y_in.dtype)
    z_in[none] = jnp.zeros(z_in.shape[1:], z_in.dtype)
    for into in edge_ins.values():
        into[ROUNDS] = jnp.zeros(into.shape[1:], into.dtype)
    wx_in[2] = jnp.zeros(wx_in.shape[1:], wx_in.dtype)
    wy_in[2] = jnp.zeros(wy_in.shape[1:], wy_in.dtype)
    wz_in[2] = jnp.zeros(wz_in.shape[1:], wz_in.dtype)

    with jax.named_scope("w_init"):
        brick_wait(init_v, local_sem.at[0])

    pack(0, planes(init_v))

    with jax.named_scope("w_barrier"):
        pl.semaphore_wait(barrier, near)
    if stages:
        pass_on(0)
    start_faces(0)

    copies[1].wait()
    eye = lax.broadcasted_iota(jnp.int32, (slots, slots), 0) == lax.broadcasted_iota(
        jnp.int32, (slots, slots), 1
    )
    for i in range(3):
        column = jnp.sum(jnp.where(eye, geo_ref[i : i + 1, :], 0.0), axis=1, keepdims=True)
        column_v[i] = jnp.broadcast_to(column * per_turn, (slots, slots))
    pltpu.make_async_copy(geo_ref, geo_all.at[me], geo_recv.at[here[0]]).start()


    fold = 2 - rows % 2
    layers, layer, part = rows // fold, here[0] // fold, lax.rem(here[0], fold)

    handed_on = len(stages) > 3 and layers <= 4

    def send_geometry(row, b, c, sem=None):
        pltpu.make_async_remote_copy(
            src_ref=geo_ref,
            dst_ref=geo_all.at[me],
            send_sem=gather_send.at[0],
            recv_sem=geo_recv.at[here[0]] if sem is None else sem,
            device_id=(row, lax.rem(here[1] + b, cols), lax.rem(here[2] + c, depths)),
            device_id_type=MESH,
        ).start()

    others_beside = [(b, c) for b in range(cols) for c in range(depths)]

    def start_geometry(*parts):
        if 0 in parts:
            for b, c in others_beside[1:]:
                send_geometry(here[0], b, c)
        for away in reversed(range(fold, rows, fold)):
            step = min(away // fold, 3)
            down = others_beside[:1] if step - 1 in parts else []
            down = down + (others_beside[1:] if min(step, 2) in parts else [])
            up, sem = down, None
            if handed_on and step > 1:
                up, sem = (others_beside[:1] if step == 2 and 1 in parts else []), geo_relay.at[0]

            def to_row(row, targets, sem):
                for b, c in targets:
                    send_geometry(row, b, c, sem)

            if down:
                pl.when(here[0] >= away)(
                    functools.partial(to_row, here[0] - away, down, None)
                )
            if up:
                pl.when(here[0] + away < rows)(
                    functools.partial(to_row, here[0] + away, up, sem)
                )

    def hand_on():
        def pass_block(q, onward):
            block = geo_all.at[(q * cols + here[1]) * depths + here[2]]
            pltpu.make_async_copy(block, block, geo_relay.at[0]).wait()

            def send(row, b, c):
                pltpu.make_async_remote_copy(
                    src_ref=block,
                    dst_ref=block,
                    send_sem=gather_send.at[0],
                    recv_sem=geo_recv.at[q],
                    device_id=(
                        row, lax.rem(here[1] + b, cols), lax.rem(here[2] + c, depths)
                    ),
                    device_id_type=MESH,
                ).start()

            def send_onward():
                for b, c in others_beside:
                    send(onward, b, c)

            pl.when(onward < rows)(send_onward)
            for b, c in others_beside[1:]:
                send(here[0], b, c)

        two = 2 * fold
        pl.when(here[0] >= two)(lambda: pass_block(here[0] - two, here[0] + fold))

    def drain_geometry():
        def spent(count, present=None):
            when(present, lambda: await_gather(geo_all, count, gather_send.at[0]))

        if not handed_on:
            spent(devices - 1)
            return
        spent(layers * group)
        spent(group - 1)
        for n in range(1, layers):
            spent(group, here[0] >= n * fold)
            if n < 3:
                spent(group if n == 1 else 1, here[0] + n * fold < rows)
        two = 2 * fold
        spent(group - 1, here[0] >= two)
        spent(group, (here[0] >= two) & (here[0] + fold < rows))

    def hand_over(q):
        blocks = geo_all.at[pl.ds(q * group, group)]
        pltpu.make_async_remote_copy(
            src_ref=blocks,
            dst_ref=blocks,
            send_sem=gather_send.at[0],
            recv_sem=geo_recv.at[q],
            device_id={"row": layer * fold + (fold - 1 - part)},
            device_id_type=MESH,
        ).start()

    def start_gather(source, gathered, sem):
        def send(device):
            pltpu.make_async_remote_copy(
                src_ref=source,
                dst_ref=gathered.at[me],
                send_sem=gather_send.at[0],
                recv_sem=sem,
                device_id=device,
                device_id_type=MESH,
            ).start()

        each_other(send)

    def await_gather(gathered, count, sem):
        whole = gathered.at[pl.ds(0, count)]
        pltpu.make_async_copy(whole, whole, sem).wait()

    copies[0].wait()
    copies[2].wait()
    for x in range(size_x):
        kind = class_v[x]
        shift = jnp.zeros(kind.shape, jnp.float32)
        for level in range(classes):
            shift = jnp.where(kind == level, shift_ref[level], shift)
        weight = relax_weight / (6.0 + shift)
        weight_v[x] = jnp.broadcast_to(weight[:, None, :], (size_y, channels, size_z))
        if x == 0:
            wx_out[0] = weight
        if x == size_x - 1:
            wx_out[1] = weight
        if x == 0:
            wy_out[...] = jnp.zeros(wy_out.shape, wy_out.dtype)
        wy_out[0, x : x + 1, :] = weight[0:1]
        wy_out[1, x : x + 1, :] = weight[size_y - 1 : size_y]
    wz_out[...] = pack_deep(in_pairs(planes(weight_v)))
    start_weights()

    copies[3].wait()
    copies[4].wait()
    cell = cell_ref[...]
    bits = size_z.bit_length() - 1
    cell_z = cell & (size_z - 1)
    cell_xy = cell >> bits
    pick_z = lax.broadcasted_iota(jnp.int32, (size_z, slots), 0) == cell_z
    pick_z = jnp.where(pick_z, 1.0, 0.0).astype(jnp.bfloat16)
    for at in range(size_x * size_y):
        at_cell[at] = jnp.broadcast_to(
            jnp.where(cell_xy == at, 1.0, 0.0), (channels, slots)
        )
    live = lax.broadcasted_iota(jnp.int32, (channels, slots), 1) < live_ref[...]
    brick_wait(source_v, local_sem.at[2])
    for x in range(size_x):
        forcing_v[0, x] = weight_v[x] * source_v[x]

    def inside(value, above, below):
        blank = jnp.zeros((1,) + cell_shape, jnp.float32)
        around = jnp.concatenate([value[1:], blank], axis=0)
        around = around + jnp.concatenate([blank, value[:-1]], axis=0)
        for other in (above, below):
            if other is not None:
                around = around + other
        flat = value.reshape(slab)
        beside = jnp.where(slab_lane == size_z - 1, 0.0, turn(flat, size_z - 1))
        beside = beside + jnp.where(slab_lane == 0, 0.0, turn(flat, 1))
        return around + beside.reshape(value.shape)

    def ends(beyond, at):
        both = (turn(beyond, -2 * at) * edge).astype(jnp.float32)
        return both[:channels], both[channels:]

    def inner(source, target, force):
        for x in range(size_x):
            value = source[x]
            around = inside(
                value,
                source[x + 1] if x + 1 < size_x else None,
                source[x - 1] if x > 0 else None,
            )
            target[x] = (1.0 - relax_weight) * value + force[x] + weight_v[x] * around

    def pick(axis, q):
        return (
            jnp.where(here[axis] > 0, q, none),
            jnp.where(here[axis] < sizes[axis] - 1, q, none),
        )

    def half_of_pair(i):
        return slice(channels * (i % 2), channels * (i % 2) + channels)

    def from_x(q, side, y):
        both = x_in[pick(0, q)[side], side, y // 2].astype(jnp.float32)
        return both[half_of_pair(y)]

    def from_y(q, side, x):
        both = y_in[pick(1, q)[side], side, x // 2].astype(jnp.float32)
        return both[half_of_pair(x)]

    def either(low, high):
        return jnp.where(even, low.astype(jnp.float32), high.astype(jnp.float32))

    def from_z(q):
        below, above = pick(2, q)
        return either(z_in[below, 0], z_in[above, 1])

    def beside_ends(natural):
        return jnp.where(even, natural, turn(natural, -2)).astype(jnp.bfloat16)

    def corner(a, b, q, side_a, side_b):
        there = exists(a, side_a) & exists(b, side_b)
        return edge_ins[a, b][jnp.where(there, q // 3, ROUNDS), side_a, side_b]

    def corner_xy(q, side_x, side_y):
        both = corner(0, 1, q, side_x, side_y).astype(jnp.float32)
        return both[half_of_pair(size_x - 1 if side_x == 0 else 0)]

    def corner_z(axis, q, side):
        return either(corner(axis, 2, q, side, 0), corner(axis, 2, q, side, 1))

    def outer(target, q):
        beyond = beside_ends(from_z(q))
        for x in range(size_x):
            for p in range(pairs):
                for y, around in zip((2 * p, 2 * p + 1), ends(beyond, x * pairs + p)):
                    if x == 0:
                        around = around + from_x(q, 0, y)
                    if x == size_x - 1:
                        around = around + from_x(q, 1, y)
                    if y == 0:
                        around = around + from_y(q, 0, x)
                    if y == size_y - 1:
                        around = around + from_y(q, 1, x)
                    target[x, y] = target[x, y] + weight_v[x, y] * around

    def spread_weights():
        for side in (0, 1):
            weight = wx_in[jnp.where(exists(0, side), side, 2)]
            rim_wx[side] = jnp.broadcast_to(weight[:, None, :], (size_y,) + cell_shape)
            weight = wy_in[jnp.where(exists(1, side), side, 2)][:size_x]
            rim_wy[side] = jnp.broadcast_to(weight[:, None, :], (size_x,) + cell_shape)
        rim_wz[...] = either(
            wz_in[jnp.where(exists(2, 0), 0, 2)], wz_in[jnp.where(exists(2, 1), 1, 2)]
        )

    def own_rim(source, q):
        for side in (0, 1):
            rim_x[side] = rim_wx[side] * source[(size_x - 1) * side]
            for x in range(size_x):
                rim_y[side, x] = rim_wy[side, x] * source[x, (size_y - 1) * side]
        own = z_out[q].astype(jnp.float32)
        rim_z[...] = rim_wz[...] * jnp.where(even, turn(own, -1), turn(own, 1))

    def rim(target, q):
        along, across = (size_x - 1) * size_y, 2 * (pairs - 1)
        around = jnp.where(low_plane, turn(corner_z(0, q, 0), -along), 0.0)
        around = around + jnp.where(high_plane, turn(corner_z(0, q, 1), along), 0.0)
        first = upper & (in_line == 0)
        final = jnp.logical_not(upper) & (in_line == pairs - 1)
        around = around + jnp.where(first, swap(turn(corner_z(1, q, 0), -across)), 0.0)
        around = around + jnp.where(final, swap(turn(corner_z(1, q, 1), across)), 0.0)
        beyond = beside_ends(rim_z[...] + rim_wz[...] * around + from_z(q + 1))
        beyond_x = [beside_ends(corner_z(0, q, side)) for side in (0, 1)]
        beyond_y = [beside_ends(corner_z(1, q, side)) for side in (0, 1)]

        def swept_x(side, p):
            found = []
            theirs = (size_x - 1) * (1 - side)
            for y, around in zip((2 * p, 2 * p + 1), ends(beyond_x[side], theirs * pairs + p)):
                if y == 0:
                    around = around + corner_xy(q, side, 0)
                if y == size_y - 1:
                    around = around + corner_xy(q, side, 1)
                found.append(rim_x[side, y] + from_x(q + 1, side, y) + rim_wx[side, y] * around)
            return found

        def swept_y(side, x):
            theirs = (size_y - 1) * (1 - side)
            around = ends(beyond_y[side], x * pairs + theirs // 2)[theirs % 2]
            if x == 0:
                around = around + corner_xy(q, 0, side)
            if x == size_x - 1:
                around = around + corner_xy(q, 1, side)
            return rim_y[side, x] + from_y(q + 1, side, x) + rim_wy[side, x] * around

        cells = []
        for x in range(size_x):
            for p in range(pairs):
                below = swept_x(0, p) if x == 0 else None
                above = swept_x(1, p) if x == size_x - 1 else None
                for i, around in enumerate(ends(beyond, x * pairs + p)):
                    y = 2 * p + i
                    if below:
                        around = around + below[i]
                    if above:
                        around = around + above[i]
                    if y == 0:
                        around = around + swept_y(0, x)
                    if y == size_y - 1:
                        around = around + swept_y(1, x)
                    cell = target[x, y] + weight_v[x, y] * around
                    target[x, y] = cell
                    cells.append(cell)
        return cells

    def sum_up(found):
        sums = [block * at_cell[at] for at, block in enumerate(found)]
        while len(sums) > 1:
            sums = [a + b for a, b in zip(sums[::2], sums[1::2])]
        return sums[0]

    pieces = 4
    chunk = slots // pieces

    def make_tiles():
        def body(i, carry):
            a, k = i // layers, lax.rem(i, layers)
            q = nearest(k, layer, layers) * fold + lax.rem(part + a, fold)
            if handed_on:
                away = q // fold - layer
                relayed = (a == 0) & (away == -2)
                pl.when(relayed)(lambda: await_gather(geo_all, group - 1, geo_recv.at[q]))
                pl.when(jnp.logical_not(relayed))(
                    lambda: await_gather(geo_all, group, geo_recv.at[q])
                )
            else:
                await_gather(geo_all, group, geo_recv.at[q])
            if fold > 1:
                pl.when(a == 0)(lambda: hand_over(q))
            for j in range(group):
                source = geo_all[q * group + j] * per_turn
                for piece in range(pieces):
                    span = slice(piece * chunk, (piece + 1) * chunk)
                    delta_x = column_v[0, span, :] - source[0:1, :]
                    delta_y = column_v[1, span, :] - source[1:2, :]
                    delta_z = column_v[2, span, :] - source[2:3, :]
                    square = delta_x * delta_x + delta_y * delta_y + delta_z * delta_z + 1e-30
                    turns = square * lax.rsqrt(square)
                    wave = cosine_of_turns(turns)
                    value = (source[3:4, :] * factor) * wave / (turns + soften * per_turn)
                    tile_v[q, span, j * slots : (j + 1) * slots] = value.astype(tile_v.dtype)
            return carry

        lax.fori_loop(0, rows, body, 0)

    def apply_tiles(r):
        total = jnp.zeros((channels, slots), jnp.float32)
        for k in range(rows):
            q = nth(k)
            with jax.named_scope(f"w_dens{r}_{k}"):
                await_gather(density_all.at[r], group - (k == 0), density_recv.at[r, q])
            values = jnp.concatenate(
                [density_all[r, q * group + j] for j in range(group)], axis=1
            )
            total = total + lax.dot_general(
                values, tile_v[q], (((1,), (1,)), ((), ())), preferred_element_type=jnp.float32
            )
        return total

    def land(sem, each):
        await_bytes(face_recv.at[sem], each)

    def drain(each):
        await_bytes(face_send.at[0], each)

    def drain_now():
        for q in range(3 * ROUNDS - 2):
            drain(face_cells)
            if q % 3 == 1:
                drain(edge_cells)
        drain(weight_cells)
        drain_geometry()
        for r in range(ROUNDS - 1):
            await_gather(density_all.at[r], devices - 1, gather_send.at[0])

    for r in range(ROUNDS):
        single, double = 3 * r, 3 * r + 1
        before = init_v if r == 0 else state_v.at[2]
        once, mid, after = state_v.at[0], state_v.at[1], state_v.at[2]
        if r == ROUNDS - 1:
            after = field_ref
        force = forcing_v.at[r]
        with jax.named_scope(f"inner{r}"):
            inner(before, once, forcing_v.at[0])
        if r > 0:
            with jax.named_scope("tilesB"):
                make_tiles()
        if r == 0:
            with jax.named_scope("w_known0"):
                early = stages[1:-2]
                if stages:
                    hear(0)
                    pass_on(1)
                    start_geometry(0)
                    if early:
                        hear(1)
                        pass_on(2)
                        start_geometry(1)
                else:
                    start_geometry(0, 1, 2)
        with jax.named_scope(f"w_single{r}"):
            land(0, face_cells)
        if r == 0 and stages:
            for stage in range(2, len(stages) - 2):
                hear(stage)
                pass_on(stage + 1)
        with jax.named_scope(f"outer{r}"):
            outer(once, single)
        if r > 0:
            with jax.named_scope(f"apply{r-1}"):
                potential = jnp.where(live, apply_tiles(r - 1), 0.0)
            with jax.named_scope(f"load{r}"):
                half_of = coupling * potential
                big = half_of.astype(jnp.bfloat16).astype(jnp.float32)
                small = half_of - big
                placed = jnp.concatenate(
                    [(at_cell[...] * part[None]).astype(jnp.bfloat16) for part in (big, small)],
                    axis=2,
                ).reshape(size_x * size_y * channels, 2 * slots)
                load = lax.dot_general(
                    placed, jnp.concatenate([pick_z, pick_z], axis=1),
                    (((1,), (1,)), ((), ())), preferred_element_type=jnp.float32,
                )
                load = load.reshape(size_x, size_y, channels, size_z)
                for x in range(size_x):
                    change = weight_v[x] * load[x]
                    force[x] = forcing_v[0, x] + change
                    once[x] = once[x] + change
        with jax.named_scope(f"pack{r}"):
            pack(double, planes(once))
        start_edges(double)
        start_faces(double)
        with jax.named_scope(f"innerd{r}"):
            inner(once, mid, force)
        with jax.named_scope(f"packd{r}"):
            pack(double + 1, planes(mid))
        start_faces(double + 1)
        if r == 0:
            with jax.named_scope("w_weights"):
                land(4, weight_cells)
                spread_weights()
            with jax.named_scope("w_known"):
                if stages:
                    hear(len(stages) - 2)
                    pass_on(len(stages) - 1)
            with jax.named_scope("st_geo"):
                if stages:
                    start_geometry(*((2,) if early else (1, 2)))
                if handed_on:
                    hand_on()
        else:
            drain_now()
        own_rim(once, double)
        with jax.named_scope(f"w_double{r}"):
            land(1, face_cells)
        with jax.named_scope(f"outerd{r}"):
            outer(mid, double)
            inner(mid, after, force)
        with jax.named_scope(f"w_edges{r}"):
            land(3, edge_cells)
        with jax.named_scope(f"w_rim{r}"):
            land(2, face_cells)
        with jax.named_scope(f"rim{r}"):
            cells = rim(after, double)
            parts = [jnp.dot(jnp.concatenate(cells[x * size_y : (x + 1) * size_y], axis=0).astype(jnp.bfloat16), pick_z, preferred_element_type=jnp.float32) for x in range(size_x)]
            density = sum_up([found[channels * i : channels * (i + 1)] for found in parts for i in range(found.shape[0] // channels)])
            density = jnp.where(live, density, 0.0).astype(jnp.bfloat16)
            density_out[r] = density
            density_all[r, me] = density
        if r == 0 and stages:
            hear(len(stages) - 1)
        with jax.named_scope(f"st_dens{r}"):
            start_gather(density_out.at[r], density_all.at[r], density_recv.at[r, here[0]])
        if r < ROUNDS - 1:
            with jax.named_scope(f"pack_s{r}"):
                pack(single + 3, planes(after))
            start_faces(single + 3)
    drain(face_cells)
    drain(edge_cells)
    drain(face_cells)
    with jax.named_scope(f"apply{ROUNDS-1}"):
        potential_ref[...] = jnp.where(live, apply_tiles(ROUNDS - 1), 0.0)

    with jax.named_scope("finish"):
        await_gather(density_all.at[ROUNDS - 1], devices - 1, gather_send.at[0])


def place(field_v, potential_v, field_hbm, potential_hbm, sem):
    channels = field_hbm.shape[0]
    copies = [
        pltpu.make_async_copy(field_v.at[:, :, e, :], field_hbm.at[e], sem.at[0])
        for e in range(channels)
    ]
    copies.append(pltpu.make_async_copy(potential_v, potential_hbm, sem.at[1]))
    for copy in copies:
        copy.start()
    pltpu.make_async_copy(field_v, field_v, sem.at[0]).wait()
    copies[-1].wait()


def local(sizes, initial_field, source_term, cell_class, class_shift, surface_cell, live_count,
          panel_geometry):
    channels, size_x, size_y, size_z = initial_field.shape
    slots = surface_cell.shape[0]
    rows, cols, depths = sizes
    devices, group = rows * cols * depths, cols * depths
    brick = (size_x, size_y, channels, size_z)
    vmem = pl.BlockSpec(memory_space=pltpu.VMEM)
    hbm = pl.BlockSpec(memory_space=pltpu.HBM)
    per_device = slots * (2 * slots + 4 * 8 + ROUNDS * 2 * 2 * channels)
    grant = devices * per_device + 36 * 4 * math.prod(brick)
    operands = [
        pltpu.with_memory_space_constraint(array, pltpu.HBM)
        for array in (
            initial_field, source_term, cell_class, class_shift,
            surface_cell.reshape(1, slots), panel_geometry,
        )
    ]
    operands.insert(5, live_count.reshape(1, 1))
    two, turns = 2 * channels, 3 * ROUNDS
    field, potential = pl.pallas_call(
        functools.partial(kernel, sizes),
        out_shape=(
            jax.ShapeDtypeStruct(brick, jnp.float32),
            jax.ShapeDtypeStruct((channels, slots), jnp.float32),
        ),
        in_specs=[hbm] * 5 + [pl.BlockSpec(memory_space=pl.ANY), hbm],
        out_specs=(vmem, vmem),
        scratch_shapes=[
            pltpu.VMEM(brick, jnp.float32),
            pltpu.VMEM(brick, jnp.float32),
            pltpu.VMEM((ROUNDS,) + brick, jnp.float32),
            pltpu.VMEM((size_x, size_y, size_z), jnp.int32),
            pltpu.VMEM(brick, jnp.float32),
            pltpu.VMEM((3,) + brick, jnp.float32),
            pltpu.VMEM((turns, 2, size_y // 2, two, size_z), jnp.bfloat16),
            pltpu.VMEM((turns + 1, 2, size_y // 2, two, size_z), jnp.bfloat16),
            pltpu.VMEM((turns, 2, size_x // 2, two, size_z), jnp.bfloat16),
            pltpu.VMEM((turns + 1, 2, size_x // 2, two, size_z), jnp.bfloat16),
            pltpu.VMEM((turns, two, size_z), jnp.bfloat16),
            pltpu.VMEM((turns + 1, 2, two, size_z), jnp.bfloat16),
            pltpu.VMEM((ROUNDS + 1, 2, 2, two, size_z), jnp.bfloat16),
            pltpu.VMEM((ROUNDS + 1, 2, 2, two, size_z), jnp.bfloat16),
            pltpu.VMEM((ROUNDS + 1, 2, 2, two, size_z), jnp.bfloat16),
            pltpu.VMEM((2, size_y, size_z), jnp.float32),
            pltpu.VMEM((3, size_y, size_z), jnp.float32),
            pltpu.VMEM((2, channels, size_z), jnp.float32),
            pltpu.VMEM((3, channels, size_z), jnp.float32),
            pltpu.VMEM((two, size_z), jnp.bfloat16),
            pltpu.VMEM((3, two, size_z), jnp.bfloat16),
            pltpu.VMEM((2, size_y, channels, size_z), jnp.float32),
            pltpu.VMEM((2, size_x, channels, size_z), jnp.float32),
            pltpu.VMEM((two, size_z), jnp.float32),
            pltpu.VMEM((2, size_y, channels, size_z), jnp.float32),
            pltpu.VMEM((2, size_x, channels, size_z), jnp.float32),
            pltpu.VMEM((two, size_z), jnp.float32),
            pltpu.VMEM((size_y + size_x + 2, channels, size_z), jnp.float32),
            pltpu.VMEM((devices, 4, slots), jnp.float32),
            pltpu.VMEM((3, slots, slots), jnp.float32),
            pltpu.VMEM((rows, slots, group * slots), jnp.bfloat16),
            pltpu.VMEM((ROUNDS, channels, slots), jnp.bfloat16),
            pltpu.VMEM((ROUNDS, devices, channels, slots), jnp.bfloat16),
            pltpu.VMEM((size_x * size_y, channels, slots), jnp.float32),
            pltpu.SMEM(class_shift.shape, jnp.float32),
            pltpu.VMEM((1, 1), jnp.int32),
            pltpu.VMEM((1, slots), jnp.int32),
            pltpu.VMEM(panel_geometry.shape, jnp.float32),
            pltpu.SemaphoreType.REGULAR((max(1, len(relays(sizes))),)),
            pltpu.SemaphoreType.DMA((7,)),
            pltpu.SemaphoreType.DMA((1,)),
            pltpu.SemaphoreType.DMA((5,)),
            pltpu.SemaphoreType.DMA((1,)),
            pltpu.SemaphoreType.DMA((1,)),
            pltpu.SemaphoreType.DMA((rows,)),
            pltpu.SemaphoreType.DMA((ROUNDS, rows)),
        ],
        compiler_params=pltpu.CompilerParams(
            collective_id=0, has_side_effects=True, vmem_limit_bytes=grant
        ),
    )(*operands)
    return pl.pallas_call(
        place,
        out_shape=(
            jax.ShapeDtypeStruct(initial_field.shape, jnp.float32),
            jax.ShapeDtypeStruct((channels, slots), jnp.float32),
        ),
        in_specs=[vmem] * 2,
        out_specs=(hbm, hbm),
        scratch_shapes=[pltpu.SemaphoreType.DMA((2,))],
        compiler_params=pltpu.CompilerParams(vmem_limit_bytes=8 * math.prod(brick)),
    )(field, potential)


def solution(mesh):
    placed = (
        P(None, "row", "col", "gz"),
        P(None, "row", "col", "gz"),
        P("row", "col", "gz"),
        P(),
        P(("row", "col", "gz")),
        P(("row", "col", "gz")),
        P(None, ("row", "col", "gz")),
    )
    return jax.shard_map(
        functools.partial(local, tuple(mesh.shape[axis] for axis in AXES)),
        mesh=mesh,
        in_specs=placed,
        out_specs=(P(None, "row", "col", "gz"), P(None, ("row", "col", "gz"))),
        check_vma=False,
    )
```
